256 devices in a mesh: ga: 8 (over z_lo, core), band: 32 (over x, z_hi, y).
Axes of the slice: x: 4, y: 4, z: 8 (z_hi: 2, z_lo: 4; z = z_hi * 4 + z_lo), core: 2. Of those that a mesh axis runs over, the one named last changes fastest.
Arguments:
- orbitals: bfloat16 [1024, 2, 65536], P('band', None, 'ga'), may hold values from -6 to 6
- projectors: bfloat16 [864, 2, 65536], P(None, None, ('ga', 'band')), may hold values from -0.015625 to 0.015625
- coupling: float32 [4, 18, 18], replicated, may hold values from -12 to 12
- species: int32 [48], replicated, may hold values from 0 to 3
- offsets: int32 [48], replicated, may hold values from 0 to 846, as said below
Outputs:
- applied: bfloat16 [1024, 2, 65536], P('band', None, 'ga')
The draws below stay inside these ranges and needn't reach their ends.
Inputs may be any that keep to these rules, and one draw needn't show every extreme that they name: Each atom's 18 projectors are the 18 consecutive rows of projectors starting at its offset; offsets are multiples of 18, and the atoms' blocks are distinct and cover all 864 rows.
All inputs are finite; a program needn't handle non-finite values.
Results may differ from the reference program's by a relative error of at most 0.0049.
Values may be sent and summed in bfloat16 or wider, within the bound.
A program may use at most 64 MiB of HBM per device.

```python
import jax
import jax.numpy as jnp
from jax import lax

NBANDS = 1024
PROJ = 18
NSP = 4
ATOMS = 48
NPW = 65536
NKB = 864


def draw_offsets(key, part):
    order = jax.random.permutation(key, ATOMS)
    return (order * PROJ).astype(jnp.int32)


def plant(drawn, stream_key, smallest, largest):
    extent = drawn.shape
    spot = [jax.random.randint(jax.random.fold_in(stream_key, axis), (), 0, extent[axis]) for axis in range(len(extent))]
    drawn = drawn.at[tuple(spot)].set(smallest)
    longest = extent.index(max(extent))
    spot[longest] = (spot[longest] + 1) % extent[longest]
    return drawn.at[tuple(spot)].set(largest)


def block_scale(key, dims, cuts, least, top_value):
    gain = 1.0
    for axis_at, blocks in cuts:
        heights = jax.random.uniform(jax.random.fold_in(jax.random.fold_in(key, 6), axis_at), (blocks,), jnp.float32, least / len(cuts), top_value / len(cuts))
        gain = gain * jnp.repeat(jnp.exp(heights), dims[axis_at] // blocks).reshape((-1,) + (1,) * (len(dims) - 1 - axis_at))
    return gain


def normal_values(stream_key, shape, spread, most, pieces=(), held_as=jnp.bfloat16):
    values = spread * jax.random.normal(stream_key, shape, jnp.float32)
    if pieces:
        values = values * block_scale(stream_key, shape, pieces, -0.22, 0.18)
    return jnp.clip(values, -most, most).astype(held_as)


def setup_inputs(seed: int = 0) -> dict:
    arg_keys = jax.random.split(jax.random.key(seed), 6)
    return {
        "orbitals": normal_values(arg_keys[0], (NBANDS, 2, NPW), 1.0, 6.0, ((0, 32), (2, 8))),
        "projectors": normal_values(arg_keys[1], (NKB, 2, NPW), (2 * NPW) ** -0.5, 0.015625, ((2, 256),)),
        "coupling": normal_values(arg_keys[2], (NSP, PROJ, PROJ), ((NPW / (18 * NKB)) ** 0.5), 12.0, (), jnp.float32),
        "species": plant(jax.random.randint(arg_keys[3], (ATOMS,), 0, NSP), jax.random.fold_in(arg_keys[3], 1), 0, NSP - 1).astype(jnp.int32),
        "offsets": draw_offsets(jax.random.fold_in(arg_keys[5], 71), 0),
    }


def reference(orbitals, projectors, coupling, species, offsets):
    total_proj = projectors.shape[0]
    total_bands = orbitals.shape[0]
    per_atom = coupling.shape[1]
    flat_proj = projectors.reshape(total_proj, -1)
    turned = jnp.concatenate([orbitals[:, 1, :], -orbitals[:, 0, :]], axis=1)
    stacked = jnp.concatenate([orbitals.reshape(total_bands, -1), turned], axis=0)
    becp = lax.dot_general(flat_proj, stacked, (((1,), (1,)), ((), ())), preferred_element_type=jnp.float32)
    becp = becp.reshape(ATOMS, per_atom, 2 * total_bands)
    blocks = (offsets // per_atom).astype(jnp.int32)
    atom_kind = jnp.zeros((ATOMS,), jnp.int32).at[blocks].set(species)
    matrices = coupling[atom_kind].astype(jnp.float32)
    dbecp = jnp.einsum("aij,ajc->aic", matrices, becp, precision=lax.Precision.HIGHEST)
    dbecp = dbecp.reshape(total_proj, 2 * total_bands).astype(jnp.bfloat16)
    real_part = lax.dot_general(dbecp, projectors[:, 0, :], (((0,), (0,)), ((), ())), preferred_element_type=jnp.float32)
    imag_part = lax.dot_general(dbecp, projectors[:, 1, :], (((0,), (0,)), ((), ())), preferred_element_type=jnp.float32)
    out_real = real_part[:total_bands] - imag_part[total_bands:]
    out_imag = imag_part[:total_bands] + real_part[total_bands:]
    return jnp.stack([out_real, out_imag], axis=1).astype(jnp.bfloat16)
```

```python
import jax
import jax.numpy as jnp
from jax import lax
from jax.experimental import pallas as pl
from jax.experimental.pallas import tpu as pltpu
from jax.sharding import PartitionSpec as P

NX, NY, NH, NZ, NC = 4, 4, 2, 4, 2
XY = NX * NY
PER_ATOM = 18
GROUP_ATOMS = 14
GROUPS = ((0, 256), (256, 256), (512, 256), (768, 128))
WIDTH = 256
ROWS = 896
HIGHEST = lax.Precision.HIGHEST
NT = (((1,), (1,)), ((), ()))
NN = (((1,), (0,)), ((), ()))


def coupling_matrix(group, cpad, species, offsets):
    row = lax.broadcasted_iota(jnp.int32, (256, 1), 0)
    row_atom = (row * 3641) >> 16
    row_in = row - row_atom * PER_ATOM
    start = (row_atom + GROUP_ATOMS * group) * PER_ATOM
    kind = jnp.sum(
        jnp.where(offsets == start, species.astype(jnp.float32), 0.0), axis=1, keepdims=True
    )
    col = lax.broadcasted_iota(jnp.int32, (256, 128), 1)
    col_kind = (col * 3641) >> 16
    col_in = col - col_kind * PER_ATOM
    pick = jnp.where(
        (col_kind.astype(jnp.float32) == kind) & (col_in == row_in), 1.0, 0.0
    ).astype(jnp.float32)
    rows = lax.dot_general(pick, cpad, NN, precision=HIGHEST, preferred_element_type=jnp.float32)
    wide = lax.broadcasted_iota(jnp.int32, (128, 256), 1)
    wide_atom = (wide * 3641) >> 16
    spread = jnp.where(
        wide - wide_atom * PER_ATOM == lax.broadcasted_iota(jnp.int32, (128, 256), 0), 1.0, 0.0
    ).astype(jnp.float32)
    full = lax.dot_general(rows, spread, NN, precision=HIGHEST, preferred_element_type=jnp.float32)
    full_row = lax.broadcasted_iota(jnp.int32, (256, 256), 0)
    full_col = lax.broadcasted_iota(jnp.int32, (256, 256), 1)
    same = ((full_row * 3641) >> 16) == ((full_col * 3641) >> 16)
    return jnp.where(same, full, 0.0)


def turn_matrix():
    row = lax.broadcasted_iota(jnp.int32, (256, 256), 0)
    col = lax.broadcasted_iota(jnp.int32, (256, 256), 1)
    even = (row & 1) == 0
    up = even & (col == row + 1)
    down = jnp.logical_not(even) & (col == row - 1)
    return (jnp.where(up, 1.0, 0.0) - jnp.where(down, 1.0, 0.0)).astype(jnp.bfloat16)


def kernel(
    orb, proj, coup, species, offsets, out,
    pz, pd, pf, xt, xj, jm, cm, cpad, sb, rb, town, zs, zr, dg, dj, acc, ab,
    pz_s, pz_r, pd_s, pd_r, pf_s, pf_r, o_s, o_r, rs_s, rs_r, z_s, z_r, ag_s, ag_r, b_s, b_r, loc_s,
):
    ga = lax.axis_index("ga")
    band = lax.axis_index("band")
    zl, core = ga // NC, ga % NC
    x, h, y = band // (NH * NY), band // NY % NH, band % NY
    me = x * NY + y

    def xy_band(k):
        return k // NY * (NH * NY) + h * NY + k % NY

    def copy(src, dst, send, recv, to_ga, to_band):
        return pltpu.make_async_remote_copy(
            src_ref=src, dst_ref=dst, send_sem=send, recv_sem=recv,
            device_id={"ga": to_ga, "band": to_band},
            device_id_type=pl.DeviceIdType.MESH,
        )

    def arrived(ref, sem):
        copy(ref, ref, sem, sem, ga, band).wait_recv()

    def left(ref, sem):
        copy(ref, ref, sem, sem, ga, band).wait_send()

    other_core = zl * NC + 1 - core
    other_half = band + NY - 2 * NY * h

    barrier = pltpu.get_barrier_semaphore()

    def greet(to_ga, to_band):
        pl.semaphore_signal(
            barrier, inc=1, device_id={"ga": to_ga, "band": to_band},
            device_id_type=pl.DeviceIdType.MESH,
        )

    greet(ga, other_half)
    for c in range(1, NZ):
        greet((zl + c) % NZ * NC + core, band)
    greet(other_core, band)

    def greet_plane(d, _):
        k = (me + d) % XY
        greet(ga, xy_band(k))
        greet(other_core, xy_band(k))
        return 0

    lax.fori_loop(1, XY, greet_plane, 0)
    pl.semaphore_wait(barrier, 1 + (NZ - 1) + 1 + 2 * (XY - 1))

    def z_copy(k):
        rows = pl.ds(GROUPS[k][0], GROUPS[k][1])
        return copy(proj.at[rows], pz.at[rows], pz_s.at[k], pz_r.at[k], ga, other_half)

    def fwd_copy(k):
        rows = pl.ds(GROUPS[k][0], GROUPS[k][1])
        return copy(pz.at[rows], pf.at[rows], pf_s.at[k], pf_r.at[k], other_core, band)

    z_copy(0).start()
    z_copy(1).start()
    own_copy = copy(proj, pd, pd_s, pd_r, other_core, band)
    own_copy.start()

    def orb_copy(k, c):
        return copy(
            orb.at[k // NY, :, k % NY, pl.ds(32 * c, 32), :],
            xt.at[core, :, pl.ds(32 * me, 32), :],
            o_s, o_r.at[core], zl * NC + c, xy_band(k),
        )

    def orb_send(d, _):
        k = (me + d) % XY
        orb_copy(k, core).start()
        orb_copy(k, 1 - core).start()
        return 0

    lax.fori_loop(1, XY, orb_send, 0)
    orb_copy(me, 1 - core).start()
    for q in range(NH):
        xt[core, q, pl.ds(32 * me, 32), :] = orb[x, q, y, pl.ds(32 * core, 32), :]

    jm[...] = turn_matrix()
    cpad[...] = jnp.zeros_like(cpad)
    for s in range(4):
        cpad[pl.ds(PER_ATOM * s, PER_ATOM), pl.ds(0, PER_ATOM)] = coup[s]
    for k in range(4):
        cm[k] = coupling_matrix(k, cpad[...], species[...], offsets[...])

    arrived(xt.at[core, :, pl.ds(0, 480), :], o_r.at[core])
    arrived(xt.at[1 - core], o_r.at[1 - core])

    def turn(i, _):
        g, q, r = i // 4, i // 2 % 2, i % 2
        rows = pl.ds(256 * r, 256)
        xj[g, q, rows, :] = lax.dot_general(
            jm[...], xt[g, q, rows, :], NN, preferred_element_type=jnp.float32
        ).astype(jnp.bfloat16)
        return 0

    lax.fori_loop(0, 8, turn, 0)
    arrived(pd, pd_r)

    pieces = ((proj, core, h), (pz, core, 1 - h), (pd, 1 - core, h), (pf, 1 - core, 1 - h))

    def first_product(k):
        start, n = GROUPS[k]

        def block(r, _):
            rows = pl.ds(256 * r, 256)
            total = None
            for ref, g, q in pieces:
                re = lax.dot_general(
                    xt[g, q, rows, :], ref[pl.ds(start, n), pl.ds(0, 256)], NT,
                    preferred_element_type=jnp.float32,
                )
                im = lax.dot_general(
                    xj[g, q, rows, :], ref[pl.ds(start, n), pl.ds(256, 256)], NT,
                    preferred_element_type=jnp.float32,
                )
                total = re + im if total is None else total + re + im
            sb[k, rows, pl.ds(0, n)] = total.astype(jnp.bfloat16)
            return 0

        lax.fori_loop(0, 2, block, 0)

    def rs_send(k):
        n = GROUPS[k][1]

        def one(d, _):
            to = (me + d) % XY
            copy(
                sb.at[k, pl.ds(32 * to, 32), pl.ds(0, n)],
                rb.at[k, XY - 1 - d, :, pl.ds(0, n)],
                rs_s.at[k], rs_r.at[k], ga, xy_band(to),
            ).start()
            return 0

        lax.fori_loop(1, XY, one, 0)

    def z_sum(k):
        n = GROUPS[k][1]
        arrived(rb.at[k, :, :, pl.ds(0, n)], rs_r.at[k])
        total = sb[k, pl.ds(32 * me, 32), pl.ds(0, n)].astype(jnp.float32)
        for d in range(XY - 1):
            total = total + rb[k, d, :, pl.ds(0, n)].astype(jnp.float32)
        town[k, :, pl.ds(0, n)] = total
        zs[k, :, pl.ds(0, n)] = total.astype(jnp.bfloat16)
        for c in range(1, NZ):
            to = (zl + c) % NZ
            copy(
                zs.at[k, :, pl.ds(0, n)], zr.at[k, NZ - 1 - c, :, pl.ds(0, n)],
                z_s.at[k], z_r.at[k], to * NC + core, band,
            ).start()

    def couple(k):
        n = GROUPS[k][1]
        arrived(zr.at[k, :, :, pl.ds(0, n)], z_r.at[k])
        total = town[k, :, pl.ds(0, n)]
        for c in range(NZ - 1):
            total = total + zr[k, c, :, pl.ds(0, n)].astype(jnp.float32)
        coupled = lax.dot_general(
            total, cm[k, pl.ds(0, n), pl.ds(0, n)], NT, precision=HIGHEST,
            preferred_element_type=jnp.float32,
        )
        mine = pl.ds(32 * me, 32)
        dg[k, mine, pl.ds(0, n)] = coupled.astype(jnp.bfloat16)

        def one(d, _):
            to = (me + d) % XY
            part = dg.at[k, mine, pl.ds(0, n)]
            copy(part, part, ag_s.at[k], ag_r.at[k], ga, xy_band(to)).start()
            return 0

        lax.fori_loop(1, XY, one, 0)

    def gather(k):
        n = GROUPS[k][1]
        arrived(dg.at[k, pl.ds(0, 480), pl.ds(0, n)], ag_r.at[k])

        def block(r, _):
            rows = pl.ds(256 * r, 256)
            dj[k, rows, pl.ds(0, n)] = (
                -lax.dot_general(
                    jm[...], dg[k, rows, pl.ds(0, n)], NN, preferred_element_type=jnp.float32
                )
            ).astype(jnp.bfloat16)
            return 0

        lax.fori_loop(0, 2, block, 0)

    def second_product(groups, first, last):
        for ref, g, q in pieces:

            def block(r, _):
                rows = pl.ds(256 * r, 256)
                total = None
                for k in groups:
                    start, n = GROUPS[k]
                    re = lax.dot_general(
                        dg[k, rows, pl.ds(0, n)], ref[pl.ds(start, n), pl.ds(0, 256)], NN,
                        preferred_element_type=jnp.float32,
                    )
                    im = lax.dot_general(
                        dj[k, rows, pl.ds(0, n)], ref[pl.ds(start, n), pl.ds(256, 256)], NN,
                        preferred_element_type=jnp.float32,
                    )
                    total = re + im if total is None else total + re + im
                if not first:
                    total = total + acc[g, q, rows, :]
                if last:
                    ab[g, q, rows, :] = total.astype(jnp.bfloat16)
                else:
                    acc[g, q, rows, :] = total
                return 0

            lax.fori_loop(0, 2, block, 0)

    for k in range(4):
        z_copy(k).wait_recv()
        fwd_copy(k).start()
        z_copy(k).wait_send()
        if k + 2 < 4:
            z_copy(k + 2).start()
        fwd_copy(k).wait_recv()
        first_product(k)
        rs_send(k)
        if k >= 1:
            z_sum(k - 1)
        if k >= 2:
            couple(k - 2)
    couple(2)
    gather(0)
    gather(1)
    second_product((0, 1), True, False)
    z_sum(3)
    gather(2)
    second_product((2,), False, False)
    couple(3)
    gather(3)
    second_product((3,), False, True)

    def back_copy(k, c):
        return copy(
            ab.at[c, :, pl.ds(32 * k, 32), :],
            out.at[x, :, y, pl.ds(32 * core, 32), :],
            b_s, b_r.at[core], zl * NC + c, xy_band(k),
        )

    def back_send(d, _):
        k = (me + d) % XY
        back_copy(k, core).start()
        back_copy(k, 1 - core).start()
        return 0

    lax.fori_loop(1, XY, back_send, 0)
    back_copy(me, 1 - core).start()
    local = pltpu.make_async_copy(
        ab.at[core, :, pl.ds(32 * me, 32), :], out.at[x, :, y, pl.ds(32 * core, 32), :], loc_s
    )
    local.start()

    left(proj, pd_s)
    for k in range(4):
        n = GROUPS[k][1]
        fwd_copy(k).wait_send()
        left(rb.at[k, :, :, pl.ds(0, n)], rs_s.at[k])
        left(zr.at[k, :, :, pl.ds(0, n)], z_s.at[k])
        left(dg.at[k, pl.ds(0, 480), pl.ds(0, n)], ag_s.at[k])
    left(xt.at[0], o_s)
    left(xt.at[0, :, pl.ds(0, 480), :], o_s)
    left(ab.at[0], b_s)
    left(ab.at[0, :, pl.ds(0, 480), :], b_s)
    local.wait()
    arrived(ab.at[core, :, pl.ds(0, 480), :], b_r.at[core])
    arrived(ab.at[1 - core], b_r.at[1 - core])


def per_device(orbitals, projectors, coupling, species, offsets):
    bf16, f32 = jnp.bfloat16, jnp.float32
    bands = orbitals.shape[0]
    orb = orbitals.reshape(bands, 2, NX, NH, NY, WIDTH).transpose(2, 3, 4, 0, 1, 5)
    orb = orb.reshape(NX, NH, NY, 2 * bands, WIDTH)
    flat = projectors.reshape(projectors.shape[0], 2 * WIDTH)
    step = GROUP_ATOMS * PER_ATOM
    parts = []
    for k in range(4):
        part = flat[step * k : step * (k + 1)]
        parts.append(jnp.pad(part, ((0, GROUPS[k][1] - part.shape[0]), (0, 0))))
    proj = jnp.concatenate(parts, axis=0)
    vmem = pl.BlockSpec(memory_space=pltpu.VMEM)
    dma = pltpu.SemaphoreType.DMA
    out = pl.pallas_call(
        kernel,
        out_shape=jax.ShapeDtypeStruct(orb.shape, bf16),
        in_specs=[vmem] * 5,
        out_specs=pl.BlockSpec(memory_space=pl.ANY),
        scratch_shapes=[
            pltpu.VMEM((ROWS, 512), bf16),
            pltpu.VMEM((ROWS, 512), bf16),
            pltpu.VMEM((ROWS, 512), bf16),
            pltpu.VMEM((2, 2, 512, 256), bf16),
            pltpu.VMEM((2, 2, 512, 256), bf16),
            pltpu.VMEM((256, 256), bf16),
            pltpu.VMEM((4, 256, 256), f32),
            pltpu.VMEM((128, 128), f32),
            pltpu.VMEM((4, 512, 256), bf16),
            pltpu.VMEM((4, XY - 1, 32, 256), bf16),
            pltpu.VMEM((4, 32, 256), f32),
            pltpu.VMEM((4, 32, 256), bf16),
            pltpu.VMEM((4, NZ - 1, 32, 256), bf16),
            pltpu.VMEM((4, 512, 256), bf16),
            pltpu.VMEM((4, 512, 256), bf16),
            pltpu.VMEM((2, 2, 512, 256), f32),
            pltpu.VMEM((2, 2, 512, 256), bf16),
            dma((4,)), dma((4,)), dma, dma, dma((4,)), dma((4,)),
            dma, dma((2,)), dma((4,)), dma((4,)), dma((4,)), dma((4,)),
            dma((4,)), dma((4,)), dma, dma((2,)), dma,
        ],
        compiler_params=pltpu.CompilerParams(collective_id=0, has_side_effects=True),
    )(orb, proj, coupling, species.reshape(1, -1), offsets.reshape(1, -1))
    out = out.reshape(NX, NH, NY, bands, 2, WIDTH).transpose(3, 4, 0, 1, 2, 5)
    return out.reshape(orbitals.shape)


def solution(mesh):
    placed = (P("band", None, "ga"), P(None, None, ("ga", "band")), P(), P(), P())
    return jax.shard_map(
        per_device, mesh=mesh, in_specs=placed, out_specs=P("band", None, "ga"), check_vma=False
    )
```

```python
import jax
import jax.numpy as jnp
from jax import lax
from jax.experimental import pallas as pl
from jax.experimental.pallas import tpu as pltpu
from jax.sharding import PartitionSpec as P

NX, NY, NH, NZ, NC = 4, 4, 2, 4, 2
XY = NX * NY
PER_ATOM = 18
GROUP_ATOMS = 14
GROUPS = ((0, 256), (256, 256), (512, 256), (768, 128))
WIDTH = 256
ROWS = 896
COUNTS = (252, 252, 252, 108)
HIGHEST = lax.Precision.HIGHEST
NT = (((1,), (1,)), ((), ()))
NN = (((1,), (0,)), ((), ()))


def coupling_matrix(group, cpad, species, offsets):
    row = lax.broadcasted_iota(jnp.int32, (256, 1), 0)
    row_atom = (row * 3641) >> 16
    row_in = row - row_atom * PER_ATOM
    start = (row_atom + GROUP_ATOMS * group) * PER_ATOM
    kind = jnp.sum(
        jnp.where(offsets == start, species.astype(jnp.float32), 0.0), axis=1, keepdims=True
    )
    col = lax.broadcasted_iota(jnp.int32, (256, 128), 1)
    col_in, col_kind = col >> 2, col & 3
    pick = jnp.where(
        (col_kind.astype(jnp.float32) == kind) & (col_in == row_in), 1.0, 0.0
    ).astype(jnp.float32)
    rows = lax.dot_general(pick, cpad, NN, precision=HIGHEST, preferred_element_type=jnp.float32)
    wide = lax.broadcasted_iota(jnp.int32, (128, 256), 1)
    wide_atom = (wide * 3641) >> 16
    spread = jnp.where(
        wide - wide_atom * PER_ATOM == lax.broadcasted_iota(jnp.int32, (128, 256), 0), 1.0, 0.0
    ).astype(jnp.float32)
    full = lax.dot_general(rows, spread, NN, precision=HIGHEST, preferred_element_type=jnp.float32)
    full_row = lax.broadcasted_iota(jnp.int32, (256, 256), 0)
    full_col = lax.broadcasted_iota(jnp.int32, (256, 256), 1)
    same = ((full_row * 3641) >> 16) == ((full_col * 3641) >> 16)
    return jnp.where(same, full, 0.0)


def turn_matrix():
    row = lax.broadcasted_iota(jnp.int32, (256, 256), 0)
    col = lax.broadcasted_iota(jnp.int32, (256, 256), 1)
    even = (row & 1) == 0
    up = even & (col == row + 1)
    down = jnp.logical_not(even) & (col == row - 1)
    return (jnp.where(up, 1.0, 0.0) - jnp.where(down, 1.0, 0.0)).astype(jnp.bfloat16)


def split_matrix():
    row = lax.broadcasted_iota(jnp.int32, (256, 256), 0)
    col = lax.broadcasted_iota(jnp.int32, (256, 256), 1)
    return jnp.where(col == (row & 127) * 2 + (row >> 7), 1.0, 0.0).astype(jnp.bfloat16)


def kernel(
    orb, proj, coup, species, offsets, out,
    praw, pc, xr, xt, xj, jm, pm, cm, cpad, sb, rb, town, zs, zr, dg, dj, acc, ab,
    pz_s, pz_r, pd_s, pd_r, pf_s, pf_r, o_s, o_r, rs_s, rs_r, z_s, z_r, ag_s, ag_r, b_s, b_r,
    own_s, oo_s, loc_s,
):
    ga = lax.axis_index("ga")
    band = lax.axis_index("band")
    zl, core = ga // NC, ga % NC
    x, h, y = band // (NH * NY), band // NY % NH, band % NY
    me = x * NY + y

    def xy_band(k):
        return k // NY * (NH * NY) + h * NY + k % NY

    def copy(src, dst, send, recv, to_ga, to_band):
        return pltpu.make_async_remote_copy(
            src_ref=src, dst_ref=dst, send_sem=send, recv_sem=recv,
            device_id={"ga": to_ga, "band": to_band},
            device_id_type=pl.DeviceIdType.MESH,
        )

    def arrived(ref, sem):
        copy(ref, ref, sem, sem, ga, band).wait_recv()

    def left(ref, sem):
        copy(ref, ref, sem, sem, ga, band).wait_send()

    other_core = zl * NC + 1 - core
    other_half = band + NY - 2 * NY * h

    barrier = pltpu.get_barrier_semaphore()

    def part(k):
        return pl.ds(GROUPS[k][0], COUNTS[k])

    def source(k):
        return proj.at[pl.ds(GROUP_ATOMS * PER_ATOM * k, COUNTS[k])]

    def columns(k, q):
        block = k // NY * (NH * NY) + q * NY + k % NY
        return pl.ds(pl.multiple_of(WIDTH * block, WIDTH), WIDTH)

    def greet(to_ga, to_band):
        pl.semaphore_signal(
            barrier, inc=1, device_id={"ga": to_ga, "band": to_band},
            device_id_type=pl.DeviceIdType.MESH,
        )

    greet(ga, other_half)
    for c in range(1, NZ):
        greet((zl + c) % NZ * NC + core, band)
    greet(other_core, band)

    def greet_plane(d, _):
        k = (me + d) % XY
        greet(ga, xy_band(k))
        greet(other_core, xy_band(k))
        return 0

    lax.fori_loop(1, XY, greet_plane, 0)
    own = [pltpu.make_async_copy(source(k), praw.at[0, part(k)], own_s.at[k]) for k in range(4)]
    for k in range(4):
        own[k].start()

    def z_copy(k):
        return copy(source(k), praw.at[1, part(k)], pz_s.at[k], pz_r.at[k], ga, other_half)

    def core_copy(k):
        return copy(source(k), praw.at[2, part(k)], pd_s.at[k], pd_r.at[k], other_core, band)

    def fwd_copy(k):
        return copy(
            praw.at[1, part(k)], praw.at[3, part(k)], pf_s.at[k], pf_r.at[k], other_core, band
        )

    for piece in range(4):
        for k in range(4):
            pad = GROUPS[k][1] - COUNTS[k]
            praw[piece, pl.ds(GROUPS[k][0] + COUNTS[k], pad)] = jnp.zeros(
                (pad, 2, WIDTH), jnp.bfloat16
            )

    pl.semaphore_wait(barrier, 1 + (NZ - 1) + 1 + 2 * (XY - 1))
    z_copy(0).start()
    z_copy(1).start()

    def orb_copy(k, c, q):
        return copy(
            orb.at[pl.ds(16 * c, 16), :, columns(k, q)],
            xr.at[core, q, pl.ds(16 * me, 16)],
            o_s, o_r.at[core], zl * NC + c, xy_band(k),
        )

    def orb_send(d, _):
        k = (me + d) % XY
        for q in range(NH):
            orb_copy(k, core, q).start()
            orb_copy(k, 1 - core, q).start()
        return 0

    lax.fori_loop(1, XY, orb_send, 0)
    own_orb = []
    for q in range(NH):
        orb_copy(me, 1 - core, q).start()
        own_orb.append(
            pltpu.make_async_copy(
                orb.at[pl.ds(16 * core, 16), :, columns(me, q)],
                xr.at[core, q, pl.ds(16 * me, 16)],
                oo_s.at[q],
            )
        )
        own_orb[q].start()
    for k in range(4):
        core_copy(k).start()

    jm[...] = turn_matrix()
    pm[...] = split_matrix()
    cpad[...] = jnp.zeros_like(cpad)
    for i in range(PER_ATOM):
        cpad[pl.ds(4 * i, 4), pl.ds(0, PER_ATOM)] = coup[i]
    for k in range(4):
        cm[k] = coupling_matrix(k, cpad[...], species[...], offsets[...])

    for k in range(4):
        own[k].wait()
        core_copy(k).wait_recv()

    def split(k, piece):
        start, n = GROUPS[k]

        def block(i, _):
            at = pl.multiple_of(start + 128 * i, 128)
            both = lax.dot_general(
                pm[...], praw[piece, pl.ds(at, 128)].reshape(256, WIDTH), NN,
                preferred_element_type=jnp.float32,
            ).astype(jnp.bfloat16)
            pc[piece, 0, pl.ds(at, 128), :] = both[:128]
            pc[piece, 1, pl.ds(at, 128), :] = both[128:]
            return 0

        lax.fori_loop(0, n // 128, block, 0)

    for k in range(4):
        split(k, 0)
        split(k, 2)

    for q in range(NH):
        own_orb[q].wait()
    arrived(xr.at[core, :, pl.ds(0, 240)], o_r.at[core])
    arrived(xr.at[1 - core], o_r.at[1 - core])

    def turn(i, _):
        g, q, r = i // 4, i // 2 % 2, i % 2
        rows = pl.ds(pl.multiple_of(256 * r, 256), 256)
        value = xr[g, q, pl.ds(pl.multiple_of(128 * r, 128), 128)].reshape(256, WIDTH)
        xt[g, q, rows, :] = value
        xj[g, q, rows, :] = lax.dot_general(
            jm[...], value, NN, preferred_element_type=jnp.float32
        ).astype(jnp.bfloat16)
        return 0

    lax.fori_loop(0, 8, turn, 0)

    pieces = ((0, core, h), (1, core, 1 - h), (2, 1 - core, h), (3, 1 - core, 1 - h))

    def first_product(k):
        start, n = GROUPS[k]

        def block(r, _):
            rows = pl.ds(256 * r, 256)
            total = None
            for i, g, q in pieces:
                re = lax.dot_general(
                    xt[g, q, rows, :], pc[i, 0, pl.ds(start, n), :], NT,
                    preferred_element_type=jnp.float32,
                )
                im = lax.dot_general(
                    xj[g, q, rows, :], pc[i, 1, pl.ds(start, n), :], NT,
                    preferred_element_type=jnp.float32,
                )
                total = re + im if total is None else total + re + im
            sb[k, rows, pl.ds(0, n)] = total.astype(jnp.bfloat16)
            return 0

        lax.fori_loop(0, 2, block, 0)

    def rs_send(k):
        n = GROUPS[k][1]

        def one(d, _):
            to = (me + d) % XY
            copy(
                sb.at[k, pl.ds(32 * to, 32), pl.ds(0, n)],
                rb.at[k, XY - 1 - d, :, pl.ds(0, n)],
                rs_s.at[k], rs_r.at[k], ga, xy_band(to),
            ).start()
            return 0

        lax.fori_loop(1, XY, one, 0)

    def z_sum(k):
        n = GROUPS[k][1]
        arrived(rb.at[k, :, :, pl.ds(0, n)], rs_r.at[k])
        total = sb[k, pl.ds(32 * me, 32), pl.ds(0, n)].astype(jnp.float32)
        for d in range(XY - 1):
            total = total + rb[k, d, :, pl.ds(0, n)].astype(jnp.float32)
        town[k, :, pl.ds(0, n)] = total
        zs[k, :, pl.ds(0, n)] = total.astype(jnp.bfloat16)
        for c in range(1, NZ):
            to = (zl + c) % NZ
            copy(
                zs.at[k, :, pl.ds(0, n)], zr.at[k, NZ - 1 - c, :, pl.ds(0, n)],
                z_s.at[k], z_r.at[k], to * NC + core, band,
            ).start()

    def couple(k):
        n = GROUPS[k][1]
        arrived(zr.at[k, :, :, pl.ds(0, n)], z_r.at[k])
        total = town[k, :, pl.ds(0, n)]
        for c in range(NZ - 1):
            total = total + zr[k, c, :, pl.ds(0, n)].astype(jnp.float32)
        coupled = lax.dot_general(
            total, cm[k, pl.ds(0, n), pl.ds(0, n)], NT, precision=HIGHEST,
            preferred_element_type=jnp.float32,
        )
        mine = pl.ds(32 * me, 32)
        dg[k, mine, pl.ds(0, n)] = coupled.astype(jnp.bfloat16)

        def one(d, _):
            to = (me + d) % XY
            part = dg.at[k, mine, pl.ds(0, n)]
            copy(part, part, ag_s.at[k], ag_r.at[k], ga, xy_band(to)).start()
            return 0

        lax.fori_loop(1, XY, one, 0)

    def gather(k):
        n = GROUPS[k][1]
        arrived(dg.at[k, pl.ds(0, 480), pl.ds(0, n)], ag_r.at[k])

        def block(r, _):
            rows = pl.ds(256 * r, 256)
            dj[k, rows, pl.ds(0, n)] = (
                -lax.dot_general(
                    jm[...], dg[k, rows, pl.ds(0, n)], NN, preferred_element_type=jnp.float32
                )
            ).astype(jnp.bfloat16)
            return 0

        lax.fori_loop(0, 2, block, 0)

    def second_piece(i, g, q, groups, first, last):
        def block(r, _):
            rows = pl.ds(pl.multiple_of(256 * r, 256), 256)
            total = None
            for k in groups:
                start, n = GROUPS[k]
                re = lax.dot_general(
                    dg[k, rows, pl.ds(0, n)], pc[i, 0, pl.ds(start, n), :], NN,
                    preferred_element_type=jnp.float32,
                )
                im = lax.dot_general(
                    dj[k, rows, pl.ds(0, n)], pc[i, 1, pl.ds(start, n), :], NN,
                    preferred_element_type=jnp.float32,
                )
                total = re + im if total is None else total + re + im
            if not first:
                total = total + acc[i, rows, :]
            if last:
                bands = pl.ds(pl.multiple_of(128 * r, 128), 128)
                ab[g, q, bands] = total.astype(jnp.bfloat16).reshape(128, 2, WIDTH)
            else:
                acc[i, rows, :] = total
            return 0

        lax.fori_loop(0, 2, block, 0)

    def second_product(groups, first):
        for i, g, q in pieces:
            second_piece(i, g, q, groups, first, False)

    for k in range(4):
        z_copy(k).wait_recv()
        fwd_copy(k).start()
        z_copy(k).wait_send()
        if k + 2 < 4:
            z_copy(k + 2).start()
        split(k, 1)
        fwd_copy(k).wait_recv()
        split(k, 3)
        first_product(k)
        rs_send(k)
        if k >= 1:
            z_sum(k - 1)
        if k >= 2:
            couple(k - 2)
    couple(2)
    gather(0)
    z_sum(3)
    gather(1)
    second_product((0, 1), True)
    couple(3)
    gather(2)
    second_product((2,), False)
    gather(3)

    def back_copy(k, c, q):
        return copy(
            ab.at[c, q, pl.ds(16 * k, 16)],
            out.at[pl.ds(16 * core, 16), :, columns(me, q)],
            b_s, b_r.at[core], zl * NC + c, xy_band(k),
        )

    for side, c in ((2, 1 - core), (0, core)):
        for i, g, q in pieces[side : side + 1] + pieces[side + 1 : side + 2]:
            second_piece(i, g, q, (3,), False, True)

        def back_send(d, _):
            k = (me + d) % XY
            for q in range(NH):
                back_copy(k, c, q).start()
            return 0

        lax.fori_loop(1, XY, back_send, 0)
        if side == 2:
            for q in range(NH):
                back_copy(me, c, q).start()
    local = [
        pltpu.make_async_copy(
            ab.at[core, q, pl.ds(16 * me, 16)],
            out.at[pl.ds(16 * core, 16), :, columns(me, q)],
            loc_s.at[q],
        )
        for q in range(NH)
    ]
    for q in range(NH):
        local[q].start()

    for k in range(4):
        n = GROUPS[k][1]
        core_copy(k).wait_send()
        fwd_copy(k).wait_send()
        left(rb.at[k, :, :, pl.ds(0, n)], rs_s.at[k])
        left(zr.at[k, :, :, pl.ds(0, n)], z_s.at[k])
        left(dg.at[k, pl.ds(0, 480), pl.ds(0, n)], ag_s.at[k])
    left(xr.at[0], o_s)
    left(xr.at[0, :, pl.ds(0, 240)], o_s)
    left(ab.at[0], b_s)
    left(ab.at[0, :, pl.ds(0, 240)], b_s)
    for q in range(NH):
        local[q].wait()
    arrived(ab.at[core, :, pl.ds(0, 240)], b_r.at[core])
    arrived(ab.at[1 - core], b_r.at[1 - core])


def per_device(orbitals, projectors, coupling, species, offsets):
    bf16, f32 = jnp.bfloat16, jnp.float32
    vmem = pl.BlockSpec(memory_space=pltpu.VMEM)
    hbm = pl.BlockSpec(memory_space=pltpu.HBM)
    dma = pltpu.SemaphoreType.DMA
    return pl.pallas_call(
        kernel,
        out_shape=jax.ShapeDtypeStruct(orbitals.shape, bf16),
        in_specs=[hbm, hbm, vmem, vmem, vmem],
        out_specs=hbm,
        scratch_shapes=[
            pltpu.VMEM((4, ROWS, 2, WIDTH), bf16),
            pltpu.VMEM((4, 2, ROWS, WIDTH), bf16),
            pltpu.VMEM((2, 2, 256, 2, WIDTH), bf16),
            pltpu.VMEM((2, 2, 512, WIDTH), bf16),
            pltpu.VMEM((2, 2, 512, WIDTH), bf16),
            pltpu.VMEM((256, 256), bf16),
            pltpu.VMEM((256, 256), bf16),
            pltpu.VMEM((4, 256, 256), f32),
            pltpu.VMEM((128, 128), f32),
            pltpu.VMEM((4, 512, 256), bf16),
            pltpu.VMEM((4, XY - 1, 32, 256), bf16),
            pltpu.VMEM((4, 32, 256), f32),
            pltpu.VMEM((4, 32, 256), bf16),
            pltpu.VMEM((4, NZ - 1, 32, 256), bf16),
            pltpu.VMEM((4, 512, 256), bf16),
            pltpu.VMEM((4, 512, 256), bf16),
            pltpu.VMEM((4, 512, WIDTH), f32),
            pltpu.VMEM((2, 2, 256, 2, WIDTH), bf16),
            dma((4,)), dma((4,)), dma((4,)), dma((4,)), dma((4,)), dma((4,)),
            dma, dma((2,)), dma((4,)), dma((4,)), dma((4,)), dma((4,)),
            dma((4,)), dma((4,)), dma, dma((2,)), dma((4,)), dma((2,)), dma((2,)),
        ],
        compiler_params=pltpu.CompilerParams(collective_id=0, has_side_effects=True),
    )(
        orbitals, projectors, coupling.transpose(1, 0, 2),
        species.reshape(1, -1), offsets.reshape(1, -1),
    )


def solution(mesh):
    placed = (P("band", None, "ga"), P(None, None, ("ga", "band")), P(), P(), P())
    return jax.shard_map(
        per_device, mesh=mesh, in_specs=placed, out_specs=P("band", None, "ga"), check_vma=False
    )
```

```python
import jax
import jax.numpy as jnp
from jax import lax
from jax.experimental import pallas as pl
from jax.experimental.pallas import tpu as pltpu
from jax.sharding import PartitionSpec as P

NX, NY, NH, NZ, NC = 4, 4, 2, 4, 2
XY = NX * NY
PER_ATOM = 18
GROUP_ATOMS = 14
GROUPS = ((0, 256), (256, 256), (512, 256), (768, 128))
WIDTH = 256
ROWS = 896
COUNTS = (252, 252, 252, 108)
HIGHEST = lax.Precision.HIGHEST
NT = (((1,), (1,)), ((), ()))
NN = (((1,), (0,)), ((), ()))


def coupling_matrix(group, cpad, species, offsets):
    row = lax.broadcasted_iota(jnp.int32, (256, 1), 0)
    row_atom = (row * 3641) >> 16
    row_in = row - row_atom * PER_ATOM
    start = (row_atom + GROUP_ATOMS * group) * PER_ATOM
    kind = jnp.sum(
        jnp.where(offsets == start, species.astype(jnp.float32), 0.0), axis=1, keepdims=True
    )
    col = lax.broadcasted_iota(jnp.int32, (256, 128), 1)
    col_in, col_kind = col >> 2, col & 3
    pick = jnp.where(
        (col_kind.astype(jnp.float32) == kind) & (col_in == row_in), 1.0, 0.0
    ).astype(jnp.float32)
    rows = lax.dot_general(pick, cpad, NN, precision=HIGHEST, preferred_element_type=jnp.float32)
    wide = lax.broadcasted_iota(jnp.int32, (128, 256), 1)
    wide_atom = (wide * 3641) >> 16
    spread = jnp.where(
        wide - wide_atom * PER_ATOM == lax.broadcasted_iota(jnp.int32, (128, 256), 0), 1.0, 0.0
    ).astype(jnp.float32)
    full = lax.dot_general(rows, spread, NN, precision=HIGHEST, preferred_element_type=jnp.float32)
    full_row = lax.broadcasted_iota(jnp.int32, (256, 256), 0)
    full_col = lax.broadcasted_iota(jnp.int32, (256, 256), 1)
    same = ((full_row * 3641) >> 16) == ((full_col * 3641) >> 16)
    return jnp.where(same, full, 0.0)


def turn_matrix():
    row = lax.broadcasted_iota(jnp.int32, (256, 256), 0)
    col = lax.broadcasted_iota(jnp.int32, (256, 256), 1)
    even = (row & 1) == 0
    up = even & (col == row + 1)
    down = jnp.logical_not(even) & (col == row - 1)
    return (jnp.where(up, 1.0, 0.0) - jnp.where(down, 1.0, 0.0)).astype(jnp.bfloat16)


def split_matrix():
    row = lax.broadcasted_iota(jnp.int32, (256, 256), 0)
    col = lax.broadcasted_iota(jnp.int32, (256, 256), 1)
    return jnp.where(col == (row & 127) * 2 + (row >> 7), 1.0, 0.0).astype(jnp.bfloat16)


def kernel(
    orb, proj, coup_hbm, species_hbm, offsets_hbm, out,
    praw, pc, xr, xt, xj, jm, pm, cm, cpad, sb, rb, town, zs, zr, dg, dj, acc, ab,
    pz_s, pz_r, pd_s, pd_r, pf_s, pf_r, o_s, o_r, rs_s, rs_r, z_s, z_r, ag_s, ag_r, b_s, b_r,
    own_s, oo_s,
    coup, species, offsets, small_s, pacc,
):
    ga = lax.axis_index("ga")
    band = lax.axis_index("band")
    zl, core = ga // NC, ga % NC
    x, h, y = band // (NH * NY), band // NY % NH, band % NY
    me = x * NY + y

    def xy_band(k):
        return k // NY * (NH * NY) + h * NY + k % NY

    def copy(src, dst, send, recv, to_ga, to_band):
        return pltpu.make_async_remote_copy(
            src_ref=src, dst_ref=dst, send_sem=send, recv_sem=recv,
            device_id={"ga": to_ga, "band": to_band},
            device_id_type=pl.DeviceIdType.MESH,
        )

    def arrived(ref, sem):
        copy(ref, ref, sem, sem, ga, band).wait_recv()

    def left(ref, sem):
        copy(ref, ref, sem, sem, ga, band).wait_send()

    other_core = zl * NC + 1 - core
    other_half = band + NY - 2 * NY * h

    barrier = pltpu.get_barrier_semaphore()

    def part(k):
        return pl.ds(GROUPS[k][0], COUNTS[k])

    def source(k):
        return proj.at[pl.ds(GROUP_ATOMS * PER_ATOM * k, COUNTS[k])]

    def columns(k, q):
        block = k // NY * (NH * NY) + q * NY + k % NY
        return pl.ds(pl.multiple_of(WIDTH * block, WIDTH), WIDTH)

    def greet(to_ga, to_band):
        pl.semaphore_signal(
            barrier, inc=1, device_id={"ga": to_ga, "band": to_band},
            device_id_type=pl.DeviceIdType.MESH,
        )

    greet(ga, other_half)
    for c in range(1, NZ):
        greet((zl + c) % NZ * NC + core, band)
    greet(other_core, band)

    def greet_plane(d, _):
        k = (me + d) % XY
        greet(ga, xy_band(k))
        greet(other_core, xy_band(k))
        return 0

    lax.fori_loop(1, XY, greet_plane, 0)
    own = [pltpu.make_async_copy(source(k), praw.at[0, part(k)], own_s.at[k]) for k in range(4)]
    for k in range(4):
        own[k].start()

    def z_copy(k):
        return copy(source(k), praw.at[1, part(k)], pz_s.at[k], pz_r.at[k], ga, other_half)

    def core_copy(k):
        return copy(source(k), praw.at[2, part(k)], pd_s.at[k], pd_r.at[k], other_core, band)

    def fwd_copy(k):
        return copy(
            praw.at[1, part(k)], praw.at[3, part(k)], pf_s.at[k], pf_r.at[k], other_core, band
        )

    for piece in range(4):
        for k in range(4):
            pad = GROUPS[k][1] - COUNTS[k]
            praw[piece, pl.ds(GROUPS[k][0] + COUNTS[k], pad)] = jnp.zeros(
                (pad, 2, WIDTH), jnp.bfloat16
            )

    pl.semaphore_wait(barrier, 1 + (NZ - 1) + 1 + 2 * (XY - 1))
    for k in range(4):
        z_copy(k).start()

    def orb_copy(k, c, q):
        return copy(
            orb.at[pl.ds(16 * c, 16), :, columns(k, q)],
            xr.at[core, q, pl.ds(16 * me, 16)],
            o_s, o_r.at[core], zl * NC + c, xy_band(k),
        )

    def orb_send(d, _):
        k = (me + d) % XY
        for q in range(NH):
            orb_copy(k, core, q).start()
            orb_copy(k, 1 - core, q).start()
        return 0

    lax.fori_loop(1, XY, orb_send, 0)
    own_orb = []
    for q in range(NH):
        orb_copy(me, 1 - core, q).start()
        own_orb.append(
            pltpu.make_async_copy(
                orb.at[pl.ds(16 * core, 16), :, columns(me, q)],
                xr.at[core, q, pl.ds(16 * me, 16)],
                oo_s.at[q],
            )
        )
        own_orb[q].start()
    for k in range(4):
        core_copy(k).start()
    small = [
        pltpu.make_async_copy(coup_hbm, coup, small_s.at[0]),
        pltpu.make_async_copy(species_hbm, species, small_s.at[1]),
        pltpu.make_async_copy(offsets_hbm, offsets, small_s.at[2]),
    ]
    for one in small:
        one.start()

    jm[...] = turn_matrix()
    pm[...] = split_matrix()
    cpad[...] = jnp.zeros_like(cpad)
    for one in small:
        one.wait()
    for i in range(PER_ATOM):
        cpad[pl.ds(4 * i, 4), pl.ds(0, PER_ATOM)] = coup[i]
    for k in range(4):
        cm[k] = coupling_matrix(k, cpad[...], species[...], offsets[...])

    for k in range(4):
        own[k].wait()
        core_copy(k).wait_recv()

    def split(k, piece):
        start, n = GROUPS[k]

        def block(i, _):
            at = pl.multiple_of(start + 128 * i, 128)
            both = lax.dot_general(
                pm[...], praw[piece, pl.ds(at, 128)].reshape(256, WIDTH), NN,
                preferred_element_type=jnp.float32,
            ).astype(jnp.bfloat16)
            pc[piece, 0, pl.ds(at, 128), :] = both[:128]
            pc[piece, 1, pl.ds(at, 128), :] = both[128:]
            return 0

        lax.fori_loop(0, n // 128, block, 0)

    for k in range(4):
        split(k, 0)
        split(k, 2)

    for q in range(NH):
        own_orb[q].wait()
    arrived(xr.at[core, :, pl.ds(0, 240)], o_r.at[core])
    arrived(xr.at[1 - core], o_r.at[1 - core])

    def turn(i, _):
        g, q, r = i // 4, i // 2 % 2, i % 2
        rows = pl.ds(pl.multiple_of(256 * r, 256), 256)
        value = xr[g, q, pl.ds(pl.multiple_of(128 * r, 128), 128)].reshape(256, WIDTH)
        xt[g, q, rows, :] = value
        xj[g, q, rows, :] = lax.dot_general(
            jm[...], value, NN, preferred_element_type=jnp.float32
        ).astype(jnp.bfloat16)
        return 0

    lax.fori_loop(0, 8, turn, 0)

    pieces = ((0, core, h), (1, core, 1 - h), (2, 1 - core, h), (3, 1 - core, 1 - h))

    def pieces_product(k, r, chosen):
        start, n = GROUPS[k]
        rows = pl.ds(pl.multiple_of(256 * r, 256), 256)
        total = None
        for i, g, q in chosen:
            re = lax.dot_general(
                xt[g, q, rows, :], pc[i, 0, pl.ds(start, n), :], NT,
                preferred_element_type=jnp.float32,
            )
            im = lax.dot_general(
                xj[g, q, rows, :], pc[i, 1, pl.ds(start, n), :], NT,
                preferred_element_type=jnp.float32,
            )
            total = re + im if total is None else total + re + im
        return rows, total

    def first_early(k):
        n = GROUPS[k][1]

        def block(r, _):
            rows, total = pieces_product(k, r, (pieces[0], pieces[2]))
            pacc[rows, pl.ds(0, n)] = total
            return 0

        lax.fori_loop(0, 2, block, 0)

    def first_product(k):
        n = GROUPS[k][1]

        def block(r, _):
            rows, total = pieces_product(k, r, (pieces[1], pieces[3]))
            sb[k, rows, pl.ds(0, n)] = (total + pacc[rows, pl.ds(0, n)]).astype(jnp.bfloat16)
            return 0

        lax.fori_loop(0, 2, block, 0)

    def rs_send(k):
        n = GROUPS[k][1]

        def one(d, _):
            to = (me + d) % XY
            copy(
                sb.at[k, pl.ds(32 * to, 32), pl.ds(0, n)],
                rb.at[k, XY - 1 - d, :, pl.ds(0, n)],
                rs_s.at[k], rs_r.at[k], ga, xy_band(to),
            ).start()
            return 0

        lax.fori_loop(1, XY, one, 0)

    def z_sum(k):
        n = GROUPS[k][1]
        arrived(rb.at[k, :, :, pl.ds(0, n)], rs_r.at[k])
        total = sb[k, pl.ds(32 * me, 32), pl.ds(0, n)].astype(jnp.float32)
        for d in range(XY - 1):
            total = total + rb[k, d, :, pl.ds(0, n)].astype(jnp.float32)
        town[k, :, pl.ds(0, n)] = total
        zs[k, :, pl.ds(0, n)] = total.astype(jnp.bfloat16)
        for c in range(1, NZ):
            to = (zl + c) % NZ
            copy(
                zs.at[k, :, pl.ds(0, n)], zr.at[k, NZ - 1 - c, :, pl.ds(0, n)],
                z_s.at[k], z_r.at[k], to * NC + core, band,
            ).start()

    def couple(k):
        n = GROUPS[k][1]
        arrived(zr.at[k, :, :, pl.ds(0, n)], z_r.at[k])
        total = town[k, :, pl.ds(0, n)]
        for c in range(NZ - 1):
            total = total + zr[k, c, :, pl.ds(0, n)].astype(jnp.float32)
        coupled = lax.dot_general(
            total, cm[k, pl.ds(0, n), pl.ds(0, n)], NT, precision=HIGHEST,
            preferred_element_type=jnp.float32,
        )
        mine = pl.ds(32 * me, 32)
        dg[k, mine, pl.ds(0, n)] = coupled.astype(jnp.bfloat16)

        def one(d, _):
            to = (me + d) % XY
            part = dg.at[k, mine, pl.ds(0, n)]
            copy(part, part, ag_s.at[k], ag_r.at[k], ga, xy_band(to)).start()
            return 0

        lax.fori_loop(1, XY, one, 0)

    def gather(k):
        n = GROUPS[k][1]
        arrived(dg.at[k, pl.ds(0, 480), pl.ds(0, n)], ag_r.at[k])

        def block(r, _):
            rows = pl.ds(256 * r, 256)
            dj[k, rows, pl.ds(0, n)] = (
                -lax.dot_general(
                    jm[...], dg[k, rows, pl.ds(0, n)], NN, preferred_element_type=jnp.float32
                )
            ).astype(jnp.bfloat16)
            return 0

        lax.fori_loop(0, 2, block, 0)

    def second_piece(i, g, q, groups, first, last):
        def block(r, _):
            rows = pl.ds(pl.multiple_of(256 * r, 256), 256)
            total = None
            for k in groups:
                start, n = GROUPS[k]
                re = lax.dot_general(
                    dg[k, rows, pl.ds(0, n)], pc[i, 0, pl.ds(start, n), :], NN,
                    preferred_element_type=jnp.float32,
                )
                im = lax.dot_general(
                    dj[k, rows, pl.ds(0, n)], pc[i, 1, pl.ds(start, n), :], NN,
                    preferred_element_type=jnp.float32,
                )
                total = re + im if total is None else total + re + im
            if not first:
                total = total + acc[i, rows, :]
            if last:
                bands = pl.ds(pl.multiple_of(128 * r, 128), 128)
                ab[g, q, bands] = total.astype(jnp.bfloat16).reshape(128, 2, WIDTH)
            else:
                acc[i, rows, :] = total
            return 0

        lax.fori_loop(0, 2, block, 0)

    def second_product(groups, first):
        for i, g, q in pieces:
            second_piece(i, g, q, groups, first, False)

    for k in range(4):
        first_early(k)
        z_copy(k).wait_recv()
        fwd_copy(k).start()
        split(k, 1)
        fwd_copy(k).wait_recv()
        split(k, 3)
        first_product(k)
        rs_send(k)
        if k >= 1:
            z_sum(k - 1)
        if k >= 2:
            couple(k - 2)
    couple(2)
    gather(0)
    z_sum(3)
    gather(1)
    second_product((0, 1), True)
    couple(3)
    gather(2)
    second_product((2,), False)
    gather(3)

    def back_copy(k, c, q):
        return copy(
            ab.at[c, q, pl.ds(16 * k, 16)],
            out.at[pl.ds(16 * core, 16), :, columns(me, q)],
            b_s, b_r.at[core], zl * NC + c, xy_band(k),
        )

    for side, c in ((2, 1 - core), (0, core)):
        for i, g, q in pieces[side : side + 1] + pieces[side + 1 : side + 2]:
            second_piece(i, g, q, (3,), False, True)

        def back_send(d, _):
            k = (me + d) % XY
            for q in range(NH):
                back_copy(k, c, q).start()
            return 0

        lax.fori_loop(1, XY, back_send, 0)
        if side == 2:
            for q in range(NH):
                back_copy(me, c, q).start()
    for q in range(NH):
        out[pl.ds(16 * core, 16), :, columns(me, q)] = ab[core, q, pl.ds(16 * me, 16)]

    for k in range(4):
        n = GROUPS[k][1]
        z_copy(k).wait_send()
        core_copy(k).wait_send()
        fwd_copy(k).wait_send()
        left(rb.at[k, :, :, pl.ds(0, n)], rs_s.at[k])
        left(zr.at[k, :, :, pl.ds(0, n)], z_s.at[k])
        left(dg.at[k, pl.ds(0, 480), pl.ds(0, n)], ag_s.at[k])
    left(xr.at[0], o_s)
    left(xr.at[0, :, pl.ds(0, 240)], o_s)
    left(ab.at[0], b_s)
    left(ab.at[0, :, pl.ds(0, 240)], b_s)
    arrived(ab.at[core, :, pl.ds(0, 240)], b_r.at[core])
    arrived(ab.at[1 - core], b_r.at[1 - core])


def per_device(orbitals, projectors, coupling, species, offsets):
    bf16, f32 = jnp.bfloat16, jnp.float32
    vmem = pl.BlockSpec(memory_space=pltpu.VMEM)
    hbm = pl.BlockSpec(memory_space=pltpu.HBM)
    dma = pltpu.SemaphoreType.DMA
    return pl.pallas_call(
        kernel,
        out_shape=pltpu.VMEM(orbitals.shape, bf16),
        in_specs=[hbm] * 5,
        out_specs=vmem,
        scratch_shapes=[
            pltpu.VMEM((4, ROWS, 2, WIDTH), bf16),
            pltpu.VMEM((4, 2, ROWS, WIDTH), bf16),
            pltpu.VMEM((2, 2, 256, 2, WIDTH), bf16),
            pltpu.VMEM((2, 2, 512, WIDTH), bf16),
            pltpu.VMEM((2, 2, 512, WIDTH), bf16),
            pltpu.VMEM((256, 256), bf16),
            pltpu.VMEM((256, 256), bf16),
            pltpu.VMEM((4, 256, 256), f32),
            pltpu.VMEM((128, 128), f32),
            pltpu.VMEM((4, 512, 256), bf16),
            pltpu.VMEM((4, XY - 1, 32, 256), bf16),
            pltpu.VMEM((4, 32, 256), f32),
            pltpu.VMEM((4, 32, 256), bf16),
            pltpu.VMEM((4, NZ - 1, 32, 256), bf16),
            pltpu.VMEM((4, 512, 256), bf16),
            pltpu.VMEM((4, 512, 256), bf16),
            pltpu.VMEM((4, 512, WIDTH), f32),
            pltpu.VMEM((2, 2, 256, 2, WIDTH), bf16),
            dma((4,)), dma((4,)), dma((4,)), dma((4,)), dma((4,)), dma((4,)),
            dma, dma((2,)), dma((4,)), dma((4,)), dma((4,)), dma((4,)),
            dma((4,)), dma((4,)), dma, dma((2,)), dma((4,)), dma((2,)),
            pltpu.VMEM((PER_ATOM, 4, PER_ATOM), f32),
            pltpu.VMEM((1, 48), jnp.int32),
            pltpu.VMEM((1, 48), jnp.int32),
            dma((3,)),
            pltpu.VMEM((512, 256), f32),
        ],
        compiler_params=pltpu.CompilerParams(collective_id=0, has_side_effects=True),
    )(
        orbitals, projectors, coupling.transpose(1, 0, 2),
        species.reshape(1, -1), offsets.reshape(1, -1),
    )


def solution(mesh):
    placed = (P("band", None, "ga"), P(None, None, ("ga", "band")), P(), P(), P())
    return jax.shard_map(
        per_device, mesh=mesh, in_specs=placed, out_specs=P("band", None, "ga"), check_vma=False
    )
```

```python
import jax
import jax.numpy as jnp
from jax import lax
from jax.experimental import pallas as pl
from jax.experimental.pallas import tpu as pltpu
from jax.sharding import PartitionSpec as P

NX, NY, NH, NZ, NC = 4, 4, 2, 4, 2
XY = NX * NY
PER_ATOM = 18
GROUP_ATOMS = 14
GROUPS = ((0, 256), (256, 256), (512, 256), (768, 128))
WIDTH = 256
ROWS = 896
COUNTS = (252, 252, 252, 108)
OFFSETS = sorted(
    ((dx, dy) for dx in range(NX) for dy in range(NY)),
    key=lambda at: (min(at[0], NX - at[0]) + min(at[1], NY - at[1]), at),
)
BATCHES = ((0, 5), (5, 11), (11, 16))
HIGHEST = lax.Precision.HIGHEST
NT = (((1,), (1,)), ((), ()))
NN = (((1,), (0,)), ((), ()))


def coupling_matrix(group, cpad, species, offsets):
    row = lax.broadcasted_iota(jnp.int32, (256, 1), 0)
    row_atom = (row * 3641) >> 16
    row_in = row - row_atom * PER_ATOM
    start = (row_atom + GROUP_ATOMS * group) * PER_ATOM
    kind = jnp.sum(
        jnp.where(offsets == start, species.astype(jnp.float32), 0.0), axis=1, keepdims=True
    )
    col = lax.broadcasted_iota(jnp.int32, (256, 128), 1)
    col_in, col_kind = col >> 2, col & 3
    pick = jnp.where(
        (col_kind.astype(jnp.float32) == kind) & (col_in == row_in), 1.0, 0.0
    ).astype(jnp.float32)
    rows = lax.dot_general(pick, cpad, NN, precision=HIGHEST, preferred_element_type=jnp.float32)
    wide = lax.broadcasted_iota(jnp.int32, (128, 256), 1)
    wide_atom = (wide * 3641) >> 16
    spread = jnp.where(
        wide - wide_atom * PER_ATOM == lax.broadcasted_iota(jnp.int32, (128, 256), 0), 1.0, 0.0
    ).astype(jnp.float32)
    full = lax.dot_general(rows, spread, NN, precision=HIGHEST, preferred_element_type=jnp.float32)
    full_row = lax.broadcasted_iota(jnp.int32, (256, 256), 0)
    full_col = lax.broadcasted_iota(jnp.int32, (256, 256), 1)
    same = ((full_row * 3641) >> 16) == ((full_col * 3641) >> 16)
    return jnp.where(same, full, 0.0)


def turn_matrix():
    row = lax.broadcasted_iota(jnp.int32, (256, 256), 0)
    col = lax.broadcasted_iota(jnp.int32, (256, 256), 1)
    even = (row & 1) == 0
    up = even & (col == row + 1)
    down = jnp.logical_not(even) & (col == row - 1)
    return (jnp.where(up, 1.0, 0.0) - jnp.where(down, 1.0, 0.0)).astype(jnp.bfloat16)


def split_matrix():
    row = lax.broadcasted_iota(jnp.int32, (256, 256), 0)
    col = lax.broadcasted_iota(jnp.int32, (256, 256), 1)
    return jnp.where(col == (row & 127) * 2 + (row >> 7), 1.0, 0.0).astype(jnp.bfloat16)


def kernel(
    orb, proj, coup_hbm, species_hbm, offsets_hbm, out,
    praw, pc, xr, xt, xj, jm, pm, cm, cpad, sb, rb, town, zs, zr, dg, dj, acc, ab,
    pz_s, pz_r, pd_s, pd_r, pf_s, pf_r, o_s, o_r, rs_s, rs_r, z_s, z_r, ag_s, ag_r, b_s, b_r,
    own_s, oo_s,
    coup, species, offsets, small_s, pacc,
):
    ga = lax.axis_index("ga")
    band = lax.axis_index("band")
    zl, core = ga // NC, ga % NC
    x, h, y = band // (NH * NY), band // NY % NH, band % NY
    me = x * NY + y

    def apart(offset, sign):
        dx, dy = offset
        return (x + NX + sign * dx) % NX * (NH * NY) + h * NY + (y + NY + sign * dy) % NY

    def xy_band(k):
        return k // NY * (NH * NY) + h * NY + k % NY

    def copy(src, dst, send, recv, to_ga, to_band):
        return pltpu.make_async_remote_copy(
            src_ref=src, dst_ref=dst, send_sem=send, recv_sem=recv,
            device_id={"ga": to_ga, "band": to_band},
            device_id_type=pl.DeviceIdType.MESH,
        )

    def arrived(ref, sem):
        copy(ref, ref, sem, sem, ga, band).wait_recv()

    def left(ref, sem):
        copy(ref, ref, sem, sem, ga, band).wait_send()

    other_core = zl * NC + 1 - core
    other_half = band + NY - 2 * NY * h

    barrier = pltpu.get_barrier_semaphore()

    def part(k):
        return pl.ds(GROUPS[k][0], COUNTS[k])

    def source(k):
        return proj.at[pl.ds(GROUP_ATOMS * PER_ATOM * k, COUNTS[k])]

    def columns(k, q):
        block = k // NY * (NH * NY) + q * NY + k % NY
        return pl.ds(pl.multiple_of(WIDTH * block, WIDTH), WIDTH)

    def greet(to_ga, to_band):
        pl.semaphore_signal(
            barrier, inc=1, device_id={"ga": to_ga, "band": to_band},
            device_id_type=pl.DeviceIdType.MESH,
        )

    greet(ga, other_half)
    for c in range(1, NZ):
        greet((zl + c) % NZ * NC + core, band)
    greet(other_core, band)

    def greet_plane(d, _):
        k = (me + d) % XY
        greet(ga, xy_band(k))
        greet(other_core, xy_band(k))
        return 0

    lax.fori_loop(1, XY, greet_plane, 0)
    own = [pltpu.make_async_copy(source(k), praw.at[0, part(k)], own_s.at[k]) for k in range(4)]
    for k in range(4):
        own[k].start()

    def z_copy(k):
        return copy(source(k), praw.at[1, part(k)], pz_s.at[k], pz_r.at[k], ga, other_half)

    def core_copy(k):
        return copy(source(k), praw.at[2, part(k)], pd_s.at[k], pd_r.at[k], other_core, band)

    def fwd_copy(k):
        return copy(
            praw.at[1, part(k)], praw.at[3, part(k)], pf_s.at[k], pf_r.at[k], other_core, band
        )

    for piece in range(4):
        for k in range(4):
            pad = GROUPS[k][1] - COUNTS[k]
            praw[piece, pl.ds(GROUPS[k][0] + COUNTS[k], pad)] = jnp.zeros(
                (pad, 2, WIDTH), jnp.bfloat16
            )

    pl.semaphore_wait(barrier, 1 + (NZ - 1) + 1 + 2 * (XY - 1))
    for k in range(4):
        z_copy(k).start()

    def orb_copy(k, c, q):
        return copy(
            orb.at[pl.ds(16 * c, 16), :, columns(k, q)],
            xr.at[core, q, pl.ds(16 * me, 16)],
            o_s, o_r.at[core], zl * NC + c, xy_band(k),
        )

    def orb_send(d, _):
        k = (me + d) % XY
        for q in range(NH):
            orb_copy(k, core, q).start()
            orb_copy(k, 1 - core, q).start()
        return 0

    lax.fori_loop(1, XY, orb_send, 0)
    own_orb = []
    for q in range(NH):
        orb_copy(me, 1 - core, q).start()
        own_orb.append(
            pltpu.make_async_copy(
                orb.at[pl.ds(16 * core, 16), :, columns(me, q)],
                xr.at[core, q, pl.ds(16 * me, 16)],
                oo_s.at[q],
            )
        )
        own_orb[q].start()
    for k in range(4):
        core_copy(k).start()
    small = [
        pltpu.make_async_copy(coup_hbm, coup, small_s.at[0]),
        pltpu.make_async_copy(species_hbm, species, small_s.at[1]),
        pltpu.make_async_copy(offsets_hbm, offsets, small_s.at[2]),
    ]
    for one in small:
        one.start()

    jm[...] = turn_matrix()
    pm[...] = split_matrix()
    cpad[...] = jnp.zeros_like(cpad)
    for one in small:
        one.wait()
    for i in range(PER_ATOM):
        cpad[pl.ds(4 * i, 4), pl.ds(0, PER_ATOM)] = coup[i]
    for k in range(4):
        cm[k] = coupling_matrix(k, cpad[...], species[...], offsets[...])

    for k in range(4):
        own[k].wait()
        core_copy(k).wait_recv()

    def split(k, piece):
        start, n = GROUPS[k]

        def block(i, _):
            at = pl.multiple_of(start + 128 * i, 128)
            both = lax.dot_general(
                pm[...], praw[piece, pl.ds(at, 128)].reshape(256, WIDTH), NN,
                preferred_element_type=jnp.float32,
            ).astype(jnp.bfloat16)
            pc[piece, 0, pl.ds(at, 128), :] = both[:128]
            pc[piece, 1, pl.ds(at, 128), :] = both[128:]
            return 0

        lax.fori_loop(0, n // 128, block, 0)

    for k in range(4):
        split(k, 0)
        split(k, 2)

    for q in range(NH):
        own_orb[q].wait()
    arrived(xr.at[core, :, pl.ds(0, 240)], o_r.at[core])
    arrived(xr.at[1 - core], o_r.at[1 - core])

    def turn(i, _):
        g, q, r = i // 4, i // 2 % 2, i % 2
        rows = pl.ds(pl.multiple_of(256 * r, 256), 256)
        value = xr[g, q, pl.ds(pl.multiple_of(128 * r, 128), 128)].reshape(256, WIDTH)
        xt[g, q, rows, :] = value
        xj[g, q, rows, :] = lax.dot_general(
            jm[...], value, NN, preferred_element_type=jnp.float32
        ).astype(jnp.bfloat16)
        return 0

    lax.fori_loop(0, 8, turn, 0)

    pieces = ((0, core, h), (1, core, 1 - h), (2, 1 - core, h), (3, 1 - core, 1 - h))

    def pieces_product(k, r, chosen):
        start, n = GROUPS[k]
        rows = pl.ds(pl.multiple_of(256 * r, 256), 256)
        total = None
        for i, g, q in chosen:
            re = lax.dot_general(
                xt[g, q, rows, :], pc[i, 0, pl.ds(start, n), :], NT,
                preferred_element_type=jnp.float32,
            )
            im = lax.dot_general(
                xj[g, q, rows, :], pc[i, 1, pl.ds(start, n), :], NT,
                preferred_element_type=jnp.float32,
            )
            total = re + im if total is None else total + re + im
        return rows, total

    def first_early(k):
        n = GROUPS[k][1]

        def block(r, _):
            rows, total = pieces_product(k, r, (pieces[0], pieces[2]))
            pacc[rows, pl.ds(0, n)] = total
            return 0

        lax.fori_loop(0, 2, block, 0)

    def first_product(k):
        n = GROUPS[k][1]

        def block(r, _):
            rows, total = pieces_product(k, r, (pieces[1], pieces[3]))
            sb[k, rows, pl.ds(0, n)] = (total + pacc[rows, pl.ds(0, n)]).astype(jnp.bfloat16)
            return 0

        lax.fori_loop(0, 2, block, 0)

    def rs_send(k):
        n = GROUPS[k][1]

        def one(d, _):
            to = (me + d) % XY
            copy(
                sb.at[k, pl.ds(32 * to, 32), pl.ds(0, n)],
                rb.at[k, XY - 1 - d, :, pl.ds(0, n)],
                rs_s.at[k], rs_r.at[k], ga, xy_band(to),
            ).start()
            return 0

        lax.fori_loop(1, XY, one, 0)

    def z_sum(k):
        n = GROUPS[k][1]
        arrived(rb.at[k, :, :, pl.ds(0, n)], rs_r.at[k])
        total = sb[k, pl.ds(32 * me, 32), pl.ds(0, n)].astype(jnp.float32)
        for d in range(XY - 1):
            total = total + rb[k, d, :, pl.ds(0, n)].astype(jnp.float32)
        town[k, :, pl.ds(0, n)] = total
        zs[k, :, pl.ds(0, n)] = total.astype(jnp.bfloat16)
        for c in range(1, NZ):
            to = (zl + c) % NZ
            copy(
                zs.at[k, :, pl.ds(0, n)], zr.at[k, NZ - 1 - c, :, pl.ds(0, n)],
                z_s.at[k], z_r.at[k], to * NC + core, band,
            ).start()

    def couple(k):
        n = GROUPS[k][1]
        arrived(zr.at[k, :, :, pl.ds(0, n)], z_r.at[k])
        total = town[k, :, pl.ds(0, n)]
        for c in range(NZ - 1):
            total = total + zr[k, c, :, pl.ds(0, n)].astype(jnp.float32)
        coupled = lax.dot_general(
            total, cm[k, pl.ds(0, n), pl.ds(0, n)], NT, precision=HIGHEST,
            preferred_element_type=jnp.float32,
        )
        dg[k, pl.ds(0, 32), pl.ds(0, n)] = coupled.astype(jnp.bfloat16)
        for batch, (first, end) in enumerate(BATCHES):
            for slot in range(max(first, 1), end):
                copy(
                    dg.at[k, pl.ds(0, 32), pl.ds(0, n)],
                    dg.at[k, pl.ds(32 * slot, 32), pl.ds(0, n)],
                    ag_s.at[k], ag_r.at[k, batch], ga, apart(OFFSETS[slot], -1),
                ).start()

    def gather_batch(k, batch):
        first, end = BATCHES[batch]
        first = max(first, 1)
        n = GROUPS[k][1]
        arrived(dg.at[k, pl.ds(32 * first, 32 * (end - first)), pl.ds(0, n)], ag_r.at[k, batch])

    def gather(k):
        n = GROUPS[k][1]
        for batch in range(3):
            gather_batch(k, batch)

        def block(r, _):
            rows = pl.ds(256 * r, 256)
            dj[k, rows, pl.ds(0, n)] = (
                -lax.dot_general(
                    jm[...], dg[k, rows, pl.ds(0, n)], NN, preferred_element_type=jnp.float32
                )
            ).astype(jnp.bfloat16)
            return 0

        lax.fori_loop(0, 2, block, 0)

    def second_piece(i, groups, first):
        def block(r, _):
            rows = pl.ds(pl.multiple_of(256 * r, 256), 256)
            total = None
            for k in groups:
                start, n = GROUPS[k]
                re = lax.dot_general(
                    dg[k, rows, pl.ds(0, n)], pc[i, 0, pl.ds(start, n), :], NN,
                    preferred_element_type=jnp.float32,
                )
                im = lax.dot_general(
                    dj[k, rows, pl.ds(0, n)], pc[i, 1, pl.ds(start, n), :], NN,
                    preferred_element_type=jnp.float32,
                )
                total = re + im if total is None else total + re + im
            if not first:
                total = total + acc[i, rows, :]
            acc[i, rows, :] = total
            return 0

        lax.fori_loop(0, 2, block, 0)

    def second_product(groups, first):
        for i in range(4):
            second_piece(i, groups, first)

    for k in range(4):
        first_early(k)
        z_copy(k).wait_recv()
        fwd_copy(k).start()
        split(k, 1)
        fwd_copy(k).wait_recv()
        split(k, 3)
        first_product(k)
        rs_send(k)
        if k >= 1:
            z_sum(k - 1)
        if k >= 2:
            couple(k - 2)
    couple(2)
    gather(0)
    z_sum(3)
    gather(1)
    second_product((0, 1), True)
    couple(3)
    gather(2)
    second_product((2,), False)

    def back_copy(slot, c, q):
        return copy(
            ab.at[c, q, pl.ds(16 * slot, 16)],
            out.at[pl.ds(16 * core, 16), :, columns(me, q)],
            b_s, b_r.at[core], zl * NC + c, apart(OFFSETS[slot], 1),
        )

    start, n = GROUPS[3]
    for batch, (first, end) in enumerate(BATCHES):
        gather_batch(3, batch)
        rows = pl.ds(32 * first, 32 * (end - first))
        value = dg[3, rows, pl.ds(0, n)].astype(jnp.float32)
        height = value.shape[0]
        even = (lax.broadcasted_iota(jnp.int32, value.shape, 0) & 1) == 0
        turned = jnp.where(
            even, -pltpu.roll(value, height - 1, 0), pltpu.roll(value, 1, 0)
        ).astype(jnp.bfloat16)
        for side, c in ((2, 1 - core), (0, core)):
            for i, g, q in pieces[side : side + 2]:
                re = lax.dot_general(
                    dg[3, rows, pl.ds(0, n)], pc[i, 0, pl.ds(start, n), :], NN,
                    preferred_element_type=jnp.float32,
                )
                im = lax.dot_general(
                    turned, pc[i, 1, pl.ds(start, n), :], NN,
                    preferred_element_type=jnp.float32,
                )
                ab[g, q, pl.ds(16 * first, 16 * (end - first))] = (
                    (re + im + acc[i, rows, :]).astype(jnp.bfloat16).reshape(height // 2, 2, WIDTH)
                )
            for slot in range(first, end):
                for q in range(NH):
                    if slot > 0 or side == 2:
                        back_copy(slot, c, q).start()
    for q in range(NH):
        out[pl.ds(16 * core, 16), :, columns(me, q)] = ab[core, q, pl.ds(0, 16)]

    for k in range(4):
        n = GROUPS[k][1]
        z_copy(k).wait_send()
        core_copy(k).wait_send()
        fwd_copy(k).wait_send()
        left(rb.at[k, :, :, pl.ds(0, n)], rs_s.at[k])
        left(zr.at[k, :, :, pl.ds(0, n)], z_s.at[k])
        left(dg.at[k, pl.ds(0, 480), pl.ds(0, n)], ag_s.at[k])
    left(xr.at[0], o_s)
    left(xr.at[0, :, pl.ds(0, 240)], o_s)
    left(ab.at[0], b_s)
    left(ab.at[0, :, pl.ds(0, 240)], b_s)
    arrived(ab.at[core, :, pl.ds(0, 240)], b_r.at[core])
    arrived(ab.at[1 - core], b_r.at[1 - core])


def per_device(orbitals, projectors, coupling, species, offsets):
    bf16, f32 = jnp.bfloat16, jnp.float32
    vmem = pl.BlockSpec(memory_space=pltpu.VMEM)
    hbm = pl.BlockSpec(memory_space=pltpu.HBM)
    dma = pltpu.SemaphoreType.DMA
    return pl.pallas_call(
        kernel,
        out_shape=pltpu.VMEM(orbitals.shape, bf16),
        in_specs=[hbm] * 5,
        out_specs=vmem,
        scratch_shapes=[
            pltpu.VMEM((4, ROWS, 2, WIDTH), bf16),
            pltpu.VMEM((4, 2, ROWS, WIDTH), bf16),
            pltpu.VMEM((2, 2, 256, 2, WIDTH), bf16),
            pltpu.VMEM((2, 2, 512, WIDTH), bf16),
            pltpu.VMEM((2, 2, 512, WIDTH), bf16),
            pltpu.VMEM((256, 256), bf16),
            pltpu.VMEM((256, 256), bf16),
            pltpu.VMEM((4, 256, 256), f32),
            pltpu.VMEM((128, 128), f32),
            pltpu.VMEM((4, 512, 256), bf16),
            pltpu.VMEM((4, XY - 1, 32, 256), bf16),
            pltpu.VMEM((4, 32, 256), f32),
            pltpu.VMEM((4, 32, 256), bf16),
            pltpu.VMEM((4, NZ - 1, 32, 256), bf16),
            pltpu.VMEM((4, 512, 256), bf16),
            pltpu.VMEM((4, 512, 256), bf16),
            pltpu.VMEM((4, 512, WIDTH), f32),
            pltpu.VMEM((2, 2, 256, 2, WIDTH), bf16),
            dma((4,)), dma((4,)), dma((4,)), dma((4,)), dma((4,)), dma((4,)),
            dma, dma((2,)), dma((4,)), dma((4,)), dma((4,)), dma((4,)),
            dma((4,)), dma((4, 3)), dma, dma((2,)), dma((4,)), dma((2,)),
            pltpu.VMEM((PER_ATOM, 4, PER_ATOM), f32),
            pltpu.VMEM((1, 48), jnp.int32),
            pltpu.VMEM((1, 48), jnp.int32),
            dma((3,)),
            pltpu.VMEM((512, 256), f32),
        ],
        compiler_params=pltpu.CompilerParams(collective_id=0, has_side_effects=True),
    )(
        orbitals, projectors, coupling.transpose(1, 0, 2),
        species.reshape(1, -1), offsets.reshape(1, -1),
    )


def solution(mesh):
    placed = (P("band", None, "ga"), P(None, None, ("ga", "band")), P(), P(), P())
    return jax.shard_map(
        per_device, mesh=mesh, in_specs=placed, out_specs=P("band", None, "ga"), check_vma=False
    )
```

```python
import jax
import jax.numpy as jnp
from jax import lax
from jax.experimental import pallas as pl
from jax.experimental.pallas import tpu as pltpu
from jax.sharding import PartitionSpec as P

NX, NY, NH, NZ, NC = 4, 4, 2, 4, 2
XY = NX * NY
PER_ATOM = 18
FIRST_ATOM = (0, 21, 35, 42)
GROUPS = ((0, 384), (384, 256), (640, 128), (768, 128))
WIDEST = 384
WIDTH = 256
ROWS = 896
COUNTS = (378, 252, 126, 108)
OFFSETS = sorted(
    ((dx, dy) for dx in range(NX) for dy in range(NY)),
    key=lambda at: (min(at[0], NX - at[0]) + min(at[1], NY - at[1]), at),
)
BATCHES = ((0, 5), (5, 11), (11, 16))
HIGHEST = lax.Precision.HIGHEST
NT = (((1,), (1,)), ((), ()))
NN = (((1,), (0,)), ((), ()))


def coupling_matrix(group, cpad, species, offsets):
    n = GROUPS[group][1]
    row = lax.broadcasted_iota(jnp.int32, (n, 1), 0)
    row_atom = (row * 3641) >> 16
    row_in = row - row_atom * PER_ATOM
    start = (row_atom + FIRST_ATOM[group]) * PER_ATOM
    kind = jnp.sum(
        jnp.where(offsets == start, species.astype(jnp.float32), 0.0), axis=1, keepdims=True
    )
    col = lax.broadcasted_iota(jnp.int32, (n, 128), 1)
    col_in, col_kind = col >> 2, col & 3
    pick = jnp.where(
        (col_kind.astype(jnp.float32) == kind) & (col_in == row_in), 1.0, 0.0
    ).astype(jnp.float32)
    rows = lax.dot_general(pick, cpad, NN, precision=HIGHEST, preferred_element_type=jnp.float32)
    wide = lax.broadcasted_iota(jnp.int32, (128, n), 1)
    wide_atom = (wide * 3641) >> 16
    spread = jnp.where(
        wide - wide_atom * PER_ATOM == lax.broadcasted_iota(jnp.int32, (128, n), 0), 1.0, 0.0
    ).astype(jnp.float32)
    full = lax.dot_general(rows, spread, NN, precision=HIGHEST, preferred_element_type=jnp.float32)
    full_row = lax.broadcasted_iota(jnp.int32, (n, n), 0)
    full_col = lax.broadcasted_iota(jnp.int32, (n, n), 1)
    same = ((full_row * 3641) >> 16) == ((full_col * 3641) >> 16)
    return jnp.where(same, full, 0.0)


def turn_matrix():
    row = lax.broadcasted_iota(jnp.int32, (256, 256), 0)
    col = lax.broadcasted_iota(jnp.int32, (256, 256), 1)
    even = (row & 1) == 0
    up = even & (col == row + 1)
    down = jnp.logical_not(even) & (col == row - 1)
    return (jnp.where(up, 1.0, 0.0) - jnp.where(down, 1.0, 0.0)).astype(jnp.bfloat16)


def split_matrix():
    row = lax.broadcasted_iota(jnp.int32, (256, 256), 0)
    col = lax.broadcasted_iota(jnp.int32, (256, 256), 1)
    return jnp.where(col == (row & 127) * 2 + (row >> 7), 1.0, 0.0).astype(jnp.bfloat16)


def kernel(
    orb, proj, coup_hbm, species_hbm, offsets_hbm, out,
    praw, pc, xr, xt, xj, jm, pm, cm, cpad, sb, rb, town, zs, zr, dg, dj, acc, ab,
    pz_s, pz_r, pd_s, pd_r, pf_s, pf_r, o_s, o_r, rs_s, rs_r, z_s, z_r, ag_s, ag_r, b_s, b_r,
    own_s, oo_s,
    coup, species, offsets, small_s, pacc,
):
    ga = lax.axis_index("ga")
    band = lax.axis_index("band")
    zl, core = ga // NC, ga % NC
    x, h, y = band // (NH * NY), band // NY % NH, band % NY
    me = x * NY + y

    def apart(offset, sign):
        dx, dy = offset
        return (x + NX + sign * dx) % NX * (NH * NY) + h * NY + (y + NY + sign * dy) % NY

    def xy_band(k):
        return k // NY * (NH * NY) + h * NY + k % NY

    def copy(src, dst, send, recv, to_ga, to_band):
        return pltpu.make_async_remote_copy(
            src_ref=src, dst_ref=dst, send_sem=send, recv_sem=recv,
            device_id={"ga": to_ga, "band": to_band},
            device_id_type=pl.DeviceIdType.MESH,
        )

    def arrived(ref, sem):
        copy(ref, ref, sem, sem, ga, band).wait_recv()

    def left(ref, sem):
        copy(ref, ref, sem, sem, ga, band).wait_send()

    other_core = zl * NC + 1 - core
    other_half = band + NY - 2 * NY * h

    barrier = pltpu.get_barrier_semaphore()

    def part(k):
        return pl.ds(GROUPS[k][0], COUNTS[k])

    def source(k):
        return proj.at[pl.ds(PER_ATOM * FIRST_ATOM[k], COUNTS[k])]

    def columns(k, q):
        block = k // NY * (NH * NY) + q * NY + k % NY
        return pl.ds(pl.multiple_of(WIDTH * block, WIDTH), WIDTH)

    def greet(to_ga, to_band):
        pl.semaphore_signal(
            barrier, inc=1, device_id={"ga": to_ga, "band": to_band},
            device_id_type=pl.DeviceIdType.MESH,
        )

    greet(ga, other_half)
    for c in range(1, NZ):
        greet((zl + c) % NZ * NC + core, band)
    greet(other_core, band)

    def greet_plane(d, _):
        k = (me + d) % XY
        greet(ga, xy_band(k))
        greet(other_core, xy_band(k))
        return 0

    lax.fori_loop(1, XY, greet_plane, 0)
    own = [pltpu.make_async_copy(source(k), praw.at[0, part(k)], own_s.at[k]) for k in range(4)]
    for k in range(4):
        own[k].start()

    def z_copy(k):
        return copy(source(k), praw.at[1, part(k)], pz_s.at[k], pz_r.at[k], ga, other_half)

    def core_copy(k):
        return copy(source(k), praw.at[2, part(k)], pd_s.at[k], pd_r.at[k], other_core, band)

    def fwd_copy(k):
        return copy(
            praw.at[1, part(k)], praw.at[3, part(k)], pf_s.at[k], pf_r.at[k], other_core, band
        )

    for piece in range(4):
        for k in range(4):
            pad = GROUPS[k][1] - COUNTS[k]
            praw[piece, pl.ds(GROUPS[k][0] + COUNTS[k], pad)] = jnp.zeros(
                (pad, 2, WIDTH), jnp.bfloat16
            )

    pl.semaphore_wait(barrier, 1 + (NZ - 1) + 1 + 2 * (XY - 1))
    for k in range(4):
        z_copy(k).start()

    def orb_copy(k, c, q):
        return copy(
            orb.at[pl.ds(16 * c, 16), :, columns(k, q)],
            xr.at[core, q, pl.ds(16 * me, 16)],
            o_s, o_r.at[core], zl * NC + c, xy_band(k),
        )

    def orb_send(d, _):
        k = (me + d) % XY
        for q in range(NH):
            orb_copy(k, core, q).start()
            orb_copy(k, 1 - core, q).start()
        return 0

    lax.fori_loop(1, XY, orb_send, 0)
    own_orb = []
    for q in range(NH):
        orb_copy(me, 1 - core, q).start()
        own_orb.append(
            pltpu.make_async_copy(
                orb.at[pl.ds(16 * core, 16), :, columns(me, q)],
                xr.at[core, q, pl.ds(16 * me, 16)],
                oo_s.at[q],
            )
        )
        own_orb[q].start()
    for k in range(4):
        core_copy(k).start()
    small = [
        pltpu.make_async_copy(coup_hbm, coup, small_s.at[0]),
        pltpu.make_async_copy(species_hbm, species, small_s.at[1]),
        pltpu.make_async_copy(offsets_hbm, offsets, small_s.at[2]),
    ]
    for one in small:
        one.start()

    jm[...] = turn_matrix()
    pm[...] = split_matrix()
    cpad[...] = jnp.zeros_like(cpad)
    for one in small:
        one.wait()
    for i in range(PER_ATOM):
        cpad[pl.ds(4 * i, 4), pl.ds(0, PER_ATOM)] = coup[i]
    for k in range(4):
        n = GROUPS[k][1]
        cm[k, pl.ds(0, n), pl.ds(0, n)] = coupling_matrix(
            k, cpad[...], species[...], offsets[...]
        )

    for k in range(4):
        own[k].wait()
        core_copy(k).wait_recv()

    def split(k, piece):
        start, n = GROUPS[k]

        def block(i, _):
            at = pl.multiple_of(start + 128 * i, 128)
            both = lax.dot_general(
                pm[...], praw[piece, pl.ds(at, 128)].reshape(256, WIDTH), NN,
                preferred_element_type=jnp.float32,
            ).astype(jnp.bfloat16)
            pc[piece, 0, pl.ds(at, 128), :] = both[:128]
            pc[piece, 1, pl.ds(at, 128), :] = both[128:]
            return 0

        lax.fori_loop(0, n // 128, block, 0)

    for k in range(4):
        split(k, 0)
        split(k, 2)

    for q in range(NH):
        own_orb[q].wait()
    arrived(xr.at[core, :, pl.ds(0, 240)], o_r.at[core])
    arrived(xr.at[1 - core], o_r.at[1 - core])

    def turn(i, _):
        g, q, r = i // 4, i // 2 % 2, i % 2
        rows = pl.ds(pl.multiple_of(256 * r, 256), 256)
        value = xr[g, q, pl.ds(pl.multiple_of(128 * r, 128), 128)].reshape(256, WIDTH)
        xt[g, q, rows, :] = value
        xj[g, q, rows, :] = lax.dot_general(
            jm[...], value, NN, preferred_element_type=jnp.float32
        ).astype(jnp.bfloat16)
        return 0

    lax.fori_loop(0, 8, turn, 0)

    pieces = ((0, core, h), (1, core, 1 - h), (2, 1 - core, h), (3, 1 - core, 1 - h))

    def pieces_product(k, r, chosen):
        start, n = GROUPS[k]
        rows = pl.ds(pl.multiple_of(256 * r, 256), 256)
        total = None
        for i, g, q in chosen:
            re = lax.dot_general(
                xt[g, q, rows, :], pc[i, 0, pl.ds(start, n), :], NT,
                preferred_element_type=jnp.float32,
            )
            im = lax.dot_general(
                xj[g, q, rows, :], pc[i, 1, pl.ds(start, n), :], NT,
                preferred_element_type=jnp.float32,
            )
            total = re + im if total is None else total + re + im
        return rows, total

    def first_early(k):
        n = GROUPS[k][1]

        def block(r, _):
            rows, total = pieces_product(k, r, (pieces[0], pieces[2]))
            pacc[rows, pl.ds(0, n)] = total
            return 0

        lax.fori_loop(0, 2, block, 0)

    def first_product(k):
        n = GROUPS[k][1]

        def block(r, _):
            rows, total = pieces_product(k, r, (pieces[1], pieces[3]))
            sb[k, rows, pl.ds(0, n)] = (total + pacc[rows, pl.ds(0, n)]).astype(jnp.bfloat16)
            return 0

        lax.fori_loop(0, 2, block, 0)

    def rs_send(k):
        n = GROUPS[k][1]

        def one(d, _):
            to = (me + d) % XY
            copy(
                sb.at[k, pl.ds(32 * to, 32), pl.ds(0, n)],
                rb.at[k, XY - 1 - d, :, pl.ds(0, n)],
                rs_s.at[k], rs_r.at[k], ga, xy_band(to),
            ).start()
            return 0

        lax.fori_loop(1, XY, one, 0)

    def z_sum(k):
        n = GROUPS[k][1]
        arrived(rb.at[k, :, :, pl.ds(0, n)], rs_r.at[k])
        total = sb[k, pl.ds(32 * me, 32), pl.ds(0, n)].astype(jnp.float32)
        for d in range(XY - 1):
            total = total + rb[k, d, :, pl.ds(0, n)].astype(jnp.float32)
        town[k, :, pl.ds(0, n)] = total
        zs[k, :, pl.ds(0, n)] = total.astype(jnp.bfloat16)
        for c in range(1, NZ):
            to = (zl + c) % NZ
            copy(
                zs.at[k, :, pl.ds(0, n)], zr.at[k, NZ - 1 - c, :, pl.ds(0, n)],
                z_s.at[k], z_r.at[k], to * NC + core, band,
            ).start()

    def couple(k):
        n = GROUPS[k][1]
        arrived(zr.at[k, :, :, pl.ds(0, n)], z_r.at[k])
        total = town[k, :, pl.ds(0, n)]
        for c in range(NZ - 1):
            total = total + zr[k, c, :, pl.ds(0, n)].astype(jnp.float32)
        coupled = lax.dot_general(
            total, cm[k, pl.ds(0, n), pl.ds(0, n)], NT, precision=HIGHEST,
            preferred_element_type=jnp.float32,
        )
        dg[k, pl.ds(0, 32), pl.ds(0, n)] = coupled.astype(jnp.bfloat16)
        for batch, (first, end) in enumerate(BATCHES):
            for slot in range(max(first, 1), end):
                copy(
                    dg.at[k, pl.ds(0, 32), pl.ds(0, n)],
                    dg.at[k, pl.ds(32 * slot, 32), pl.ds(0, n)],
                    ag_s.at[k], ag_r.at[k, batch], ga, apart(OFFSETS[slot], -1),
                ).start()

    def gather_batch(k, batch):
        first, end = BATCHES[batch]
        first = max(first, 1)
        n = GROUPS[k][1]
        arrived(dg.at[k, pl.ds(32 * first, 32 * (end - first)), pl.ds(0, n)], ag_r.at[k, batch])

    def gather(k):
        n = GROUPS[k][1]
        for batch in range(3):
            gather_batch(k, batch)

        def block(r, _):
            rows = pl.ds(256 * r, 256)
            dj[k, rows, pl.ds(0, n)] = (
                -lax.dot_general(
                    jm[...], dg[k, rows, pl.ds(0, n)], NN, preferred_element_type=jnp.float32
                )
            ).astype(jnp.bfloat16)
            return 0

        lax.fori_loop(0, 2, block, 0)

    def second_piece(i, groups, first):
        def block(r, _):
            rows = pl.ds(pl.multiple_of(256 * r, 256), 256)
            total = None
            for k in groups:
                start, n = GROUPS[k]
                re = lax.dot_general(
                    dg[k, rows, pl.ds(0, n)], pc[i, 0, pl.ds(start, n), :], NN,
                    preferred_element_type=jnp.float32,
                )
                im = lax.dot_general(
                    dj[k, rows, pl.ds(0, n)], pc[i, 1, pl.ds(start, n), :], NN,
                    preferred_element_type=jnp.float32,
                )
                total = re + im if total is None else total + re + im
            if not first:
                total = total + acc[i, rows, :]
            acc[i, rows, :] = total
            return 0

        lax.fori_loop(0, 2, block, 0)

    def second_product(groups, first):
        for i in range(4):
            second_piece(i, groups, first)

    for k in range(4):
        first_early(k)
        z_copy(k).wait_recv()
        fwd_copy(k).start()
        split(k, 1)
        fwd_copy(k).wait_recv()
        split(k, 3)
        first_product(k)
        rs_send(k)
        if k >= 1:
            z_sum(k - 1)
        if k >= 2:
            couple(k - 2)
    couple(2)
    gather(0)
    z_sum(3)
    gather(1)
    second_product((0, 1), True)
    couple(3)
    gather(2)
    second_product((2,), False)

    def back_copy(slot, c, q):
        return copy(
            ab.at[c, q, pl.ds(16 * slot, 16)],
            out.at[pl.ds(16 * core, 16), :, columns(me, q)],
            b_s, b_r.at[core], zl * NC + c, apart(OFFSETS[slot], 1),
        )

    start, n = GROUPS[3]
    for batch, (first, end) in enumerate(BATCHES):
        gather_batch(3, batch)
        rows = pl.ds(32 * first, 32 * (end - first))
        value = dg[3, rows, pl.ds(0, n)].astype(jnp.float32)
        height = value.shape[0]
        even = (lax.broadcasted_iota(jnp.int32, value.shape, 0) & 1) == 0
        turned = jnp.where(
            even, -pltpu.roll(value, height - 1, 0), pltpu.roll(value, 1, 0)
        ).astype(jnp.bfloat16)
        for side, c in ((2, 1 - core), (0, core)):
            for i, g, q in pieces[side : side + 2]:
                re = lax.dot_general(
                    dg[3, rows, pl.ds(0, n)], pc[i, 0, pl.ds(start, n), :], NN,
                    preferred_element_type=jnp.float32,
                )
                im = lax.dot_general(
                    turned, pc[i, 1, pl.ds(start, n), :], NN,
                    preferred_element_type=jnp.float32,
                )
                ab[g, q, pl.ds(16 * first, 16 * (end - first))] = (
                    (re + im + acc[i, rows, :]).astype(jnp.bfloat16).reshape(height // 2, 2, WIDTH)
                )
            for slot in range(first, end):
                for q in range(NH):
                    if slot > 0 or side == 2:
                        back_copy(slot, c, q).start()
    for q in range(NH):
        out[pl.ds(16 * core, 16), :, columns(me, q)] = ab[core, q, pl.ds(0, 16)]

    for k in range(4):
        n = GROUPS[k][1]
        z_copy(k).wait_send()
        core_copy(k).wait_send()
        fwd_copy(k).wait_send()
        left(rb.at[k, :, :, pl.ds(0, n)], rs_s.at[k])
        left(zr.at[k, :, :, pl.ds(0, n)], z_s.at[k])
        left(dg.at[k, pl.ds(0, 480), pl.ds(0, n)], ag_s.at[k])
    left(xr.at[0], o_s)
    left(xr.at[0, :, pl.ds(0, 240)], o_s)
    left(ab.at[0], b_s)
    left(ab.at[0, :, pl.ds(0, 240)], b_s)
    arrived(ab.at[core, :, pl.ds(0, 240)], b_r.at[core])
    arrived(ab.at[1 - core], b_r.at[1 - core])


def per_device(orbitals, projectors, coupling, species, offsets):
    bf16, f32 = jnp.bfloat16, jnp.float32
    vmem = pl.BlockSpec(memory_space=pltpu.VMEM)
    hbm = pl.BlockSpec(memory_space=pltpu.HBM)
    dma = pltpu.SemaphoreType.DMA
    return pl.pallas_call(
        kernel,
        out_shape=pltpu.VMEM(orbitals.shape, bf16),
        in_specs=[hbm] * 5,
        out_specs=vmem,
        scratch_shapes=[
            pltpu.VMEM((4, ROWS, 2, WIDTH), bf16),
            pltpu.VMEM((4, 2, ROWS, WIDTH), bf16),
            pltpu.VMEM((2, 2, 256, 2, WIDTH), bf16),
            pltpu.VMEM((2, 2, 512, WIDTH), bf16),
            pltpu.VMEM((2, 2, 512, WIDTH), bf16),
            pltpu.VMEM((256, 256), bf16),
            pltpu.VMEM((256, 256), bf16),
            pltpu.VMEM((4, WIDEST, WIDEST), f32),
            pltpu.VMEM((128, 128), f32),
            pltpu.VMEM((4, 512, WIDEST), bf16),
            pltpu.VMEM((4, XY - 1, 32, WIDEST), bf16),
            pltpu.VMEM((4, 32, WIDEST), f32),
            pltpu.VMEM((4, 32, WIDEST), bf16),
            pltpu.VMEM((4, NZ - 1, 32, WIDEST), bf16),
            pltpu.VMEM((4, 512, WIDEST), bf16),
            pltpu.VMEM((4, 512, WIDEST), bf16),
            pltpu.VMEM((4, 512, WIDTH), f32),
            pltpu.VMEM((2, 2, 256, 2, WIDTH), bf16),
            dma((4,)), dma((4,)), dma((4,)), dma((4,)), dma((4,)), dma((4,)),
            dma, dma((2,)), dma((4,)), dma((4,)), dma((4,)), dma((4,)),
            dma((4,)), dma((4, 3)), dma, dma((2,)), dma((4,)), dma((2,)),
            pltpu.VMEM((PER_ATOM, 4, PER_ATOM), f32),
            pltpu.VMEM((1, 48), jnp.int32),
            pltpu.VMEM((1, 48), jnp.int32),
            dma((3,)),
            pltpu.VMEM((512, WIDEST), f32),
        ],
        compiler_params=pltpu.CompilerParams(collective_id=0, has_side_effects=True),
    )(
        orbitals, projectors, coupling.transpose(1, 0, 2),
        species.reshape(1, -1), offsets.reshape(1, -1),
    )


def solution(mesh):
    placed = (P("band", None, "ga"), P(None, None, ("ga", "band")), P(), P(), P())
    return jax.shard_map(
        per_device, mesh=mesh, in_specs=placed, out_specs=P("band", None, "ga"), check_vma=False
    )
```

```python
import jax
import jax.numpy as jnp
from jax import lax
from jax.experimental import pallas as pl
from jax.experimental.pallas import tpu as pltpu
from jax.sharding import PartitionSpec as P

NX, NY, NH, NZ, NC = 4, 4, 2, 4, 2
XY = NX * NY
PER_ATOM = 18
GROUP_ATOMS = 14
GROUPS = ((0, 256), (256, 256), (512, 256), (768, 128))
WIDTH = 256
ROWS = 896
COUNTS = (252, 252, 252, 108)
OFFSETS = sorted(
    ((dx, dy) for dx in range(NX) for dy in range(NY)),
    key=lambda at: (min(at[0], NX - at[0]) + min(at[1], NY - at[1]), at),
)
BATCHES = ((0, 5), (5, 11), (11, 16))
HIGHEST = lax.Precision.HIGHEST
NT = (((1,), (1,)), ((), ()))
NN = (((1,), (0,)), ((), ()))


def coupling_matrix(group, cpad, species, offsets):
    row = lax.broadcasted_iota(jnp.int32, (256, 1), 0)
    row_atom = (row * 3641) >> 16
    row_in = row - row_atom * PER_ATOM
    start = (row_atom + GROUP_ATOMS * group) * PER_ATOM
    kind = jnp.sum(
        jnp.where(offsets == start, species.astype(jnp.float32), 0.0), axis=1, keepdims=True
    )
    col = lax.broadcasted_iota(jnp.int32, (256, 128), 1)
    col_in, col_kind = col >> 2, col & 3
    pick = jnp.where(
        (col_kind.astype(jnp.float32) == kind) & (col_in == row_in), 1.0, 0.0
    ).astype(jnp.float32)
    rows = lax.dot_general(pick, cpad, NN, precision=HIGHEST, preferred_element_type=jnp.float32)
    wide = lax.broadcasted_iota(jnp.int32, (128, 256), 1)
    wide_atom = (wide * 3641) >> 16
    spread = jnp.where(
        wide - wide_atom * PER_ATOM == lax.broadcasted_iota(jnp.int32, (128, 256), 0), 1.0, 0.0
    ).astype(jnp.float32)
    full = lax.dot_general(rows, spread, NN, precision=HIGHEST, preferred_element_type=jnp.float32)
    full_row = lax.broadcasted_iota(jnp.int32, (256, 256), 0)
    full_col = lax.broadcasted_iota(jnp.int32, (256, 256), 1)
    same = ((full_row * 3641) >> 16) == ((full_col * 3641) >> 16)
    return jnp.where(same, full, 0.0)


def turn_matrix():
    row = lax.broadcasted_iota(jnp.int32, (256, 256), 0)
    col = lax.broadcasted_iota(jnp.int32, (256, 256), 1)
    even = (row & 1) == 0
    up = even & (col == row + 1)
    down = jnp.logical_not(even) & (col == row - 1)
    return (jnp.where(up, 1.0, 0.0) - jnp.where(down, 1.0, 0.0)).astype(jnp.bfloat16)


def split_matrix():
    row = lax.broadcasted_iota(jnp.int32, (256, 256), 0)
    col = lax.broadcasted_iota(jnp.int32, (256, 256), 1)
    return jnp.where(col == (row & 127) * 2 + (row >> 7), 1.0, 0.0).astype(jnp.bfloat16)


def kernel(
    orb, proj, coup_hbm, species_hbm, offsets_hbm, out,
    praw, pc, xr, xt, xj, jm, pm, cm, cpad, sb, rb, town, zs, zr, dg, dj, acc, ab,
    pz_s, pz_r, pd_s, pd_r, pf_s, pf_r, o_s, o_r, rs_s, rs_r, z_s, z_r, ag_s, ag_r, b_s, b_r,
    own_s, oo_s,
    coup, species, offsets, small_s, pacc,
):
    ga = lax.axis_index("ga")
    band = lax.axis_index("band")
    zl, core = ga // NC, ga % NC
    x, h, y = band // (NH * NY), band // NY % NH, band % NY
    me = x * NY + y

    def apart(offset, sign):
        dx, dy = offset
        return (x + NX + sign * dx) % NX * (NH * NY) + h * NY + (y + NY + sign * dy) % NY

    def xy_band(k):
        return k // NY * (NH * NY) + h * NY + k % NY

    def copy(src, dst, send, recv, to_ga, to_band):
        return pltpu.make_async_remote_copy(
            src_ref=src, dst_ref=dst, send_sem=send, recv_sem=recv,
            device_id={"ga": to_ga, "band": to_band},
            device_id_type=pl.DeviceIdType.MESH,
        )

    def arrived(ref, sem):
        copy(ref, ref, sem, sem, ga, band).wait_recv()

    def left(ref, sem):
        copy(ref, ref, sem, sem, ga, band).wait_send()

    other_core = zl * NC + 1 - core
    other_half = band + NY - 2 * NY * h

    barrier = pltpu.get_barrier_semaphore()

    def part(k):
        return pl.ds(GROUPS[k][0], COUNTS[k])

    def source(k):
        return proj.at[pl.ds(GROUP_ATOMS * PER_ATOM * k, COUNTS[k])]

    def columns(k, q):
        block = k // NY * (NH * NY) + q * NY + k % NY
        return pl.ds(pl.multiple_of(WIDTH * block, WIDTH), WIDTH)

    def greet(to_ga, to_band):
        pl.semaphore_signal(
            barrier, inc=1, device_id={"ga": to_ga, "band": to_band},
            device_id_type=pl.DeviceIdType.MESH,
        )

    greet(ga, other_half)
    for c in range(1, NZ):
        greet((zl + c) % NZ * NC + core, band)
    greet(other_core, band)

    def greet_plane(d, _):
        k = (me + d) % XY
        greet(ga, xy_band(k))
        greet(other_core, xy_band(k))
        return 0

    lax.fori_loop(1, XY, greet_plane, 0)
    own = [pltpu.make_async_copy(source(k), praw.at[0, part(k)], own_s.at[k]) for k in range(4)]
    for k in range(4):
        own[k].start()

    def z_copy(k):
        return copy(source(k), praw.at[1, part(k)], pz_s.at[k], pz_r.at[k], ga, other_half)

    def core_copy(k):
        return copy(source(k), praw.at[2, part(k)], pd_s.at[k], pd_r.at[k], other_core, band)

    def fwd_copy(k):
        return copy(
            praw.at[1, part(k)], praw.at[3, part(k)], pf_s.at[k], pf_r.at[k], other_core, band
        )

    for piece in range(4):
        for k in range(4):
            pad = GROUPS[k][1] - COUNTS[k]
            praw[piece, pl.ds(GROUPS[k][0] + COUNTS[k], pad)] = jnp.zeros(
                (pad, 2, WIDTH), jnp.bfloat16
            )

    pl.semaphore_wait(barrier, 1 + (NZ - 1) + 1 + 2 * (XY - 1))
    for k in range(4):
        z_copy(k).start()

    def orb_copy(k, c, q):
        return copy(
            orb.at[pl.ds(16 * c, 16), :, columns(k, q)],
            xr.at[core, q, pl.ds(16 * me, 16)],
            o_s, o_r.at[core], zl * NC + c, xy_band(k),
        )

    def orb_send(d, _):
        k = (me + d) % XY
        for q in range(NH):
            orb_copy(k, core, q).start()
            orb_copy(k, 1 - core, q).start()
        return 0

    lax.fori_loop(1, XY, orb_send, 0)
    own_orb = []
    for q in range(NH):
        orb_copy(me, 1 - core, q).start()
        own_orb.append(
            pltpu.make_async_copy(
                orb.at[pl.ds(16 * core, 16), :, columns(me, q)],
                xr.at[core, q, pl.ds(16 * me, 16)],
                oo_s.at[q],
            )
        )
        own_orb[q].start()
    for k in range(4):
        core_copy(k).start()
    small = [
        pltpu.make_async_copy(coup_hbm, coup, small_s.at[0]),
        pltpu.make_async_copy(species_hbm, species, small_s.at[1]),
        pltpu.make_async_copy(offsets_hbm, offsets, small_s.at[2]),
    ]
    for one in small:
        one.start()

    jm[...] = turn_matrix()
    pm[...] = split_matrix()
    cpad[...] = jnp.zeros_like(cpad)
    for one in small:
        one.wait()
    for i in range(PER_ATOM):
        cpad[pl.ds(4 * i, 4), pl.ds(0, PER_ATOM)] = coup[i]
    for k in range(4):
        cm[k] = coupling_matrix(k, cpad[...], species[...], offsets[...])

    for k in range(4):
        own[k].wait()
        core_copy(k).wait_recv()

    def split(k, piece):
        start, n = GROUPS[k]

        def block(i, _):
            at = pl.multiple_of(start + 128 * i, 128)
            both = lax.dot_general(
                pm[...], praw[piece, pl.ds(at, 128)].reshape(256, WIDTH), NN,
                preferred_element_type=jnp.float32,
            ).astype(jnp.bfloat16)
            pc[piece, 0, pl.ds(at, 128), :] = both[:128]
            pc[piece, 1, pl.ds(at, 128), :] = both[128:]
            return 0

        lax.fori_loop(0, n // 128, block, 0)

    for k in range(4):
        split(k, 0)
        split(k, 2)

    for q in range(NH):
        own_orb[q].wait()
    arrived(xr.at[core, :, pl.ds(0, 240)], o_r.at[core])
    arrived(xr.at[1 - core], o_r.at[1 - core])

    def turn(i, _):
        g, q, r = i // 4, i // 2 % 2, i % 2
        rows = pl.ds(pl.multiple_of(256 * r, 256), 256)
        value = xr[g, q, pl.ds(pl.multiple_of(128 * r, 128), 128)].reshape(256, WIDTH)
        xt[g, q, rows, :] = value
        xj[g, q, rows, :] = lax.dot_general(
            jm[...], value, NN, preferred_element_type=jnp.float32
        ).astype(jnp.bfloat16)
        return 0

    lax.fori_loop(0, 8, turn, 0)

    pieces = ((0, core, h), (1, core, 1 - h), (2, 1 - core, h), (3, 1 - core, 1 - h))

    def pieces_product(k, r, chosen):
        start, n = GROUPS[k]
        rows = pl.ds(pl.multiple_of(256 * r, 256), 256)
        total = None
        for i, g, q in chosen:
            re = lax.dot_general(
                xt[g, q, rows, :], pc[i, 0, pl.ds(start, n), :], NT,
                preferred_element_type=jnp.float32,
            )
            im = lax.dot_general(
                xj[g, q, rows, :], pc[i, 1, pl.ds(start, n), :], NT,
                preferred_element_type=jnp.float32,
            )
            total = re + im if total is None else total + re + im
        return rows, total

    def first_early(k):
        n = GROUPS[k][1]

        def block(r, _):
            rows, total = pieces_product(k, r, (pieces[0], pieces[2]))
            pacc[rows, pl.ds(0, n)] = total
            return 0

        lax.fori_loop(0, 2, block, 0)

    def first_product(k):
        n = GROUPS[k][1]

        def block(r, _):
            rows, total = pieces_product(k, r, (pieces[1], pieces[3]))
            sb[k, rows, pl.ds(0, n)] = (total + pacc[rows, pl.ds(0, n)]).astype(jnp.bfloat16)
            return 0

        lax.fori_loop(0, 2, block, 0)

    def rs_send(k):
        n = GROUPS[k][1]

        def one(d, _):
            to = (me + d) % XY
            copy(
                sb.at[k, pl.ds(32 * to, 32), pl.ds(0, n)],
                rb.at[k, XY - 1 - d, :, pl.ds(0, n)],
                rs_s.at[k], rs_r.at[k], ga, xy_band(to),
            ).start()
            return 0

        lax.fori_loop(1, XY, one, 0)

    def z_sum(k):
        n = GROUPS[k][1]
        arrived(rb.at[k, :, :, pl.ds(0, n)], rs_r.at[k])
        total = sb[k, pl.ds(32 * me, 32), pl.ds(0, n)].astype(jnp.float32)
        for d in range(XY - 1):
            total = total + rb[k, d, :, pl.ds(0, n)].astype(jnp.float32)
        town[k, :, pl.ds(0, n)] = total
        zs[k, :, pl.ds(0, n)] = total.astype(jnp.bfloat16)
        for c in range(1, NZ):
            to = (zl + c) % NZ
            copy(
                zs.at[k, :, pl.ds(0, n)], zr.at[k, NZ - 1 - c, :, pl.ds(0, n)],
                z_s.at[k], z_r.at[k], to * NC + core, band,
            ).start()

    def couple(k):
        n = GROUPS[k][1]
        arrived(zr.at[k, :, :, pl.ds(0, n)], z_r.at[k])
        total = town[k, :, pl.ds(0, n)]
        for c in range(NZ - 1):
            total = total + zr[k, c, :, pl.ds(0, n)].astype(jnp.float32)
        coupled = lax.dot_general(
            total, cm[k, pl.ds(0, n), pl.ds(0, n)], NT, precision=HIGHEST,
            preferred_element_type=jnp.float32,
        )
        dg[k, pl.ds(0, 32), pl.ds(0, n)] = coupled.astype(jnp.bfloat16)
        for batch, (first, end) in enumerate(BATCHES):
            for slot in range(max(first, 1), end):
                copy(
                    dg.at[k, pl.ds(0, 32), pl.ds(0, n)],
                    dg.at[k, pl.ds(32 * slot, 32), pl.ds(0, n)],
                    ag_s.at[k], ag_r.at[k, batch], ga, apart(OFFSETS[slot], -1),
                ).start()

    def gather_batch(k, batch):
        first, end = BATCHES[batch]
        first = max(first, 1)
        n = GROUPS[k][1]
        arrived(dg.at[k, pl.ds(32 * first, 32 * (end - first)), pl.ds(0, n)], ag_r.at[k, batch])

    def gather(k):
        n = GROUPS[k][1]
        for batch in range(3):
            gather_batch(k, batch)

        def block(r, _):
            rows = pl.ds(256 * r, 256)
            dj[k, rows, pl.ds(0, n)] = (
                -lax.dot_general(
                    jm[...], dg[k, rows, pl.ds(0, n)], NN, preferred_element_type=jnp.float32
                )
            ).astype(jnp.bfloat16)
            return 0

        lax.fori_loop(0, 2, block, 0)

    def second_piece(i, groups, first):
        def block(r, _):
            rows = pl.ds(pl.multiple_of(256 * r, 256), 256)
            total = None
            for k in groups:
                start, n = GROUPS[k]
                re = lax.dot_general(
                    dg[k, rows, pl.ds(0, n)], pc[i, 0, pl.ds(start, n), :], NN,
                    preferred_element_type=jnp.float32,
                )
                im = lax.dot_general(
                    dj[k, rows, pl.ds(0, n)], pc[i, 1, pl.ds(start, n), :], NN,
                    preferred_element_type=jnp.float32,
                )
                total = re + im if total is None else total + re + im
            if not first:
                total = total + acc[i, rows, :]
            acc[i, rows, :] = total
            return 0

        lax.fori_loop(0, 2, block, 0)

    def second_product(groups, first):
        for i in range(4):
            second_piece(i, groups, first)

    for k in range(4):
        first_early(k)
        z_copy(k).wait_recv()
        fwd_copy(k).start()
        split(k, 1)
        fwd_copy(k).wait_recv()
        split(k, 3)
        first_product(k)
        rs_send(k)
        if k in (1, 2):
            couple(k - 1)
        if k in (0, 1):
            z_sum(k)
        if k == 2:
            gather(0)
    second_product((0,), True)
    z_sum(2)
    gather(1)
    second_product((1,), False)
    z_sum(3)
    couple(2)
    couple(3)
    gather(2)
    second_product((2,), False)

    def back_copy(slot, c, q):
        return copy(
            ab.at[c, q, pl.ds(16 * slot, 16)],
            out.at[pl.ds(16 * core, 16), :, columns(me, q)],
            b_s, b_r.at[core], zl * NC + c, apart(OFFSETS[slot], 1),
        )

    start, n = GROUPS[3]
    for batch, (first, end) in enumerate(BATCHES):
        gather_batch(3, batch)
        rows = pl.ds(32 * first, 32 * (end - first))
        value = dg[3, rows, pl.ds(0, n)].astype(jnp.float32)
        height = value.shape[0]
        even = (lax.broadcasted_iota(jnp.int32, value.shape, 0) & 1) == 0
        turned = jnp.where(
            even, -pltpu.roll(value, height - 1, 0), pltpu.roll(value, 1, 0)
        ).astype(jnp.bfloat16)
        for side, c in ((2, 1 - core), (0, core)):
            for i, g, q in pieces[side : side + 2]:
                re = lax.dot_general(
                    dg[3, rows, pl.ds(0, n)], pc[i, 0, pl.ds(start, n), :], NN,
                    preferred_element_type=jnp.float32,
                )
                im = lax.dot_general(
                    turned, pc[i, 1, pl.ds(start, n), :], NN,
                    preferred_element_type=jnp.float32,
                )
                ab[g, q, pl.ds(16 * first, 16 * (end - first))] = (
                    (re + im + acc[i, rows, :]).astype(jnp.bfloat16).reshape(height // 2, 2, WIDTH)
                )
            for slot in range(first, end):
                for q in range(NH):
                    if slot > 0 or side == 2:
                        back_copy(slot, c, q).start()
    for q in range(NH):
        out[pl.ds(16 * core, 16), :, columns(me, q)] = ab[core, q, pl.ds(0, 16)]

    for k in range(4):
        n = GROUPS[k][1]
        z_copy(k).wait_send()
        core_copy(k).wait_send()
        fwd_copy(k).wait_send()
        left(rb.at[k, :, :, pl.ds(0, n)], rs_s.at[k])
        left(zr.at[k, :, :, pl.ds(0, n)], z_s.at[k])
        left(dg.at[k, pl.ds(0, 480), pl.ds(0, n)], ag_s.at[k])
    left(xr.at[0], o_s)
    left(xr.at[0, :, pl.ds(0, 240)], o_s)
    left(ab.at[0], b_s)
    left(ab.at[0, :, pl.ds(0, 240)], b_s)
    arrived(ab.at[core, :, pl.ds(0, 240)], b_r.at[core])
    arrived(ab.at[1 - core], b_r.at[1 - core])


def per_device(orbitals, projectors, coupling, species, offsets):
    bf16, f32 = jnp.bfloat16, jnp.float32
    vmem = pl.BlockSpec(memory_space=pltpu.VMEM)
    hbm = pl.BlockSpec(memory_space=pltpu.HBM)
    dma = pltpu.SemaphoreType.DMA
    return pl.pallas_call(
        kernel,
        out_shape=pltpu.VMEM(orbitals.shape, bf16),
        in_specs=[hbm] * 5,
        out_specs=vmem,
        scratch_shapes=[
            pltpu.VMEM((4, ROWS, 2, WIDTH), bf16),
            pltpu.VMEM((4, 2, ROWS, WIDTH), bf16),
            pltpu.VMEM((2, 2, 256, 2, WIDTH), bf16),
            pltpu.VMEM((2, 2, 512, WIDTH), bf16),
            pltpu.VMEM((2, 2, 512, WIDTH), bf16),
            pltpu.VMEM((256, 256), bf16),
            pltpu.VMEM((256, 256), bf16),
            pltpu.VMEM((4, 256, 256), f32),
            pltpu.VMEM((128, 128), f32),
            pltpu.VMEM((4, 512, 256), bf16),
            pltpu.VMEM((4, XY - 1, 32, 256), bf16),
            pltpu.VMEM((4, 32, 256), f32),
            pltpu.VMEM((4, 32, 256), bf16),
            pltpu.VMEM((4, NZ - 1, 32, 256), bf16),
            pltpu.VMEM((4, 512, 256), bf16),
            pltpu.VMEM((4, 512, 256), bf16),
            pltpu.VMEM((4, 512, WIDTH), f32),
            pltpu.VMEM((2, 2, 256, 2, WIDTH), bf16),
            dma((4,)), dma((4,)), dma((4,)), dma((4,)), dma((4,)), dma((4,)),
            dma, dma((2,)), dma((4,)), dma((4,)), dma((4,)), dma((4,)),
            dma((4,)), dma((4, 3)), dma, dma((2,)), dma((4,)), dma((2,)),
            pltpu.VMEM((PER_ATOM, 4, PER_ATOM), f32),
            pltpu.VMEM((1, 48), jnp.int32),
            pltpu.VMEM((1, 48), jnp.int32),
            dma((3,)),
            pltpu.VMEM((512, 256), f32),
        ],
        compiler_params=pltpu.CompilerParams(collective_id=0, has_side_effects=True),
    )(
        orbitals, projectors, coupling.transpose(1, 0, 2),
        species.reshape(1, -1), offsets.reshape(1, -1),
    )


def solution(mesh):
    placed = (P("band", None, "ga"), P(None, None, ("ga", "band")), P(), P(), P())
    return jax.shard_map(
        per_device, mesh=mesh, in_specs=placed, out_specs=P("band", None, "ga"), check_vma=False
    )
```

```python
import jax
import jax.numpy as jnp
from jax import lax
from jax.experimental import pallas as pl
from jax.experimental.pallas import tpu as pltpu
from jax.sharding import PartitionSpec as P

NX, NY, NH, NZ, NC = 4, 4, 2, 4, 2
XY = NX * NY
PER_ATOM = 18
GROUP_ATOMS = 14
GROUPS = ((0, 256), (256, 256), (512, 256), (768, 128))
WIDTH = 256
LEVELS = 4
ROWS = 896
COUNTS = (252, 252, 252, 108)
OFFSETS = sorted(
    ((dx, dy) for dx in range(NX) for dy in range(NY)),
    key=lambda at: (min(at[0], NX - at[0]) + min(at[1], NY - at[1]), at),
)
BATCHES = ((0, 5), (5, 11), (11, 16))
HIGHEST = lax.Precision.HIGHEST
NT = (((1,), (1,)), ((), ()))
NN = (((1,), (0,)), ((), ()))


def coupling_matrix(group, cpad, species, offsets):
    row = lax.broadcasted_iota(jnp.int32, (256, 1), 0)
    row_atom = (row * 3641) >> 16
    row_in = row - row_atom * PER_ATOM
    start = (row_atom + GROUP_ATOMS * group) * PER_ATOM
    kind = jnp.sum(
        jnp.where(offsets == start, species.astype(jnp.float32), 0.0), axis=1, keepdims=True
    )
    col = lax.broadcasted_iota(jnp.int32, (256, 128), 1)
    col_in, col_kind = col >> 2, col & 3
    pick = jnp.where(
        (col_kind.astype(jnp.float32) == kind) & (col_in == row_in), 1.0, 0.0
    ).astype(jnp.float32)
    rows = lax.dot_general(pick, cpad, NN, precision=HIGHEST, preferred_element_type=jnp.float32)
    wide = lax.broadcasted_iota(jnp.int32, (128, 256), 1)
    wide_atom = (wide * 3641) >> 16
    spread = jnp.where(
        wide - wide_atom * PER_ATOM == lax.broadcasted_iota(jnp.int32, (128, 256), 0), 1.0, 0.0
    ).astype(jnp.float32)
    full = lax.dot_general(rows, spread, NN, precision=HIGHEST, preferred_element_type=jnp.float32)
    full_row = lax.broadcasted_iota(jnp.int32, (256, 256), 0)
    full_col = lax.broadcasted_iota(jnp.int32, (256, 256), 1)
    same = ((full_row * 3641) >> 16) == ((full_col * 3641) >> 16)
    return jnp.where(same, full, 0.0)


def turn_matrix():
    row = lax.broadcasted_iota(jnp.int32, (256, 256), 0)
    col = lax.broadcasted_iota(jnp.int32, (256, 256), 1)
    even = (row & 1) == 0
    up = even & (col == row + 1)
    down = jnp.logical_not(even) & (col == row - 1)
    return (jnp.where(up, 1.0, 0.0) - jnp.where(down, 1.0, 0.0)).astype(jnp.bfloat16)


def split_matrix():
    row = lax.broadcasted_iota(jnp.int32, (256, 256), 0)
    col = lax.broadcasted_iota(jnp.int32, (256, 256), 1)
    return jnp.where(col == (row & 127) * 2 + (row >> 7), 1.0, 0.0).astype(jnp.bfloat16)


def kernel(
    orb, proj, coup_hbm, species_hbm, offsets_hbm, out,
    praw, pc, xr, xt, xj, jm, pm, cm, cpad, sb, rb, town, zs, zr, dg, dj, acc, ab,
    pz_s, pz_r, pd_s, pd_r, pf_s, pf_r, o_s, o_r, rs_s, rs_r, z_s, z_r, ag_s, ag_r, b_s, b_r,
    own_s, oo_s,
    coup, species, offsets, small_s, pacc, level_s,
):
    ga = lax.axis_index("ga")
    band = lax.axis_index("band")
    zl, core = ga // NC, ga % NC
    x, h, y = band // (NH * NY), band // NY % NH, band % NY
    me = x * NY + y

    def apart(offset, sign):
        dx, dy = offset
        return (x + NX + sign * dx) % NX * (NH * NY) + h * NY + (y + NY + sign * dy) % NY

    def xy_band(k):
        return k // NY * (NH * NY) + h * NY + k % NY

    def copy(src, dst, send, recv, to_ga, to_band):
        return pltpu.make_async_remote_copy(
            src_ref=src, dst_ref=dst, send_sem=send, recv_sem=recv,
            device_id={"ga": to_ga, "band": to_band},
            device_id_type=pl.DeviceIdType.MESH,
        )

    def arrived(ref, sem):
        copy(ref, ref, sem, sem, ga, band).wait_recv()

    def left(ref, sem):
        copy(ref, ref, sem, sem, ga, band).wait_send()

    other_core = zl * NC + 1 - core
    other_half = band + NY - 2 * NY * h

    barrier = pltpu.get_barrier_semaphore()

    def part(k):
        return pl.ds(GROUPS[k][0], COUNTS[k])

    def source(k):
        return proj.at[pl.ds(GROUP_ATOMS * PER_ATOM * k, COUNTS[k])]

    def columns(k, q):
        block = k // NY * (NH * NY) + q * NY + k % NY
        return pl.ds(pl.multiple_of(WIDTH * block, WIDTH), WIDTH)

    def greet(sem, to_ga, to_band):
        pl.semaphore_signal(
            sem, inc=1, device_id={"ga": to_ga, "band": to_band},
            device_id_type=pl.DeviceIdType.MESH,
        )

    def greet_near(sem):
        for offset in ((1, 0), (NX - 1, 0), (0, 1), (0, NY - 1)):
            greet(sem, ga, apart(offset, 1))
        greet(sem, other_core, band)

        @pl.when(zl > 0)
        def _():
            greet(sem, ga - NC, band)

        @pl.when(zl < NZ - 1)
        def _():
            greet(sem, ga + NC, band)

    near = 5 + (zl + NZ - 1) // NZ + (2 * (NZ - 1) - 1 - zl) // (NZ - 1)
    greet(barrier, ga, other_half)
    greet_near(barrier)

    own = [pltpu.make_async_copy(source(k), praw.at[0, part(k)], own_s.at[k]) for k in range(4)]
    for k in range(4):
        own[k].start()

    def z_copy(k):
        return copy(source(k), praw.at[1, part(k)], pz_s.at[k], pz_r.at[k], ga, other_half)

    def core_copy(k):
        return copy(source(k), praw.at[2, part(k)], pd_s.at[k], pd_r.at[k], other_core, band)

    def fwd_copy(k):
        return copy(
            praw.at[1, part(k)], praw.at[3, part(k)], pf_s.at[k], pf_r.at[k], other_core, band
        )

    for piece in range(4):
        for k in range(4):
            pad = GROUPS[k][1] - COUNTS[k]
            praw[piece, pl.ds(GROUPS[k][0] + COUNTS[k], pad)] = jnp.zeros(
                (pad, 2, WIDTH), jnp.bfloat16
            )

    pl.semaphore_wait(barrier, near + 1)
    for k in range(4):
        z_copy(k).start()
    for k in range(4):
        core_copy(k).start()
    for level in range(LEVELS):
        greet_near(level_s.at[level])
        pl.semaphore_wait(level_s.at[level], near)

    def orb_copy(k, c, q):
        return copy(
            orb.at[pl.ds(16 * c, 16), :, columns(k, q)],
            xr.at[core, q, pl.ds(16 * me, 16)],
            o_s, o_r.at[core], zl * NC + c, xy_band(k),
        )

    def orb_send(d, _):
        k = (me + d) % XY
        for q in range(NH):
            orb_copy(k, core, q).start()
            orb_copy(k, 1 - core, q).start()
        return 0

    lax.fori_loop(1, XY, orb_send, 0)
    own_orb = []
    for q in range(NH):
        orb_copy(me, 1 - core, q).start()
        own_orb.append(
            pltpu.make_async_copy(
                orb.at[pl.ds(16 * core, 16), :, columns(me, q)],
                xr.at[core, q, pl.ds(16 * me, 16)],
                oo_s.at[q],
            )
        )
        own_orb[q].start()
    small = [
        pltpu.make_async_copy(coup_hbm, coup, small_s.at[0]),
        pltpu.make_async_copy(species_hbm, species, small_s.at[1]),
        pltpu.make_async_copy(offsets_hbm, offsets, small_s.at[2]),
    ]
    for one in small:
        one.start()

    jm[...] = turn_matrix()
    pm[...] = split_matrix()
    cpad[...] = jnp.zeros_like(cpad)
    for one in small:
        one.wait()
    for i in range(PER_ATOM):
        cpad[pl.ds(4 * i, 4), pl.ds(0, PER_ATOM)] = coup[i]
    for k in range(4):
        cm[k] = coupling_matrix(k, cpad[...], species[...], offsets[...])

    for k in range(4):
        own[k].wait()
        core_copy(k).wait_recv()

    def split(k, piece):
        start, n = GROUPS[k]

        def block(i, _):
            at = pl.multiple_of(start + 128 * i, 128)
            both = lax.dot_general(
                pm[...], praw[piece, pl.ds(at, 128)].reshape(256, WIDTH), NN,
                preferred_element_type=jnp.float32,
            ).astype(jnp.bfloat16)
            pc[piece, 0, pl.ds(at, 128), :] = both[:128]
            pc[piece, 1, pl.ds(at, 128), :] = both[128:]
            return 0

        lax.fori_loop(0, n // 128, block, 0)

    for k in range(4):
        split(k, 0)
        split(k, 2)

    for q in range(NH):
        own_orb[q].wait()
    arrived(xr.at[core, :, pl.ds(0, 240)], o_r.at[core])
    arrived(xr.at[1 - core], o_r.at[1 - core])

    def turn(i, _):
        g, q, r = i // 4, i // 2 % 2, i % 2
        rows = pl.ds(pl.multiple_of(256 * r, 256), 256)
        value = xr[g, q, pl.ds(pl.multiple_of(128 * r, 128), 128)].reshape(256, WIDTH)
        xt[g, q, rows, :] = value
        xj[g, q, rows, :] = lax.dot_general(
            jm[...], value, NN, preferred_element_type=jnp.float32
        ).astype(jnp.bfloat16)
        return 0

    lax.fori_loop(0, 8, turn, 0)

    pieces = ((0, core, h), (1, core, 1 - h), (2, 1 - core, h), (3, 1 - core, 1 - h))

    def pieces_product(k, r, chosen):
        start, n = GROUPS[k]
        rows = pl.ds(pl.multiple_of(256 * r, 256), 256)
        total = None
        for i, g, q in chosen:
            re = lax.dot_general(
                xt[g, q, rows, :], pc[i, 0, pl.ds(start, n), :], NT,
                preferred_element_type=jnp.float32,
            )
            im = lax.dot_general(
                xj[g, q, rows, :], pc[i, 1, pl.ds(start, n), :], NT,
                preferred_element_type=jnp.float32,
            )
            total = re + im if total is None else total + re + im
        return rows, total

    def first_early(k):
        n = GROUPS[k][1]

        def block(r, _):
            rows, total = pieces_product(k, r, (pieces[0], pieces[2]))
            pacc[rows, pl.ds(0, n)] = total
            return 0

        lax.fori_loop(0, 2, block, 0)

    def first_product(k):
        n = GROUPS[k][1]

        def block(r, _):
            rows, total = pieces_product(k, r, (pieces[1], pieces[3]))
            sb[k, rows, pl.ds(0, n)] = (total + pacc[rows, pl.ds(0, n)]).astype(jnp.bfloat16)
            return 0

        lax.fori_loop(0, 2, block, 0)

    def rs_send(k):
        n = GROUPS[k][1]

        def one(d, _):
            to = (me + d) % XY
            copy(
                sb.at[k, pl.ds(32 * to, 32), pl.ds(0, n)],
                rb.at[k, XY - 1 - d, :, pl.ds(0, n)],
                rs_s.at[k], rs_r.at[k], ga, xy_band(to),
            ).start()
            return 0

        lax.fori_loop(1, XY, one, 0)

    def z_sum(k):
        n = GROUPS[k][1]
        arrived(rb.at[k, :, :, pl.ds(0, n)], rs_r.at[k])
        total = sb[k, pl.ds(32 * me, 32), pl.ds(0, n)].astype(jnp.float32)
        for d in range(XY - 1):
            total = total + rb[k, d, :, pl.ds(0, n)].astype(jnp.float32)
        town[k, :, pl.ds(0, n)] = total
        zs[k, :, pl.ds(0, n)] = total.astype(jnp.bfloat16)
        for c in range(1, NZ):
            to = (zl + c) % NZ
            copy(
                zs.at[k, :, pl.ds(0, n)], zr.at[k, NZ - 1 - c, :, pl.ds(0, n)],
                z_s.at[k], z_r.at[k], to * NC + core, band,
            ).start()

    def couple(k):
        n = GROUPS[k][1]
        arrived(zr.at[k, :, :, pl.ds(0, n)], z_r.at[k])
        total = town[k, :, pl.ds(0, n)]
        for c in range(NZ - 1):
            total = total + zr[k, c, :, pl.ds(0, n)].astype(jnp.float32)
        coupled = lax.dot_general(
            total, cm[k, pl.ds(0, n), pl.ds(0, n)], NT, precision=HIGHEST,
            preferred_element_type=jnp.float32,
        )
        dg[k, pl.ds(0, 32), pl.ds(0, n)] = coupled.astype(jnp.bfloat16)
        for batch, (first, end) in enumerate(BATCHES):
            for slot in range(max(first, 1), end):
                copy(
                    dg.at[k, pl.ds(0, 32), pl.ds(0, n)],
                    dg.at[k, pl.ds(32 * slot, 32), pl.ds(0, n)],
                    ag_s.at[k], ag_r.at[k, batch], ga, apart(OFFSETS[slot], -1),
                ).start()

    def gather_batch(k, batch):
        first, end = BATCHES[batch]
        first = max(first, 1)
        n = GROUPS[k][1]
        arrived(dg.at[k, pl.ds(32 * first, 32 * (end - first)), pl.ds(0, n)], ag_r.at[k, batch])

    def gather(k):
        n = GROUPS[k][1]
        for batch in range(3):
            gather_batch(k, batch)

        def block(r, _):
            rows = pl.ds(256 * r, 256)
            dj[k, rows, pl.ds(0, n)] = (
                -lax.dot_general(
                    jm[...], dg[k, rows, pl.ds(0, n)], NN, preferred_element_type=jnp.float32
                )
            ).astype(jnp.bfloat16)
            return 0

        lax.fori_loop(0, 2, block, 0)

    def second_piece(i, groups, first):
        def block(r, _):
            rows = pl.ds(pl.multiple_of(256 * r, 256), 256)
            total = None
            for k in groups:
                start, n = GROUPS[k]
                re = lax.dot_general(
                    dg[k, rows, pl.ds(0, n)], pc[i, 0, pl.ds(start, n), :], NN,
                    preferred_element_type=jnp.float32,
                )
                im = lax.dot_general(
                    dj[k, rows, pl.ds(0, n)], pc[i, 1, pl.ds(start, n), :], NN,
                    preferred_element_type=jnp.float32,
                )
                total = re + im if total is None else total + re + im
            if not first:
                total = total + acc[i, rows, :]
            acc[i, rows, :] = total
            return 0

        lax.fori_loop(0, 2, block, 0)

    def second_product(groups, first):
        for i in range(4):
            second_piece(i, groups, first)

    for k in range(4):
        first_early(k)
        z_copy(k).wait_recv()
        fwd_copy(k).start()
        split(k, 1)
        fwd_copy(k).wait_recv()
        split(k, 3)
        first_product(k)
        rs_send(k)
        if k >= 1:
            z_sum(k - 1)
        if k >= 2:
            couple(k - 2)
    gather(0)
    z_sum(3)
    couple(2)
    gather(1)
    second_product((0, 1), True)
    couple(3)
    gather(2)
    second_product((2,), False)

    def back_copy(slot, c, q):
        return copy(
            ab.at[c, q, pl.ds(16 * slot, 16)],
            out.at[pl.ds(16 * core, 16), :, columns(me, q)],
            b_s, b_r.at[core], zl * NC + c, apart(OFFSETS[slot], 1),
        )

    start, n = GROUPS[3]
    for batch, (first, end) in enumerate(BATCHES):
        gather_batch(3, batch)
        rows = pl.ds(32 * first, 32 * (end - first))
        value = dg[3, rows, pl.ds(0, n)].astype(jnp.float32)
        height = value.shape[0]
        even = (lax.broadcasted_iota(jnp.int32, value.shape, 0) & 1) == 0
        turned = jnp.where(
            even, -pltpu.roll(value, height - 1, 0), pltpu.roll(value, 1, 0)
        ).astype(jnp.bfloat16)
        for side, c in ((2, 1 - core), (0, core)):
            for i, g, q in pieces[side : side + 2]:
                re = lax.dot_general(
                    dg[3, rows, pl.ds(0, n)], pc[i, 0, pl.ds(start, n), :], NN,
                    preferred_element_type=jnp.float32,
                )
                im = lax.dot_general(
                    turned, pc[i, 1, pl.ds(start, n), :], NN,
                    preferred_element_type=jnp.float32,
                )
                ab[g, q, pl.ds(16 * first, 16 * (end - first))] = (
                    (re + im + acc[i, rows, :]).astype(jnp.bfloat16).reshape(height // 2, 2, WIDTH)
                )
            for slot in range(first, end):
                for q in range(NH):
                    if slot > 0 or side == 2:
                        back_copy(slot, c, q).start()
    for q in range(NH):
        out[pl.ds(16 * core, 16), :, columns(me, q)] = ab[core, q, pl.ds(0, 16)]

    for k in range(4):
        n = GROUPS[k][1]
        z_copy(k).wait_send()
        core_copy(k).wait_send()
        fwd_copy(k).wait_send()
        left(rb.at[k, :, :, pl.ds(0, n)], rs_s.at[k])
        left(zr.at[k, :, :, pl.ds(0, n)], z_s.at[k])
        left(dg.at[k, pl.ds(0, 480), pl.ds(0, n)], ag_s.at[k])
    left(xr.at[0], o_s)
    left(xr.at[0, :, pl.ds(0, 240)], o_s)
    left(ab.at[0], b_s)
    left(ab.at[0, :, pl.ds(0, 240)], b_s)
    arrived(ab.at[core, :, pl.ds(0, 240)], b_r.at[core])
    arrived(ab.at[1 - core], b_r.at[1 - core])


def per_device(orbitals, projectors, coupling, species, offsets):
    bf16, f32 = jnp.bfloat16, jnp.float32
    vmem = pl.BlockSpec(memory_space=pltpu.VMEM)
    hbm = pl.BlockSpec(memory_space=pltpu.HBM)
    dma = pltpu.SemaphoreType.DMA
    return pl.pallas_call(
        kernel,
        out_shape=pltpu.VMEM(orbitals.shape, bf16),
        in_specs=[hbm] * 5,
        out_specs=vmem,
        scratch_shapes=[
            pltpu.VMEM((4, ROWS, 2, WIDTH), bf16),
            pltpu.VMEM((4, 2, ROWS, WIDTH), bf16),
            pltpu.VMEM((2, 2, 256, 2, WIDTH), bf16),
            pltpu.VMEM((2, 2, 512, WIDTH), bf16),
            pltpu.VMEM((2, 2, 512, WIDTH), bf16),
            pltpu.VMEM((256, 256), bf16),
            pltpu.VMEM((256, 256), bf16),
            pltpu.VMEM((4, 256, 256), f32),
            pltpu.VMEM((128, 128), f32),
            pltpu.VMEM((4, 512, 256), bf16),
            pltpu.VMEM((4, XY - 1, 32, 256), bf16),
            pltpu.VMEM((4, 32, 256), f32),
            pltpu.VMEM((4, 32, 256), bf16),
            pltpu.VMEM((4, NZ - 1, 32, 256), bf16),
            pltpu.VMEM((4, 512, 256), bf16),
            pltpu.VMEM((4, 512, 256), bf16),
            pltpu.VMEM((4, 512, WIDTH), f32),
            pltpu.VMEM((2, 2, 256, 2, WIDTH), bf16),
            dma((4,)), dma((4,)), dma((4,)), dma((4,)), dma((4,)), dma((4,)),
            dma, dma((2,)), dma((4,)), dma((4,)), dma((4,)), dma((4,)),
            dma((4,)), dma((4, 3)), dma, dma((2,)), dma((4,)), dma((2,)),
            pltpu.VMEM((PER_ATOM, 4, PER_ATOM), f32),
            pltpu.VMEM((1, 48), jnp.int32),
            pltpu.VMEM((1, 48), jnp.int32),
            dma((3,)),
            pltpu.VMEM((512, 256), f32),
            pltpu.SemaphoreType.REGULAR((LEVELS,)),
        ],
        compiler_params=pltpu.CompilerParams(collective_id=0, has_side_effects=True),
    )(
        orbitals, projectors, coupling.transpose(1, 0, 2),
        species.reshape(1, -1), offsets.reshape(1, -1),
    )


def solution(mesh):
    placed = (P("band", None, "ga"), P(None, None, ("ga", "band")), P(), P(), P())
    return jax.shard_map(
        per_device, mesh=mesh, in_specs=placed, out_specs=P("band", None, "ga"), check_vma=False
    )
```

```python
import jax
import jax.numpy as jnp
from jax import lax
from jax.experimental import pallas as pl
from jax.experimental.pallas import tpu as pltpu
from jax.sharding import PartitionSpec as P

NX, NY, NH, NZ, NC = 4, 4, 2, 4, 2
XY = NX * NY
PER_ATOM = 18
GROUP_ATOMS = 14
GROUPS = ((0, 256), (256, 256), (512, 256), (768, 128))
WIDTH = 256
LEVELS = 4
ROWS = 896
COUNTS = (252, 252, 252, 108)
OFFSETS = sorted(
    ((dx, dy) for dx in range(NX) for dy in range(NY)),
    key=lambda at: (min(at[0], NX - at[0]) + min(at[1], NY - at[1]), at),
)
BATCHES = ((0, 5), (5, 8), (8, 16))
HIGHEST = lax.Precision.HIGHEST
NT = (((1,), (1,)), ((), ()))
NN = (((1,), (0,)), ((), ()))


def coupling_matrix(group, cpad, species, offsets):
    row = lax.broadcasted_iota(jnp.int32, (256, 1), 0)
    row_atom = (row * 3641) >> 16
    row_in = row - row_atom * PER_ATOM
    start = (row_atom + GROUP_ATOMS * group) * PER_ATOM
    kind = jnp.sum(
        jnp.where(offsets == start, species.astype(jnp.float32), 0.0), axis=1, keepdims=True
    )
    col = lax.broadcasted_iota(jnp.int32, (256, 128), 1)
    col_in, col_kind = col >> 2, col & 3
    pick = jnp.where(
        (col_kind.astype(jnp.float32) == kind) & (col_in == row_in), 1.0, 0.0
    ).astype(jnp.float32)
    rows = lax.dot_general(pick, cpad, NN, precision=HIGHEST, preferred_element_type=jnp.float32)
    wide = lax.broadcasted_iota(jnp.int32, (128, 256), 1)
    wide_atom = (wide * 3641) >> 16
    spread = jnp.where(
        wide - wide_atom * PER_ATOM == lax.broadcasted_iota(jnp.int32, (128, 256), 0), 1.0, 0.0
    ).astype(jnp.float32)
    full = lax.dot_general(rows, spread, NN, precision=HIGHEST, preferred_element_type=jnp.float32)
    full_row = lax.broadcasted_iota(jnp.int32, (256, 256), 0)
    full_col = lax.broadcasted_iota(jnp.int32, (256, 256), 1)
    same = ((full_row * 3641) >> 16) == ((full_col * 3641) >> 16)
    return jnp.where(same, full, 0.0)


def turn_matrix():
    row = lax.broadcasted_iota(jnp.int32, (256, 256), 0)
    col = lax.broadcasted_iota(jnp.int32, (256, 256), 1)
    even = (row & 1) == 0
    up = even & (col == row + 1)
    down = jnp.logical_not(even) & (col == row - 1)
    return (jnp.where(up, 1.0, 0.0) - jnp.where(down, 1.0, 0.0)).astype(jnp.bfloat16)


def split_matrix():
    row = lax.broadcasted_iota(jnp.int32, (256, 256), 0)
    col = lax.broadcasted_iota(jnp.int32, (256, 256), 1)
    return jnp.where(col == (row & 127) * 2 + (row >> 7), 1.0, 0.0).astype(jnp.bfloat16)


def kernel(
    orb, proj, coup_hbm, species_hbm, offsets_hbm, out,
    praw, pc, xr, xt, xj, jm, pm, cm, cpad, sb, rb, town, zs, zr, dg, dj, acc, ab,
    pz_s, pz_r, pd_s, pd_r, pf_s, pf_r, o_s, o_r, rs_s, rs_r, z_s, z_r, ag_s, ag_r, b_s, b_r,
    own_s, oo_s,
    coup, species, offsets, small_s, pacc, level_s,
):
    ga = lax.axis_index("ga")
    band = lax.axis_index("band")
    zl, core = ga // NC, ga % NC
    x, h, y = band // (NH * NY), band // NY % NH, band % NY
    me = x * NY + y

    def apart(offset, sign):
        dx, dy = offset
        return (x + NX + sign * dx) % NX * (NH * NY) + h * NY + (y + NY + sign * dy) % NY

    def xy_band(k):
        return k // NY * (NH * NY) + h * NY + k % NY

    def copy(src, dst, send, recv, to_ga, to_band):
        return pltpu.make_async_remote_copy(
            src_ref=src, dst_ref=dst, send_sem=send, recv_sem=recv,
            device_id={"ga": to_ga, "band": to_band},
            device_id_type=pl.DeviceIdType.MESH,
        )

    def arrived(ref, sem):
        copy(ref, ref, sem, sem, ga, band).wait_recv()

    def left(ref, sem):
        copy(ref, ref, sem, sem, ga, band).wait_send()

    other_core = zl * NC + 1 - core
    other_half = band + NY - 2 * NY * h

    barrier = pltpu.get_barrier_semaphore()

    def part(k):
        return pl.ds(GROUPS[k][0], COUNTS[k])

    def source(k):
        return proj.at[pl.ds(GROUP_ATOMS * PER_ATOM * k, COUNTS[k])]

    def columns(k, q):
        block = k // NY * (NH * NY) + q * NY + k % NY
        return pl.ds(pl.multiple_of(WIDTH * block, WIDTH), WIDTH)

    def greet(sem, to_ga, to_band):
        pl.semaphore_signal(
            sem, inc=1, device_id={"ga": to_ga, "band": to_band},
            device_id_type=pl.DeviceIdType.MESH,
        )

    def greet_near(sem):
        for offset in ((1, 0), (NX - 1, 0), (0, 1), (0, NY - 1)):
            greet(sem, ga, apart(offset, 1))
        greet(sem, other_core, band)

        @pl.when(zl > 0)
        def _():
            greet(sem, ga - NC, band)

        @pl.when(zl < NZ - 1)
        def _():
            greet(sem, ga + NC, band)

    near = 5 + (zl + NZ - 1) // NZ + (2 * (NZ - 1) - 1 - zl) // (NZ - 1)
    greet(barrier, ga, other_half)
    greet_near(barrier)

    own = [pltpu.make_async_copy(source(k), praw.at[0, part(k)], own_s.at[k]) for k in range(4)]
    for k in range(4):
        own[k].start()

    def z_copy(k):
        return copy(source(k), praw.at[1, part(k)], pz_s.at[k], pz_r.at[k], ga, other_half)

    def core_copy(k):
        return copy(source(k), praw.at[2, part(k)], pd_s.at[k], pd_r.at[k], other_core, band)

    def fwd_copy(k):
        return copy(
            praw.at[1, part(k)], praw.at[3, part(k)], pf_s.at[k], pf_r.at[k], other_core, band
        )

    for piece in range(4):
        for k in range(4):
            pad = GROUPS[k][1] - COUNTS[k]
            praw[piece, pl.ds(GROUPS[k][0] + COUNTS[k], pad)] = jnp.zeros(
                (pad, 2, WIDTH), jnp.bfloat16
            )

    pl.semaphore_wait(barrier, near + 1)
    for k in range(4):
        z_copy(k).start()
    for k in range(4):
        core_copy(k).start()
    for level in range(LEVELS):
        greet_near(level_s.at[level])
        pl.semaphore_wait(level_s.at[level], near)

    def orb_copy(k, c, q):
        return copy(
            orb.at[pl.ds(16 * c, 16), :, columns(k, q)],
            xr.at[core, q, pl.ds(16 * me, 16)],
            o_s, o_r.at[core], zl * NC + c, xy_band(k),
        )

    def orb_send(d, _):
        k = (me + d) % XY
        for q in range(NH):
            orb_copy(k, core, q).start()
            orb_copy(k, 1 - core, q).start()
        return 0

    lax.fori_loop(1, XY, orb_send, 0)
    own_orb = []
    for q in range(NH):
        orb_copy(me, 1 - core, q).start()
        own_orb.append(
            pltpu.make_async_copy(
                orb.at[pl.ds(16 * core, 16), :, columns(me, q)],
                xr.at[core, q, pl.ds(16 * me, 16)],
                oo_s.at[q],
            )
        )
        own_orb[q].start()
    small = [
        pltpu.make_async_copy(coup_hbm, coup, small_s.at[0]),
        pltpu.make_async_copy(species_hbm, species, small_s.at[1]),
        pltpu.make_async_copy(offsets_hbm, offsets, small_s.at[2]),
    ]
    for one in small:
        one.start()

    jm[...] = turn_matrix()
    pm[...] = split_matrix()
    cpad[...] = jnp.zeros_like(cpad)
    for one in small:
        one.wait()
    for i in range(PER_ATOM):
        cpad[pl.ds(4 * i, 4), pl.ds(0, PER_ATOM)] = coup[i]
    for k in range(4):
        cm[k] = coupling_matrix(k, cpad[...], species[...], offsets[...])

    for k in range(4):
        own[k].wait()
        core_copy(k).wait_recv()

    def split(k, piece):
        start, n = GROUPS[k]

        def block(i, _):
            at = pl.multiple_of(start + 128 * i, 128)
            both = lax.dot_general(
                pm[...], praw[piece, pl.ds(at, 128)].reshape(256, WIDTH), NN,
                preferred_element_type=jnp.float32,
            ).astype(jnp.bfloat16)
            pc[piece, 0, pl.ds(at, 128), :] = both[:128]
            pc[piece, 1, pl.ds(at, 128), :] = both[128:]
            return 0

        lax.fori_loop(0, n // 128, block, 0, unroll=True)

    for k in range(4):
        split(k, 0)
        split(k, 2)

    for q in range(NH):
        own_orb[q].wait()
    arrived(xr.at[core, :, pl.ds(0, 240)], o_r.at[core])
    arrived(xr.at[1 - core], o_r.at[1 - core])

    def turn(i, _):
        g, q, r = i // 4, i // 2 % 2, i % 2
        rows = pl.ds(pl.multiple_of(256 * r, 256), 256)
        value = xr[g, q, pl.ds(pl.multiple_of(128 * r, 128), 128)].reshape(256, WIDTH)
        xt[g, q, rows, :] = value
        xj[g, q, rows, :] = lax.dot_general(
            jm[...], value, NN, preferred_element_type=jnp.float32
        ).astype(jnp.bfloat16)
        return 0

    lax.fori_loop(0, 8, turn, 0)

    pieces = ((0, core, h), (1, core, 1 - h), (2, 1 - core, h), (3, 1 - core, 1 - h))

    def pieces_product(k, r, chosen):
        start, n = GROUPS[k]
        rows = pl.ds(pl.multiple_of(256 * r, 256), 256)
        total = None
        for i, g, q in chosen:
            re = lax.dot_general(
                xt[g, q, rows, :], pc[i, 0, pl.ds(start, n), :], NT,
                preferred_element_type=jnp.float32,
            )
            im = lax.dot_general(
                xj[g, q, rows, :], pc[i, 1, pl.ds(start, n), :], NT,
                preferred_element_type=jnp.float32,
            )
            total = re + im if total is None else total + re + im
        return rows, total

    def first_early(k):
        n = GROUPS[k][1]

        def block(r, _):
            rows, total = pieces_product(k, r, (pieces[0], pieces[2]))
            pacc[rows, pl.ds(0, n)] = total
            return 0

        lax.fori_loop(0, 2, block, 0, unroll=True)

    def first_product(k):
        n = GROUPS[k][1]

        def block(r, _):
            rows, total = pieces_product(k, r, (pieces[1], pieces[3]))
            sb[k, rows, pl.ds(0, n)] = (total + pacc[rows, pl.ds(0, n)]).astype(jnp.bfloat16)
            return 0

        lax.fori_loop(0, 2, block, 0, unroll=True)

    def rs_send(k):
        n = GROUPS[k][1]

        def one(d, _):
            to = (me + d) % XY
            copy(
                sb.at[k, pl.ds(32 * to, 32), pl.ds(0, n)],
                rb.at[k, XY - 1 - d, :, pl.ds(0, n)],
                rs_s.at[k], rs_r.at[k], ga, xy_band(to),
            ).start()
            return 0

        lax.fori_loop(1, XY, one, 0, unroll=True)

    def z_sum(k):
        n = GROUPS[k][1]
        arrived(rb.at[k, :, :, pl.ds(0, n)], rs_r.at[k])
        total = sb[k, pl.ds(32 * me, 32), pl.ds(0, n)].astype(jnp.float32)
        for d in range(XY - 1):
            total = total + rb[k, d, :, pl.ds(0, n)].astype(jnp.float32)
        town[k, :, pl.ds(0, n)] = total
        zs[k, :, pl.ds(0, n)] = total.astype(jnp.bfloat16)
        for c in range(1, NZ):
            to = (zl + c) % NZ
            copy(
                zs.at[k, :, pl.ds(0, n)], zr.at[k, NZ - 1 - c, :, pl.ds(0, n)],
                z_s.at[k], z_r.at[k], to * NC + core, band,
            ).start()

    def couple(k):
        n = GROUPS[k][1]
        arrived(zr.at[k, :, :, pl.ds(0, n)], z_r.at[k])
        total = town[k, :, pl.ds(0, n)]
        for c in range(NZ - 1):
            total = total + zr[k, c, :, pl.ds(0, n)].astype(jnp.float32)
        coupled = lax.dot_general(
            total, cm[k, pl.ds(0, n), pl.ds(0, n)], NT, precision=HIGHEST,
            preferred_element_type=jnp.float32,
        )
        dg[k, pl.ds(0, 32), pl.ds(0, n)] = coupled.astype(jnp.bfloat16)
        for batch, (first, end) in enumerate(BATCHES):
            for slot in range(max(first, 1), end):
                copy(
                    dg.at[k, pl.ds(0, 32), pl.ds(0, n)],
                    dg.at[k, pl.ds(32 * slot, 32), pl.ds(0, n)],
                    ag_s.at[k], ag_r.at[k, batch], ga, apart(OFFSETS[slot], -1),
                ).start()

    def gather_batch(k, batch):
        first, end = BATCHES[batch]
        first = max(first, 1)
        n = GROUPS[k][1]
        arrived(dg.at[k, pl.ds(32 * first, 32 * (end - first)), pl.ds(0, n)], ag_r.at[k, batch])

    def gather(k):
        n = GROUPS[k][1]
        for batch in range(3):
            gather_batch(k, batch)

        def block(r, _):
            rows = pl.ds(256 * r, 256)
            dj[k, rows, pl.ds(0, n)] = (
                -lax.dot_general(
                    jm[...], dg[k, rows, pl.ds(0, n)], NN, preferred_element_type=jnp.float32
                )
            ).astype(jnp.bfloat16)
            return 0

        lax.fori_loop(0, 2, block, 0, unroll=True)

    def second_piece(i, groups):
        def block(r, _):
            rows = pl.ds(pl.multiple_of(256 * r, 256), 256)
            total = None
            for k in groups:
                start, n = GROUPS[k]
                re = lax.dot_general(
                    dg[k, rows, pl.ds(0, n)], pc[i, 0, pl.ds(start, n), :], NN,
                    preferred_element_type=jnp.float32,
                )
                im = lax.dot_general(
                    dj[k, rows, pl.ds(0, n)], pc[i, 1, pl.ds(start, n), :], NN,
                    preferred_element_type=jnp.float32,
                )
                total = re + im if total is None else total + re + im
            acc[i, rows, :] = total
            return 0

        lax.fori_loop(0, 2, block, 0, unroll=True)

    def second_product(groups):
        for i in range(4):
            second_piece(i, groups)

    for k in range(4):
        first_early(k)
        z_copy(k).wait_recv()
        fwd_copy(k).start()
        split(k, 1)
        fwd_copy(k).wait_recv()
        split(k, 3)
        first_product(k)
        rs_send(k)
        if k >= 1:
            z_sum(k - 1)
        if k >= 2:
            couple(k - 2)
    gather(0)
    z_sum(3)
    couple(2)
    gather(1)
    second_product((0, 1))
    couple(3)

    def back_copy(slot, c, q):
        return copy(
            ab.at[c, q, pl.ds(16 * slot, 16)],
            out.at[pl.ds(16 * core, 16), :, columns(me, q)],
            b_s, b_r.at[core], zl * NC + c, apart(OFFSETS[slot], 1),
        )

    late = (2, 3)
    for batch, (first, end) in enumerate(BATCHES):
        rows = pl.ds(32 * first, 32 * (end - first))
        height = 32 * (end - first)
        turned = {}
        for k in late:
            n = GROUPS[k][1]
            gather_batch(k, batch)
            value = dg[k, rows, pl.ds(0, n)].astype(jnp.float32)
            even = (lax.broadcasted_iota(jnp.int32, value.shape, 0) & 1) == 0
            turned[k] = jnp.where(
                even, -pltpu.roll(value, height - 1, 0), pltpu.roll(value, 1, 0)
            ).astype(jnp.bfloat16)
        for side, c in ((2, 1 - core), (0, core)):
            for i, g, q in pieces[side : side + 2]:
                total = acc[i, rows, :]
                for k in late:
                    start, n = GROUPS[k]
                    re = lax.dot_general(
                        dg[k, rows, pl.ds(0, n)], pc[i, 0, pl.ds(start, n), :], NN,
                        preferred_element_type=jnp.float32,
                    )
                    im = lax.dot_general(
                        turned[k], pc[i, 1, pl.ds(start, n), :], NN,
                        preferred_element_type=jnp.float32,
                    )
                    total = total + (re + im)
                ab[g, q, pl.ds(16 * first, 16 * (end - first))] = (
                    total.astype(jnp.bfloat16).reshape(height // 2, 2, WIDTH)
                )
            for slot in range(first, end):
                for q in range(NH):
                    if slot > 0 or side == 2:
                        back_copy(slot, c, q).start()
    for q in range(NH):
        out[pl.ds(16 * core, 16), :, columns(me, q)] = ab[core, q, pl.ds(0, 16)]

    for k in range(4):
        n = GROUPS[k][1]
        z_copy(k).wait_send()
        core_copy(k).wait_send()
        fwd_copy(k).wait_send()
        left(rb.at[k, :, :, pl.ds(0, n)], rs_s.at[k])
        left(zr.at[k, :, :, pl.ds(0, n)], z_s.at[k])
        left(dg.at[k, pl.ds(0, 480), pl.ds(0, n)], ag_s.at[k])
    left(xr.at[0], o_s)
    left(xr.at[0, :, pl.ds(0, 240)], o_s)
    left(ab.at[0], b_s)
    left(ab.at[0, :, pl.ds(0, 240)], b_s)
    arrived(ab.at[core, :, pl.ds(0, 240)], b_r.at[core])
    arrived(ab.at[1 - core], b_r.at[1 - core])


def per_device(orbitals, projectors, coupling, species, offsets):
    bf16, f32 = jnp.bfloat16, jnp.float32
    vmem = pl.BlockSpec(memory_space=pltpu.VMEM)
    hbm = pl.BlockSpec(memory_space=pltpu.HBM)
    dma = pltpu.SemaphoreType.DMA
    return pl.pallas_call(
        kernel,
        out_shape=pltpu.VMEM(orbitals.shape, bf16),
        in_specs=[hbm] * 5,
        out_specs=vmem,
        scratch_shapes=[
            pltpu.VMEM((4, ROWS, 2, WIDTH), bf16),
            pltpu.VMEM((4, 2, ROWS, WIDTH), bf16),
            pltpu.VMEM((2, 2, 256, 2, WIDTH), bf16),
            pltpu.VMEM((2, 2, 512, WIDTH), bf16),
            pltpu.VMEM((2, 2, 512, WIDTH), bf16),
            pltpu.VMEM((256, 256), bf16),
            pltpu.VMEM((256, 256), bf16),
            pltpu.VMEM((4, 256, 256), f32),
            pltpu.VMEM((128, 128), f32),
            pltpu.VMEM((4, 512, 256), bf16),
            pltpu.VMEM((4, XY - 1, 32, 256), bf16),
            pltpu.VMEM((4, 32, 256), f32),
            pltpu.VMEM((4, 32, 256), bf16),
            pltpu.VMEM((4, NZ - 1, 32, 256), bf16),
            pltpu.VMEM((4, 512, 256), bf16),
            pltpu.VMEM((4, 512, 256), bf16),
            pltpu.VMEM((4, 512, WIDTH), f32),
            pltpu.VMEM((2, 2, 256, 2, WIDTH), bf16),
            dma((4,)), dma((4,)), dma((4,)), dma((4,)), dma((4,)), dma((4,)),
            dma, dma((2,)), dma((4,)), dma((4,)), dma((4,)), dma((4,)),
            dma((4,)), dma((4, 3)), dma, dma((2,)), dma((4,)), dma((2,)),
            pltpu.VMEM((PER_ATOM, 4, PER_ATOM), f32),
            pltpu.VMEM((1, 48), jnp.int32),
            pltpu.VMEM((1, 48), jnp.int32),
            dma((3,)),
            pltpu.VMEM((512, 256), f32),
            pltpu.SemaphoreType.REGULAR((LEVELS,)),
        ],
        compiler_params=pltpu.CompilerParams(collective_id=0, has_side_effects=True),
    )(
        orbitals, projectors, coupling.transpose(1, 0, 2),
        species.reshape(1, -1), offsets.reshape(1, -1),
    )


def solution(mesh):
    placed = (P("band", None, "ga"), P(None, None, ("ga", "band")), P(), P(), P())
    return jax.shard_map(
        per_device, mesh=mesh, in_specs=placed, out_specs=P("band", None, "ga"), check_vma=False
    )
```

```python
import jax
import jax.numpy as jnp
from jax import lax
from jax.experimental import pallas as pl
from jax.experimental.pallas import tpu as pltpu
from jax.sharding import PartitionSpec as P

NX, NY, NH, NZ, NC = 4, 4, 2, 4, 2
XY = NX * NY
PER_ATOM = 18
GROUP_ATOMS = 14
GROUPS = ((0, 256), (256, 256), (512, 256), (768, 128))
WIDTH = 256
LEVELS = 4
ROWS = 896
COUNTS = (252, 252, 252, 108)
OFFSETS = sorted(
    ((dx, dy) for dx in range(NX) for dy in range(NY)),
    key=lambda at: (min(at[0], NX - at[0]) + min(at[1], NY - at[1]), at),
)
BATCHES = ((0, 5), (5, 8), (8, 16))
HIGHEST = lax.Precision.HIGHEST
NT = (((1,), (1,)), ((), ()))
NN = (((1,), (0,)), ((), ()))


def coupling_matrix(group, cpad, species, offsets):
    row = lax.broadcasted_iota(jnp.int32, (256, 1), 0)
    row_atom = (row * 3641) >> 16
    row_in = row - row_atom * PER_ATOM
    start = (row_atom + GROUP_ATOMS * group) * PER_ATOM
    kind = jnp.sum(
        jnp.where(offsets == start, species.astype(jnp.float32), 0.0), axis=1, keepdims=True
    )
    col = lax.broadcasted_iota(jnp.int32, (256, 128), 1)
    col_in, col_kind = col >> 2, col & 3
    pick = jnp.where(
        (col_kind.astype(jnp.float32) == kind) & (col_in == row_in), 1.0, 0.0
    ).astype(jnp.float32)
    rows = lax.dot_general(pick, cpad, NN, precision=HIGHEST, preferred_element_type=jnp.float32)
    wide = lax.broadcasted_iota(jnp.int32, (128, 256), 1)
    wide_atom = (wide * 3641) >> 16
    spread = jnp.where(
        wide - wide_atom * PER_ATOM == lax.broadcasted_iota(jnp.int32, (128, 256), 0), 1.0, 0.0
    ).astype(jnp.float32)
    full = lax.dot_general(rows, spread, NN, precision=HIGHEST, preferred_element_type=jnp.float32)
    full_row = lax.broadcasted_iota(jnp.int32, (256, 256), 0)
    full_col = lax.broadcasted_iota(jnp.int32, (256, 256), 1)
    same = ((full_row * 3641) >> 16) == ((full_col * 3641) >> 16)
    return jnp.where(same, full, 0.0)


def turn_matrix():
    row = lax.broadcasted_iota(jnp.int32, (256, 256), 0)
    col = lax.broadcasted_iota(jnp.int32, (256, 256), 1)
    even = (row & 1) == 0
    up = even & (col == row + 1)
    down = jnp.logical_not(even) & (col == row - 1)
    return (jnp.where(up, 1.0, 0.0) - jnp.where(down, 1.0, 0.0)).astype(jnp.bfloat16)


def split_matrix():
    row = lax.broadcasted_iota(jnp.int32, (256, 256), 0)
    col = lax.broadcasted_iota(jnp.int32, (256, 256), 1)
    return jnp.where(col == (row & 127) * 2 + (row >> 7), 1.0, 0.0).astype(jnp.bfloat16)


def kernel(
    orb, proj, coup_hbm, species_hbm, offsets_hbm, out,
    praw, pc, xr, xt, xj, jm, pm, cm, cpad, sb, rb, town, zs, zr, dg, dj, acc, ab,
    pz_s, pz_r, pd_s, pd_r, pf_s, pf_r, o_s, o_r, rs_s, rs_r, z_s, z_r, ag_s, ag_r, b_s, b_r,
    own_s, oo_s,
    coup, species, offsets, small_s, pacc, level_s,
):
    ga = lax.axis_index("ga")
    band = lax.axis_index("band")
    zl, core = ga // NC, ga % NC
    x, h, y = band // (NH * NY), band // NY % NH, band % NY
    me = x * NY + y

    def apart(offset, sign):
        dx, dy = offset
        return (x + NX + sign * dx) % NX * (NH * NY) + h * NY + (y + NY + sign * dy) % NY

    def xy_band(k):
        return k // NY * (NH * NY) + h * NY + k % NY

    def copy(src, dst, send, recv, to_ga, to_band):
        return pltpu.make_async_remote_copy(
            src_ref=src, dst_ref=dst, send_sem=send, recv_sem=recv,
            device_id={"ga": to_ga, "band": to_band},
            device_id_type=pl.DeviceIdType.MESH,
        )

    def arrived(ref, sem):
        copy(ref, ref, sem, sem, ga, band).wait_recv()

    def left(ref, sem):
        copy(ref, ref, sem, sem, ga, band).wait_send()

    other_core = zl * NC + 1 - core
    other_half = band + NY - 2 * NY * h

    barrier = pltpu.get_barrier_semaphore()

    def part(k):
        return pl.ds(GROUPS[k][0], COUNTS[k])

    def source(k):
        return proj.at[pl.ds(GROUP_ATOMS * PER_ATOM * k, COUNTS[k])]

    def columns(k, q):
        block = k // NY * (NH * NY) + q * NY + k % NY
        return pl.ds(pl.multiple_of(WIDTH * block, WIDTH), WIDTH)

    def greet(sem, to_ga, to_band):
        pl.semaphore_signal(
            sem, inc=1, device_id={"ga": to_ga, "band": to_band},
            device_id_type=pl.DeviceIdType.MESH,
        )

    def greet_near(sem):
        for offset in ((1, 0), (NX - 1, 0), (0, 1), (0, NY - 1)):
            greet(sem, ga, apart(offset, 1))
        greet(sem, other_core, band)

        @pl.when(zl > 0)
        def _():
            greet(sem, ga - NC, band)

        @pl.when(zl < NZ - 1)
        def _():
            greet(sem, ga + NC, band)

    near = 5 + (zl + NZ - 1) // NZ + (2 * (NZ - 1) - 1 - zl) // (NZ - 1)
    greet(barrier, ga, other_half)
    greet_near(barrier)

    own = [pltpu.make_async_copy(source(k), praw.at[0, part(k)], own_s.at[k]) for k in range(4)]
    for k in range(4):
        own[k].start()

    def z_copy(k):
        return copy(source(k), praw.at[1, part(k)], pz_s.at[k], pz_r.at[k], ga, other_half)

    def core_copy(k):
        return copy(source(k), praw.at[2, part(k)], pd_s.at[k], pd_r.at[k], other_core, band)

    def fwd_copy(k):
        return copy(
            praw.at[1, part(k)], praw.at[3, part(k)], pf_s.at[k], pf_r.at[k], other_core, band
        )

    for piece in range(4):
        for k in range(4):
            pad = GROUPS[k][1] - COUNTS[k]
            praw[piece, pl.ds(GROUPS[k][0] + COUNTS[k], pad)] = jnp.zeros(
                (pad, 2, WIDTH), jnp.bfloat16
            )

    pl.semaphore_wait(barrier, near + 1)
    for k in range(4):
        z_copy(k).start()
    for k in range(4):
        core_copy(k).start()
    for level in range(LEVELS):
        greet_near(level_s.at[level])
        pl.semaphore_wait(level_s.at[level], near)

    def orb_copy(k, c, q):
        return copy(
            orb.at[pl.ds(16 * c, 16), :, columns(k, q)],
            xr.at[core, q, pl.ds(16 * me, 16)],
            o_s, o_r.at[core], zl * NC + c, xy_band(k),
        )

    def orb_send(d, _):
        k = (me + d) % XY
        for q in range(NH):
            orb_copy(k, core, q).start()
            orb_copy(k, 1 - core, q).start()
        return 0

    lax.fori_loop(1, XY, orb_send, 0)
    own_orb = []
    for q in range(NH):
        orb_copy(me, 1 - core, q).start()
        own_orb.append(
            pltpu.make_async_copy(
                orb.at[pl.ds(16 * core, 16), :, columns(me, q)],
                xr.at[core, q, pl.ds(16 * me, 16)],
                oo_s.at[q],
            )
        )
        own_orb[q].start()
    small = [
        pltpu.make_async_copy(coup_hbm, coup, small_s.at[0]),
        pltpu.make_async_copy(species_hbm, species, small_s.at[1]),
        pltpu.make_async_copy(offsets_hbm, offsets, small_s.at[2]),
    ]
    for one in small:
        one.start()

    jm[...] = turn_matrix()
    pm[...] = split_matrix()
    cpad[...] = jnp.zeros_like(cpad)
    for one in small:
        one.wait()
    for i in range(PER_ATOM):
        cpad[pl.ds(4 * i, 4), pl.ds(0, PER_ATOM)] = coup[i]
    for k in range(4):
        cm[k] = coupling_matrix(k, cpad[...], species[...], offsets[...])

    for k in range(4):
        own[k].wait()
        core_copy(k).wait_recv()

    def split(k, piece):
        start, n = GROUPS[k]

        def block(i, _):
            at = pl.multiple_of(start + 128 * i, 128)
            both = lax.dot_general(
                pm[...], praw[piece, pl.ds(at, 128)].reshape(256, WIDTH), NN,
                preferred_element_type=jnp.float32,
            ).astype(jnp.bfloat16)
            pc[piece, 0, pl.ds(at, 128), :] = both[:128]
            pc[piece, 1, pl.ds(at, 128), :] = both[128:]
            return 0

        lax.fori_loop(0, n // 128, block, 0, unroll=True)

    for k in range(4):
        split(k, 0)
        split(k, 2)

    for q in range(NH):
        own_orb[q].wait()
    arrived(xr.at[core, :, pl.ds(0, 240)], o_r.at[core])
    arrived(xr.at[1 - core], o_r.at[1 - core])

    def turn(i, _):
        g, q, r = i // 4, i // 2 % 2, i % 2
        rows = pl.ds(pl.multiple_of(256 * r, 256), 256)
        value = xr[g, q, pl.ds(pl.multiple_of(128 * r, 128), 128)].reshape(256, WIDTH)
        xt[g, q, rows, :] = value
        xj[g, q, rows, :] = lax.dot_general(
            jm[...], value, NN, preferred_element_type=jnp.float32
        ).astype(jnp.bfloat16)
        return 0

    lax.fori_loop(0, 8, turn, 0)

    pieces = ((0, core, h), (1, core, 1 - h), (2, 1 - core, h), (3, 1 - core, 1 - h))

    def pieces_product(k, r, chosen):
        start, n = GROUPS[k]
        rows = pl.ds(pl.multiple_of(256 * r, 256), 256)
        total = None
        for i, g, q in chosen:
            re = lax.dot_general(
                xt[g, q, rows, :], pc[i, 0, pl.ds(start, n), :], NT,
                preferred_element_type=jnp.float32,
            )
            im = lax.dot_general(
                xj[g, q, rows, :], pc[i, 1, pl.ds(start, n), :], NT,
                preferred_element_type=jnp.float32,
            )
            total = re + im if total is None else total + re + im
        return rows, total

    def first_early(k):
        n = GROUPS[k][1]

        def block(r, _):
            rows, total = pieces_product(k, r, (pieces[0], pieces[2]))
            pacc[rows, pl.ds(0, n)] = total
            return 0

        lax.fori_loop(0, 2, block, 0, unroll=True)

    def first_product(k):
        n = GROUPS[k][1]

        def block(r, _):
            rows, total = pieces_product(k, r, (pieces[1], pieces[3]))
            sb[k, rows, pl.ds(0, n)] = (total + pacc[rows, pl.ds(0, n)]).astype(jnp.bfloat16)
            return 0

        lax.fori_loop(0, 2, block, 0, unroll=True)

    def rs_send(k):
        n = GROUPS[k][1]

        def one(d, _):
            to = (me + d) % XY
            copy(
                sb.at[k, pl.ds(32 * to, 32), pl.ds(0, n)],
                rb.at[k, XY - 1 - d, :, pl.ds(0, n)],
                rs_s.at[k], rs_r.at[k], ga, xy_band(to),
            ).start()
            return 0

        lax.fori_loop(1, XY, one, 0, unroll=True)

    def z_sum(k):
        n = GROUPS[k][1]
        arrived(rb.at[k, :, :, pl.ds(0, n)], rs_r.at[k])
        total = sb[k, pl.ds(32 * me, 32), pl.ds(0, n)].astype(jnp.float32)
        for d in range(XY - 1):
            total = total + rb[k, d, :, pl.ds(0, n)].astype(jnp.float32)
        town[k, :, pl.ds(0, n)] = total
        zs[k, :, pl.ds(0, n)] = total.astype(jnp.bfloat16)
        for c in range(1, NZ):
            to = (zl + c) % NZ
            copy(
                zs.at[k, :, pl.ds(0, n)], zr.at[k, NZ - 1 - c, :, pl.ds(0, n)],
                z_s.at[k], z_r.at[k], to * NC + core, band,
            ).start()

    def couple(k):
        n = GROUPS[k][1]
        arrived(zr.at[k, :, :, pl.ds(0, n)], z_r.at[k])
        total = town[k, :, pl.ds(0, n)]
        for c in range(NZ - 1):
            total = total + zr[k, c, :, pl.ds(0, n)].astype(jnp.float32)
        coupled = lax.dot_general(
            total, cm[k, pl.ds(0, n), pl.ds(0, n)], NT, precision=HIGHEST,
            preferred_element_type=jnp.float32,
        )
        dg[k, pl.ds(0, 32), pl.ds(0, n)] = coupled.astype(jnp.bfloat16)
        for batch, (first, end) in enumerate(BATCHES):
            for slot in range(max(first, 1), end):
                copy(
                    dg.at[k, pl.ds(0, 32), pl.ds(0, n)],
                    dg.at[k, pl.ds(32 * slot, 32), pl.ds(0, n)],
                    ag_s.at[k], ag_r.at[k, batch], ga, apart(OFFSETS[slot], -1),
                ).start()

    def gather_batch(k, batch):
        first, end = BATCHES[batch]
        first = max(first, 1)
        n = GROUPS[k][1]
        arrived(dg.at[k, pl.ds(32 * first, 32 * (end - first)), pl.ds(0, n)], ag_r.at[k, batch])

    def gather(k):
        n = GROUPS[k][1]
        for batch in range(3):
            gather_batch(k, batch)

        def block(r, _):
            rows = pl.ds(256 * r, 256)
            dj[k, rows, pl.ds(0, n)] = (
                -lax.dot_general(
                    jm[...], dg[k, rows, pl.ds(0, n)], NN, preferred_element_type=jnp.float32
                )
            ).astype(jnp.bfloat16)
            return 0

        lax.fori_loop(0, 2, block, 0, unroll=True)

    def second_piece(i, groups):
        def block(r, _):
            rows = pl.ds(pl.multiple_of(256 * r, 256), 256)
            total = None
            for k in groups:
                start, n = GROUPS[k]
                re = lax.dot_general(
                    dg[k, rows, pl.ds(0, n)], pc[i, 0, pl.ds(start, n), :], NN,
                    preferred_element_type=jnp.float32,
                )
                im = lax.dot_general(
                    dj[k, rows, pl.ds(0, n)], pc[i, 1, pl.ds(start, n), :], NN,
                    preferred_element_type=jnp.float32,
                )
                total = re + im if total is None else total + re + im
            acc[i, rows, :] = total
            return 0

        lax.fori_loop(0, 2, block, 0, unroll=True)

    def second_product(groups):
        for i in range(4):
            second_piece(i, groups)

    for k in range(4):
        first_early(k)
        z_copy(k).wait_recv()
        fwd_copy(k).start()
        split(k, 1)
        fwd_copy(k).wait_recv()
        split(k, 3)
        first_product(k)
        rs_send(k)
        if k >= 1:
            z_sum(k - 1)
        if k >= 2:
            couple(k - 2)
    gather(0)
    z_sum(3)
    couple(2)
    second_product((0,))
    couple(3)

    def back_copy(slot, c, q):
        return copy(
            ab.at[c, q, pl.ds(16 * slot, 16)],
            out.at[pl.ds(16 * core, 16), :, columns(me, q)],
            b_s, b_r.at[core], zl * NC + c, apart(OFFSETS[slot], 1),
        )

    late = (1, 2, 3)
    for batch, (first, end) in enumerate(BATCHES):
        rows = pl.ds(32 * first, 32 * (end - first))
        height = 32 * (end - first)
        turned = {}
        for k in late:
            n = GROUPS[k][1]
            gather_batch(k, batch)
            value = dg[k, rows, pl.ds(0, n)].astype(jnp.float32)
            even = (lax.broadcasted_iota(jnp.int32, value.shape, 0) & 1) == 0
            turned[k] = jnp.where(
                even, -pltpu.roll(value, height - 1, 0), pltpu.roll(value, 1, 0)
            ).astype(jnp.bfloat16)
        for side, c in ((2, 1 - core), (0, core)):
            for i, g, q in pieces[side : side + 2]:
                total = acc[i, rows, :]
                for k in late:
                    start, n = GROUPS[k]
                    re = lax.dot_general(
                        dg[k, rows, pl.ds(0, n)], pc[i, 0, pl.ds(start, n), :], NN,
                        preferred_element_type=jnp.float32,
                    )
                    im = lax.dot_general(
                        turned[k], pc[i, 1, pl.ds(start, n), :], NN,
                        preferred_element_type=jnp.float32,
                    )
                    total = total + (re + im)
                ab[g, q, pl.ds(16 * first, 16 * (end - first))] = (
                    total.astype(jnp.bfloat16).reshape(height // 2, 2, WIDTH)
                )
            for slot in range(first, end):
                for q in range(NH):
                    if slot > 0 or side == 2:
                        back_copy(slot, c, q).start()
    for q in range(NH):
        out[pl.ds(16 * core, 16), :, columns(me, q)] = ab[core, q, pl.ds(0, 16)]

    for k in range(4):
        n = GROUPS[k][1]
        z_copy(k).wait_send()
        core_copy(k).wait_send()
        fwd_copy(k).wait_send()
        left(rb.at[k, :, :, pl.ds(0, n)], rs_s.at[k])
        left(zr.at[k, :, :, pl.ds(0, n)], z_s.at[k])
        left(dg.at[k, pl.ds(0, 480), pl.ds(0, n)], ag_s.at[k])
    left(xr.at[0], o_s)
    left(xr.at[0, :, pl.ds(0, 240)], o_s)
    left(ab.at[0], b_s)
    left(ab.at[0, :, pl.ds(0, 240)], b_s)
    arrived(ab.at[core, :, pl.ds(0, 240)], b_r.at[core])
    arrived(ab.at[1 - core], b_r.at[1 - core])


def per_device(orbitals, projectors, coupling, species, offsets):
    bf16, f32 = jnp.bfloat16, jnp.float32
    vmem = pl.BlockSpec(memory_space=pltpu.VMEM)
    hbm = pl.BlockSpec(memory_space=pltpu.HBM)
    dma = pltpu.SemaphoreType.DMA
    return pl.pallas_call(
        kernel,
        out_shape=pltpu.VMEM(orbitals.shape, bf16),
        in_specs=[hbm] * 5,
        out_specs=vmem,
        scratch_shapes=[
            pltpu.VMEM((4, ROWS, 2, WIDTH), bf16),
            pltpu.VMEM((4, 2, ROWS, WIDTH), bf16),
            pltpu.VMEM((2, 2, 256, 2, WIDTH), bf16),
            pltpu.VMEM((2, 2, 512, WIDTH), bf16),
            pltpu.VMEM((2, 2, 512, WIDTH), bf16),
            pltpu.VMEM((256, 256), bf16),
            pltpu.VMEM((256, 256), bf16),
            pltpu.VMEM((4, 256, 256), f32),
            pltpu.VMEM((128, 128), f32),
            pltpu.VMEM((4, 512, 256), bf16),
            pltpu.VMEM((4, XY - 1, 32, 256), bf16),
            pltpu.VMEM((4, 32, 256), f32),
            pltpu.VMEM((4, 32, 256), bf16),
            pltpu.VMEM((4, NZ - 1, 32, 256), bf16),
            pltpu.VMEM((4, 512, 256), bf16),
            pltpu.VMEM((4, 512, 256), bf16),
            pltpu.VMEM((4, 512, WIDTH), f32),
            pltpu.VMEM((2, 2, 256, 2, WIDTH), bf16),
            dma((4,)), dma((4,)), dma((4,)), dma((4,)), dma((4,)), dma((4,)),
            dma, dma((2,)), dma((4,)), dma((4,)), dma((4,)), dma((4,)),
            dma((4,)), dma((4, 3)), dma, dma((2,)), dma((4,)), dma((2,)),
            pltpu.VMEM((PER_ATOM, 4, PER_ATOM), f32),
            pltpu.VMEM((1, 48), jnp.int32),
            pltpu.VMEM((1, 48), jnp.int32),
            dma((3,)),
            pltpu.VMEM((512, 256), f32),
            pltpu.SemaphoreType.REGULAR((LEVELS,)),
        ],
        compiler_params=pltpu.CompilerParams(collective_id=0, has_side_effects=True),
    )(
        orbitals, projectors, coupling.transpose(1, 0, 2),
        species.reshape(1, -1), offsets.reshape(1, -1),
    )


def solution(mesh):
    placed = (P("band", None, "ga"), P(None, None, ("ga", "band")), P(), P(), P())
    return jax.shard_map(
        per_device, mesh=mesh, in_specs=placed, out_specs=P("band", None, "ga"), check_vma=False
    )
```

```python
import jax
import jax.numpy as jnp
from jax import lax
from jax.experimental import pallas as pl
from jax.experimental.pallas import tpu as pltpu
from jax.sharding import PartitionSpec as P

NX, NY, NH, NZ, NC = 4, 4, 2, 4, 2
XY = NX * NY
PER_ATOM = 18
GROUP_ATOMS = 14
GROUPS = ((0, 256), (256, 256), (512, 256), (768, 128))
WIDTH = 256
LEVELS = 4
ROWS = 896
COUNTS = (252, 252, 252, 108)
OFFSETS = sorted(
    ((dx, dy) for dx in range(NX) for dy in range(NY)),
    key=lambda at: (min(at[0], NX - at[0]) + min(at[1], NY - at[1]), at),
)
BATCHES = ((0, 5), (5, 8), (8, 16))
HIGHEST = lax.Precision.HIGHEST
NT = (((1,), (1,)), ((), ()))
NN = (((1,), (0,)), ((), ()))


def coupling_matrix(group, cpad, species, offsets):
    row = lax.broadcasted_iota(jnp.int32, (256, 1), 0)
    row_atom = (row * 3641) >> 16
    row_in = row - row_atom * PER_ATOM
    start = (row_atom + GROUP_ATOMS * group) * PER_ATOM
    kind = jnp.sum(
        jnp.where(offsets == start, species.astype(jnp.float32), 0.0), axis=1, keepdims=True
    )
    col = lax.broadcasted_iota(jnp.int32, (256, 128), 1)
    col_in, col_kind = col >> 2, col & 3
    pick = jnp.where(
        (col_kind.astype(jnp.float32) == kind) & (col_in == row_in), 1.0, 0.0
    ).astype(jnp.float32)
    rows = lax.dot_general(pick, cpad, NN, precision=HIGHEST, preferred_element_type=jnp.float32)
    wide = lax.broadcasted_iota(jnp.int32, (128, 256), 1)
    wide_atom = (wide * 3641) >> 16
    spread = jnp.where(
        wide - wide_atom * PER_ATOM == lax.broadcasted_iota(jnp.int32, (128, 256), 0), 1.0, 0.0
    ).astype(jnp.float32)
    full = lax.dot_general(rows, spread, NN, precision=HIGHEST, preferred_element_type=jnp.float32)
    full_row = lax.broadcasted_iota(jnp.int32, (256, 256), 0)
    full_col = lax.broadcasted_iota(jnp.int32, (256, 256), 1)
    same = ((full_row * 3641) >> 16) == ((full_col * 3641) >> 16)
    return jnp.where(same, full, 0.0)


def turn_matrix():
    row = lax.broadcasted_iota(jnp.int32, (256, 256), 0)
    col = lax.broadcasted_iota(jnp.int32, (256, 256), 1)
    even = (row & 1) == 0
    up = even & (col == row + 1)
    down = jnp.logical_not(even) & (col == row - 1)
    return (jnp.where(up, 1.0, 0.0) - jnp.where(down, 1.0, 0.0)).astype(jnp.bfloat16)


def split_matrix():
    row = lax.broadcasted_iota(jnp.int32, (256, 256), 0)
    col = lax.broadcasted_iota(jnp.int32, (256, 256), 1)
    return jnp.where(col == (row & 127) * 2 + (row >> 7), 1.0, 0.0).astype(jnp.bfloat16)


def kernel(
    orb, proj, coup_hbm, species_hbm, offsets_hbm, out,
    praw, pc, xr, xt, xj, jm, pm, cm, cpad, sb, rb, town, zs, zr, dg, dj, acc, ab,
    pz_s, pz_r, pd_s, pd_r, pf_s, pf_r, o_s, o_r, rs_s, rs_r, z_s, z_r, ag_s, ag_r, b_s, b_r,
    own_s, oo_s,
    coup, species, offsets, small_s, pacc, level_s,
):
    ga = lax.axis_index("ga")
    band = lax.axis_index("band")
    zl, core = ga // NC, ga % NC
    x, h, y = band // (NH * NY), band // NY % NH, band % NY
    me = x * NY + y

    def apart(offset, sign):
        dx, dy = offset
        return (x + NX + sign * dx) % NX * (NH * NY) + h * NY + (y + NY + sign * dy) % NY

    def xy_band(k):
        return k // NY * (NH * NY) + h * NY + k % NY

    def copy(src, dst, send, recv, to_ga, to_band):
        return pltpu.make_async_remote_copy(
            src_ref=src, dst_ref=dst, send_sem=send, recv_sem=recv,
            device_id={"ga": to_ga, "band": to_band},
            device_id_type=pl.DeviceIdType.MESH,
        )

    def arrived(ref, sem):
        copy(ref, ref, sem, sem, ga, band).wait_recv()

    def left(ref, sem):
        copy(ref, ref, sem, sem, ga, band).wait_send()

    other_core = zl * NC + 1 - core
    other_half = band + NY - 2 * NY * h

    barrier = pltpu.get_barrier_semaphore()

    def part(k):
        return pl.ds(GROUPS[k][0], COUNTS[k])

    def source(k):
        return proj.at[pl.ds(GROUP_ATOMS * PER_ATOM * k, COUNTS[k])]

    def columns(k, q):
        block = k // NY * (NH * NY) + q * NY + k % NY
        return pl.ds(pl.multiple_of(WIDTH * block, WIDTH), WIDTH)

    def greet(sem, to_ga, to_band):
        pl.semaphore_signal(
            sem, inc=1, device_id={"ga": to_ga, "band": to_band},
            device_id_type=pl.DeviceIdType.MESH,
        )

    def greet_near(sem):
        for offset in ((1, 0), (NX - 1, 0), (0, 1), (0, NY - 1)):
            greet(sem, ga, apart(offset, 1))
        greet(sem, other_core, band)

        @pl.when(zl > 0)
        def _():
            greet(sem, ga - NC, band)

        @pl.when(zl < NZ - 1)
        def _():
            greet(sem, ga + NC, band)

    near = 5 + (zl + NZ - 1) // NZ + (2 * (NZ - 1) - 1 - zl) // (NZ - 1)
    greet(barrier, ga, other_half)
    greet_near(barrier)

    own = [pltpu.make_async_copy(source(k), praw.at[0, part(k)], own_s.at[k]) for k in range(4)]
    for k in range(4):
        own[k].start()

    def z_copy(k):
        return copy(source(k), praw.at[1, part(k)], pz_s.at[k], pz_r.at[k], ga, other_half)

    def core_copy(k):
        return copy(source(k), praw.at[2, part(k)], pd_s.at[k], pd_r.at[k], other_core, band)

    def fwd_copy(k):
        return copy(
            praw.at[1, part(k)], praw.at[3, part(k)], pf_s.at[k], pf_r.at[k], other_core, band
        )

    for piece in range(4):
        for k in range(4):
            pad = GROUPS[k][1] - COUNTS[k]
            praw[piece, pl.ds(GROUPS[k][0] + COUNTS[k], pad)] = jnp.zeros(
                (pad, 2, WIDTH), jnp.bfloat16
            )

    pl.semaphore_wait(barrier, near + 1)
    for k in range(4):
        z_copy(k).start()
    for k in range(4):
        core_copy(k).start()
    for level in range(LEVELS):
        greet_near(level_s.at[level])
        pl.semaphore_wait(level_s.at[level], near)

    def orb_copy(k, c, q):
        return copy(
            orb.at[pl.ds(16 * c, 16), :, columns(k, q)],
            xr.at[core, q, pl.ds(16 * me, 16)],
            o_s, o_r.at[core], zl * NC + c, xy_band(k),
        )

    def orb_send(d, _):
        k = (me + d) % XY
        for q in range(NH):
            orb_copy(k, core, q).start()
            orb_copy(k, 1 - core, q).start()
        return 0

    lax.fori_loop(1, XY, orb_send, 0)
    own_orb = []
    for q in range(NH):
        orb_copy(me, 1 - core, q).start()
        own_orb.append(
            pltpu.make_async_copy(
                orb.at[pl.ds(16 * core, 16), :, columns(me, q)],
                xr.at[core, q, pl.ds(16 * me, 16)],
                oo_s.at[q],
            )
        )
        own_orb[q].start()
    small = [
        pltpu.make_async_copy(coup_hbm, coup, small_s.at[0]),
        pltpu.make_async_copy(species_hbm, species, small_s.at[1]),
        pltpu.make_async_copy(offsets_hbm, offsets, small_s.at[2]),
    ]
    for one in small:
        one.start()

    jm[...] = turn_matrix()
    pm[...] = split_matrix()
    cpad[...] = jnp.zeros_like(cpad)
    for one in small:
        one.wait()
    for i in range(PER_ATOM):
        cpad[pl.ds(4 * i, 4), pl.ds(0, PER_ATOM)] = coup[i]
    for k in range(4):
        cm[k] = coupling_matrix(k, cpad[...], species[...], offsets[...])

    for k in range(4):
        own[k].wait()
        core_copy(k).wait_recv()

    def split(k, piece):
        start, n = GROUPS[k]

        def block(i, _):
            at = pl.multiple_of(start + 128 * i, 128)
            both = lax.dot_general(
                pm[...], praw[piece, pl.ds(at, 128)].reshape(256, WIDTH), NN,
                preferred_element_type=jnp.float32,
            ).astype(jnp.bfloat16)
            pc[piece, 0, pl.ds(at, 128), :] = both[:128]
            pc[piece, 1, pl.ds(at, 128), :] = both[128:]
            return 0

        lax.fori_loop(0, n // 128, block, 0, unroll=True)

    for k in range(4):
        split(k, 0)
        split(k, 2)

    for q in range(NH):
        own_orb[q].wait()
    arrived(xr.at[core, :, pl.ds(0, 240)], o_r.at[core])
    arrived(xr.at[1 - core], o_r.at[1 - core])

    def turn(i, _):
        g, q, r = i // 4, i // 2 % 2, i % 2
        rows = pl.ds(pl.multiple_of(256 * r, 256), 256)
        value = xr[g, q, pl.ds(pl.multiple_of(128 * r, 128), 128)].reshape(256, WIDTH)
        xt[g, q, rows, :] = value
        xj[g, q, rows, :] = lax.dot_general(
            jm[...], value, NN, preferred_element_type=jnp.float32
        ).astype(jnp.bfloat16)
        return 0

    lax.fori_loop(0, 8, turn, 0)

    pieces = ((0, core, h), (1, core, 1 - h), (2, 1 - core, h), (3, 1 - core, 1 - h))

    def pieces_product(k, r, chosen):
        start, n = GROUPS[k]
        rows = pl.ds(pl.multiple_of(256 * r, 256), 256)
        total = None
        for i, g, q in chosen:
            re = lax.dot_general(
                xt[g, q, rows, :], pc[i, 0, pl.ds(start, n), :], NT,
                preferred_element_type=jnp.float32,
            )
            im = lax.dot_general(
                xj[g, q, rows, :], pc[i, 1, pl.ds(start, n), :], NT,
                preferred_element_type=jnp.float32,
            )
            total = re + im if total is None else total + re + im
        return rows, total

    def first_early(k):
        n = GROUPS[k][1]

        def block(r, _):
            rows, total = pieces_product(k, r, (pieces[0], pieces[2]))
            pacc[rows, pl.ds(0, n)] = total
            return 0

        lax.fori_loop(0, 2, block, 0, unroll=True)

    def first_arrived(k):
        n = GROUPS[k][1]

        def block(r, _):
            rows, total = pieces_product(k, r, (pieces[1],))
            pacc[rows, pl.ds(0, n)] = total + pacc[rows, pl.ds(0, n)]
            return 0

        lax.fori_loop(0, 2, block, 0, unroll=True)

    def first_product(k):
        n = GROUPS[k][1]

        def block(r, _):
            rows, total = pieces_product(k, r, (pieces[3],))
            sb[k, rows, pl.ds(0, n)] = (total + pacc[rows, pl.ds(0, n)]).astype(jnp.bfloat16)
            return 0

        lax.fori_loop(0, 2, block, 0, unroll=True)

    def rs_send(k):
        n = GROUPS[k][1]

        def one(d, _):
            to = (me + d) % XY
            copy(
                sb.at[k, pl.ds(32 * to, 32), pl.ds(0, n)],
                rb.at[k, XY - 1 - d, :, pl.ds(0, n)],
                rs_s.at[k], rs_r.at[k], ga, xy_band(to),
            ).start()
            return 0

        lax.fori_loop(1, XY, one, 0, unroll=True)

    def z_sum(k):
        n = GROUPS[k][1]
        arrived(rb.at[k, :, :, pl.ds(0, n)], rs_r.at[k])
        total = sb[k, pl.ds(32 * me, 32), pl.ds(0, n)].astype(jnp.float32)
        for d in range(XY - 1):
            total = total + rb[k, d, :, pl.ds(0, n)].astype(jnp.float32)
        town[k, :, pl.ds(0, n)] = total
        zs[k, :, pl.ds(0, n)] = total.astype(jnp.bfloat16)
        for c in range(1, NZ):
            to = (zl + c) % NZ
            copy(
                zs.at[k, :, pl.ds(0, n)], zr.at[k, NZ - 1 - c, :, pl.ds(0, n)],
                z_s.at[k], z_r.at[k], to * NC + core, band,
            ).start()

    def couple(k):
        n = GROUPS[k][1]
        arrived(zr.at[k, :, :, pl.ds(0, n)], z_r.at[k])
        total = town[k, :, pl.ds(0, n)]
        for c in range(NZ - 1):
            total = total + zr[k, c, :, pl.ds(0, n)].astype(jnp.float32)
        coupled = lax.dot_general(
            total, cm[k, pl.ds(0, n), pl.ds(0, n)], NT, precision=HIGHEST,
            preferred_element_type=jnp.float32,
        )
        dg[k, pl.ds(0, 32), pl.ds(0, n)] = coupled.astype(jnp.bfloat16)
        for batch, (first, end) in enumerate(BATCHES):
            for slot in range(max(first, 1), end):
                copy(
                    dg.at[k, pl.ds(0, 32), pl.ds(0, n)],
                    dg.at[k, pl.ds(32 * slot, 32), pl.ds(0, n)],
                    ag_s.at[k], ag_r.at[k, batch], ga, apart(OFFSETS[slot], -1),
                ).start()

    def gather_batch(k, batch):
        first, end = BATCHES[batch]
        first = max(first, 1)
        n = GROUPS[k][1]
        arrived(dg.at[k, pl.ds(32 * first, 32 * (end - first)), pl.ds(0, n)], ag_r.at[k, batch])

    def gather(k):
        n = GROUPS[k][1]
        for batch in range(3):
            gather_batch(k, batch)

        def block(r, _):
            rows = pl.ds(256 * r, 256)
            dj[k, rows, pl.ds(0, n)] = (
                -lax.dot_general(
                    jm[...], dg[k, rows, pl.ds(0, n)], NN, preferred_element_type=jnp.float32
                )
            ).astype(jnp.bfloat16)
            return 0

        lax.fori_loop(0, 2, block, 0, unroll=True)

    def second_piece(i, groups):
        def block(r, _):
            rows = pl.ds(pl.multiple_of(256 * r, 256), 256)
            total = None
            for k in groups:
                start, n = GROUPS[k]
                re = lax.dot_general(
                    dg[k, rows, pl.ds(0, n)], pc[i, 0, pl.ds(start, n), :], NN,
                    preferred_element_type=jnp.float32,
                )
                im = lax.dot_general(
                    dj[k, rows, pl.ds(0, n)], pc[i, 1, pl.ds(start, n), :], NN,
                    preferred_element_type=jnp.float32,
                )
                total = re + im if total is None else total + re + im
            acc[i, rows, :] = total
            return 0

        lax.fori_loop(0, 2, block, 0, unroll=True)

    def second_product(groups):
        for i in range(4):
            second_piece(i, groups)

    for k in range(4):
        first_early(k)
        z_copy(k).wait_recv()
        fwd_copy(k).start()
        split(k, 1)
        first_arrived(k)
        fwd_copy(k).wait_recv()
        split(k, 3)
        first_product(k)
        rs_send(k)
        if k >= 1:
            z_sum(k - 1)
        if k >= 2:
            couple(k - 2)
    gather(0)
    z_sum(3)
    couple(2)
    second_product((0,))
    couple(3)

    def back_copy(slot, c, q):
        return copy(
            ab.at[c, q, pl.ds(16 * slot, 16)],
            out.at[pl.ds(16 * core, 16), :, columns(me, q)],
            b_s, b_r.at[core], zl * NC + c, apart(OFFSETS[slot], 1),
        )

    late = (1, 2, 3)
    for batch, (first, end) in enumerate(BATCHES):
        rows = pl.ds(32 * first, 32 * (end - first))
        height = 32 * (end - first)
        turned = {}
        for k in late:
            n = GROUPS[k][1]
            gather_batch(k, batch)
            value = dg[k, rows, pl.ds(0, n)].astype(jnp.float32)
            even = (lax.broadcasted_iota(jnp.int32, value.shape, 0) & 1) == 0
            turned[k] = jnp.where(
                even, -pltpu.roll(value, height - 1, 0), pltpu.roll(value, 1, 0)
            ).astype(jnp.bfloat16)
        for side, c in ((2, 1 - core), (0, core)):
            for i, g, q in pieces[side : side + 2]:
                total = acc[i, rows, :]
                for k in late:
                    start, n = GROUPS[k]
                    re = lax.dot_general(
                        dg[k, rows, pl.ds(0, n)], pc[i, 0, pl.ds(start, n), :], NN,
                        preferred_element_type=jnp.float32,
                    )
                    im = lax.dot_general(
                        turned[k], pc[i, 1, pl.ds(start, n), :], NN,
                        preferred_element_type=jnp.float32,
                    )
                    total = total + (re + im)
                ab[g, q, pl.ds(16 * first, 16 * (end - first))] = (
                    total.astype(jnp.bfloat16).reshape(height // 2, 2, WIDTH)
                )
            for slot in range(first, end):
                for q in range(NH):
                    if slot > 0 or side == 2:
                        back_copy(slot, c, q).start()
    for q in range(NH):
        out[pl.ds(16 * core, 16), :, columns(me, q)] = ab[core, q, pl.ds(0, 16)]

    for k in range(4):
        n = GROUPS[k][1]
        z_copy(k).wait_send()
        core_copy(k).wait_send()
        fwd_copy(k).wait_send()
        left(rb.at[k, :, :, pl.ds(0, n)], rs_s.at[k])
        left(zr.at[k, :, :, pl.ds(0, n)], z_s.at[k])
        left(dg.at[k, pl.ds(0, 480), pl.ds(0, n)], ag_s.at[k])
    left(xr.at[0], o_s)
    left(xr.at[0, :, pl.ds(0, 240)], o_s)
    left(ab.at[0], b_s)
    left(ab.at[0, :, pl.ds(0, 240)], b_s)
    arrived(ab.at[core, :, pl.ds(0, 240)], b_r.at[core])
    arrived(ab.at[1 - core], b_r.at[1 - core])


def per_device(orbitals, projectors, coupling, species, offsets):
    bf16, f32 = jnp.bfloat16, jnp.float32
    vmem = pl.BlockSpec(memory_space=pltpu.VMEM)
    hbm = pl.BlockSpec(memory_space=pltpu.HBM)
    dma = pltpu.SemaphoreType.DMA
    return pl.pallas_call(
        kernel,
        out_shape=pltpu.VMEM(orbitals.shape, bf16),
        in_specs=[hbm] * 5,
        out_specs=vmem,
        scratch_shapes=[
            pltpu.VMEM((4, ROWS, 2, WIDTH), bf16),
            pltpu.VMEM((4, 2, ROWS, WIDTH), bf16),
            pltpu.VMEM((2, 2, 256, 2, WIDTH), bf16),
            pltpu.VMEM((2, 2, 512, WIDTH), bf16),
            pltpu.VMEM((2, 2, 512, WIDTH), bf16),
            pltpu.VMEM((256, 256), bf16),
            pltpu.VMEM((256, 256), bf16),
            pltpu.VMEM((4, 256, 256), f32),
            pltpu.VMEM((128, 128), f32),
            pltpu.VMEM((4, 512, 256), bf16),
            pltpu.VMEM((4, XY - 1, 32, 256), bf16),
            pltpu.VMEM((4, 32, 256), f32),
            pltpu.VMEM((4, 32, 256), bf16),
            pltpu.VMEM((4, NZ - 1, 32, 256), bf16),
            pltpu.VMEM((4, 512, 256), bf16),
            pltpu.VMEM((4, 512, 256), bf16),
            pltpu.VMEM((4, 512, WIDTH), f32),
            pltpu.VMEM((2, 2, 256, 2, WIDTH), bf16),
            dma((4,)), dma((4,)), dma((4,)), dma((4,)), dma((4,)), dma((4,)),
            dma, dma((2,)), dma((4,)), dma((4,)), dma((4,)), dma((4,)),
            dma((4,)), dma((4, 3)), dma, dma((2,)), dma((4,)), dma((2,)),
            pltpu.VMEM((PER_ATOM, 4, PER_ATOM), f32),
            pltpu.VMEM((1, 48), jnp.int32),
            pltpu.VMEM((1, 48), jnp.int32),
            dma((3,)),
            pltpu.VMEM((512, 256), f32),
            pltpu.SemaphoreType.REGULAR((LEVELS,)),
        ],
        compiler_params=pltpu.CompilerParams(collective_id=0, has_side_effects=True),
    )(
        orbitals, projectors, coupling.transpose(1, 0, 2),
        species.reshape(1, -1), offsets.reshape(1, -1),
    )


def solution(mesh):
    placed = (P("band", None, "ga"), P(None, None, ("ga", "band")), P(), P(), P())
    return jax.shard_map(
        per_device, mesh=mesh, in_specs=placed, out_specs=P("band", None, "ga"), check_vma=False
    )
```
